32 devices in a mesh: gx: 4 (over y, x), gy: 4 (over z), gz: 2 (over core).
Axes of the slice: x: 2, y: 2, z: 4, core: 2. Of those that a mesh axis runs over, the one named last changes fastest.
Arguments:
- residual: float32 [3, 32, 256, 512], P(None, 'gz', 'gx', 'gy'), may hold values from -32 to 32
- edge_diag: float32 [3, 32, 256, 512], P(None, 'gz', 'gx', 'gy'), may hold values from 6.5 to 9
- node_shift: float32 [32, 256, 512], P('gz', 'gx', 'gy'), may hold values from 0.05 to 3
- coarse_shift: float32 [16, 128, 256], P('gz', 'gx', 'gy'), may hold values from 0.05 to 3
Outputs:
- correction: float32 [3, 32, 256, 512], P(None, 'gz', 'gx', 'gy')
The draws below stay inside these ranges and needn't reach their ends.
All inputs are finite; a program needn't handle non-finite values.
Results may differ from the reference program's by a relative error of at most 0.000021.
Values sent between devices are 32-bit elements; how exact they have to be, the bound alone decides.
A program may use at most 128 MiB of HBM per device.

```python
import math
import jax
import jax.numpy as jnp

NX = 256
NY = 512
NZ = 32


def draw_residual(key, part):
    second_key = jax.random.fold_in(jax.random.fold_in(key, 11), 1)
    zpos = jnp.arange(NZ, dtype=jnp.float32) / NZ
    xpos = jnp.arange(NX, dtype=jnp.float32) / NX
    ramp = 2.0 * (1.0 + zpos)[:, None, None] * (1.0 + xpos)[None, :, None] * jnp.ones((1, 1, NY), jnp.float32)
    rough = jnp.clip(jax.random.normal(second_key, (3, NZ, NX, NY), jnp.float32), -4.0, 4.0)
    values = ramp[None] * rough
    return values.astype(jnp.float32)


def level_of(own_key, shape, shards, least, top_value):
    loudness = 1.0
    for position, shards_of in shards:
        draws = jax.random.uniform(jax.random.fold_in(jax.random.fold_in(own_key, 6), position), (shards_of,), jnp.float32, least / len(shards), top_value / len(shards))
        loudness = loudness * jnp.repeat(jnp.exp(draws), shape[position] // shards_of).reshape((-1,) + (1,) * (len(shape) - 1 - position))
    return loudness


def setup_inputs(seed: int = 0) -> dict:
    keys = jax.random.split(jax.random.key(seed), 5)
    return {
        "residual": draw_residual(jax.random.fold_in(keys[4], 71), 0),
        "edge_diag": jnp.clip(6.5 + 2.5 * jax.random.uniform(keys[1], (3, NZ, NX, NY), jnp.float32) ** level_of(keys[1], (3, NZ, NX, NY), ((1, 2), (2, 4), (3, 4)), -0.2, 0.2), 6.5, 9.0),
        "node_shift": jnp.clip(jnp.exp(math.log(3.0) - 4.0943445 * jax.random.uniform(keys[2], (NZ, NX, NY), jnp.float32) ** level_of(keys[2], (NZ, NX, NY), ((0, 2), (1, 4), (2, 4)), -0.2, 0.2)), 0.05, 3.0),
        "coarse_shift": jnp.clip(jnp.exp(math.log(3.0) - 4.0943445 * jax.random.uniform(keys[3], (NZ // 2, NX // 2, NY // 2), jnp.float32) ** level_of(keys[3], (NZ // 2, NX // 2, NY // 2), ((0, 2), (1, 4), (2, 4)), -0.2, 0.2)), 0.05, 3.0),
    }


def neighbours(padded):
    total = padded[2:, 1:-1, 1:-1] + padded[:-2, 1:-1, 1:-1]
    total = total + padded[1:-1, 2:, 1:-1] + padded[1:-1, :-2, 1:-1]
    return total + padded[1:-1, 1:-1, 2:] + padded[1:-1, 1:-1, :-2]


def apply_op(field, diagonal):
    return diagonal * field - neighbours(jnp.pad(field, 1))


def reference(residual, edge_diag, node_shift, coarse_shift):
    scaled = residual / edge_diag
    padded = jnp.pad(scaled, ((0, 0), (1, 1), (1, 1), (1, 1)))
    edge_near = jnp.stack([neighbours(padded[component]) for component in range(3)])
    smooth_part = 2.0 * scaled - (edge_diag * scaled - edge_near) / edge_diag
    nodal_rhs = (padded[0, :-2, 1:-1, 1:-1] - scaled[0]) + (padded[1, 1:-1, :-2, 1:-1] - scaled[1]) + (padded[2, 1:-1, 1:-1, :-2] - scaled[2])
    node_diag = 6.0 + node_shift
    first_guess = nodal_rhs / node_diag
    node_res = nodal_rhs - apply_op(first_guess, node_diag)
    sx, sy, sz = node_res.shape
    coarse_rhs = node_res.reshape(sx // 2, 2, sy // 2, 2, sz // 2, 2).sum(axis=(1, 3, 5))
    coarse_diag = 6.0 + coarse_shift
    first_dir = coarse_rhs / coarse_diag
    first_image = apply_op(first_dir, coarse_diag)
    second_dir = first_image / coarse_diag
    second_image = apply_op(second_dir, coarse_diag)
    gone = jnp.sum(first_dir * coarse_rhs)
    gtwo = jnp.sum(second_dir * coarse_rhs)
    hone = jnp.sum(first_dir * first_image)
    hmix = jnp.sum(second_dir * first_image)
    htwo = jnp.sum(second_dir * second_image)
    coef_two = (gtwo - hmix * gone / hone) / (htwo - hmix * hmix / hone)
    coef_one = (gone - hmix * coef_two) / hone
    coarse_sol = coef_one * first_dir + coef_two * second_dir
    spread = jnp.broadcast_to(coarse_sol[:, None, :, None, :, None], (sx // 2, 2, sy // 2, 2, sz // 2, 2)).reshape(sx, sy, sz)
    nodal = first_guess + spread
    final_nodal = nodal + (nodal_rhs - apply_op(nodal, node_diag)) / node_diag
    fpad = jnp.pad(final_nodal, 1)
    grads = jnp.stack([fpad[2:, 1:-1, 1:-1] - final_nodal, fpad[1:-1, 2:, 1:-1] - final_nodal, fpad[1:-1, 1:-1, 2:] - final_nodal])
    return smooth_part + grads
```

```python
import functools
import itertools
import math

import jax
import jax.numpy as jnp
from jax import lax
from jax.experimental import pallas as pl
from jax.experimental.pallas import tpu as pltpu
from jax.sharding import PartitionSpec as P

MESH = pl.DeviceIdType.MESH
AXES = ("gz", "gx", "gy")
FGI, V1I, V2I, F0I = 3, 4, 5, 6
PAD = 8
FEW = 32


def phases_of(sizes):
    return ((0, 1, 2),) if math.prod(sizes) <= FEW else ((1, 2), (0,))


def greeted(sizes, rounds, moves):
    near = set(itertools.product((-1, 0, 1), repeat=3))
    known = set(near)
    for _ in range(rounds):
        known |= {tuple(p + q for p, q in zip(k, m)) for k in known for m in moves}
    needed = set()
    for axes in phases_of(sizes):
        spans = [range(1 - sizes[a], sizes[a]) if a in axes else (0,) for a in range(3)]
        needed |= set(itertools.product(*spans))
    every = near | (needed - known)
    return sorted(o for o in every if any(o) and all(abs(p) < n for p, n in zip(o, sizes)))


def kernel(
    sizes,
    res, dia, shf, csh, OB, G1, G2, CO,
    R, D, NI, CS, S, FG, CI, CR, A1, T, V1, V2, F,
    SX, RX, SY, RY,
    in_sem, send_sem, recv_sem, psend, precv, *slots_of,
):
    phases = phases_of(sizes)
    n0, n1, n2 = NI.shape
    m0, m1, m2 = CS.shape
    groups = n1 // 8
    me = [lax.axis_index(a) for a in AXES]
    rows = pl.ds(PAD, n1)

    def offsets(axes):
        every = itertools.product(*[range(sizes[a]) for a in axes])
        return [offs for offs in every if any(offs)]

    def partner(axes, offs, sign):
        return {
            AXES[a]: lax.rem(me[a] + (o if sign > 0 else sizes[a] - o), sizes[a]) for a, o in zip(axes, offs)
        }

    loads = []
    for k in (1, 2, 0):
        for src, dst in ((res, R), (dia, D)):
            loads.append(pltpu.make_async_copy(src.at[k], dst.at[k], in_sem.at[len(loads)]))
    loads.append(pltpu.make_async_copy(shf, NI, in_sem.at[6]))
    loads.append(pltpu.make_async_copy(csh, CS, in_sem.at[7]))
    for c in loads:
        c.start()

    zplane = jnp.zeros((n1, n2), jnp.float32)
    for k in range(3):
        S[k, 0, rows] = zplane
        S[k, n0 + 1, rows] = zplane
        F[k, n0, 0:n1] = zplane
    FG[0, rows] = zplane
    FG[n0 + 1, rows] = zplane
    for V in (V1, V2):
        V[0, rows] = zplane
        V[m0 + 1, rows] = zplane
    RX[...] = jnp.zeros(RX.shape, jnp.float32)
    RY[...] = jnp.zeros(RY.shape, jnp.float32)
    barrier = pltpu.get_barrier_semaphore()
    faces = [tuple(d if b == a else 0 for b in range(3)) for a in range(3) for d in (-1, 1)]
    total = jnp.int32(0)
    for offs in greeted(sizes, 4, faces):
        there = functools.reduce(
            jnp.logical_and, [(me[a] + o >= 0) & (me[a] + o < sizes[a]) for a, o in enumerate(offs) if o]
        )
        peer = {AXES[a]: me[a] + o for a, o in enumerate(offs) if o}
        pl.when(there)(
            lambda peer=peer: pl.semaphore_signal(barrier, inc=1, device_id=peer, device_id_type=MESH)
        )
        total = total + there.astype(jnp.int32)

    lane = lax.broadcasted_iota(jnp.int32, (8, n2), 1)
    lane_full = lax.broadcasted_iota(jnp.int32, (n1, n2), 1)
    row_full = lax.broadcasted_iota(jnp.int32, (n1, n2), 0)
    row8 = lax.broadcasted_iota(jnp.int32, (8, n2), 0)
    keys = {p: ((lane + p // 2) // p) % (n2 // p) for p in (2, 4)}
    is_low = {p: (lane % p) >= p // 2 for p in (2, 4)}

    def place(i, g, p):
        k = i * groups + g
        per = n2 // p
        return k // per, k % per

    def pack(f, plane, count, p):
        accs = [jnp.zeros((8, n2), jnp.float32) for _ in range(place(count - 1, groups - 1, p)[0] + 1)]
        for i in range(count):
            x = plane(i)
            for g in range(groups):
                v, kk = place(i, g, p)
                part = x[8 * g : 8 * g + 8]
                if kk:
                    part = pltpu.roll(part, p * kk, 1)
                accs[v] = jnp.where(keys[p] == kk, part, accs[v])
        for v, acc in enumerate(accs):
            SY[f, v] = acc

    def arrived(f, p):
        return [jnp.where(is_low[p], RY[f, 0, v], RY[f, 1, v]) for v in range(RY.shape[2])]

    def halo(ws, i, p):
        parts = []
        for g in range(groups):
            v, kk = place(i, g, p)
            parts.append(pltpu.roll(ws[v], n2 - p * kk, 1) if kk else ws[v])
        return jnp.concatenate(parts, axis=0)

    def from_low(x, h, sh=1):
        return pltpu.roll(jnp.where(lane_full >= n2 - sh, h, x), sh, 1)

    def from_high(x, h, sh=1):
        return pltpu.roll(jnp.where(lane_full < sh, h, x), n2 - sh, 1)

    def inplane(ref, x, h, sh):
        near = ref[pl.ds(PAD - sh, n1)] + ref[pl.ds(PAD + sh, n1)]
        return near + from_low(x, h, sh) + from_high(x, h, sh)

    def local_near(ref, i, n, sh):
        x = ref[1 + i, rows]
        near = jnp.where(row_full >= sh, ref[1 + i, pl.ds(PAD - sh, n1)], 0.0)
        near = near + jnp.where(row_full < n1 - sh, ref[1 + i, pl.ds(PAD + sh, n1)], 0.0)
        near = near + jnp.where(lane_full >= sh, pltpu.roll(x, sh, 1), 0.0)
        near = near + jnp.where(lane_full < n2 - sh, pltpu.roll(x, n2 - sh, 1), 0.0)
        if i > 0:
            near = near + ref[i, rows]
        if i < n - 1:
            near = near + ref[i + 2, rows]
        return near

    def edges(f, p):
        sh = p // 2
        return [
            jnp.where(is_low[p], pltpu.roll(RY[f, 1, v], n2 - sh, 1), pltpu.roll(RY[f, 0, v], sh, 1))
            for v in range(RY.shape[2])
        ]

    def outer_near(near, ref, f, ws, i, n, p):
        sh = p // 2
        if i == 0:
            near = near + ref[0, rows]
        if i == n - 1:
            near = near + ref[n + 1, rows]
        side = (lane_full < sh) | (lane_full >= n2 - sh)
        near = near + jnp.where(side, halo(ws, i, p), 0.0)
        low = near[0:8] + jnp.where(row8 < sh, RX[f, 0, i : i + 1], 0.0)
        high = near[n1 - 8 : n1] + jnp.where(row8 >= 8 - sh, RX[f, 1, i : i + 1], 0.0)
        return jnp.concatenate([low, near[8 : n1 - 8], high], axis=0)

    def field(f):
        if f < 3:
            return S.at[f], n0
        return {FGI: (FG, n0), V1I: (V1, m0), V2I: (V2, m0)}[f]

    def message(f, a, d):
        if a == 0:
            if f >= F0I:
                src, dst = F.at[f - F0I, 0, pl.ds(0, n1)], F.at[f - F0I, n0, pl.ds(0, n1)]
            else:
                ref, n = field(f)
                src = ref.at[n if d else 1, rows]
                dst = ref.at[0 if d else n + 1, rows]
        elif a == 1:
            count = m0 if f in (V1I, V2I) else n0
            src, dst = SX.at[f, d, pl.ds(0, count)], RX.at[f, 1 - d, pl.ds(0, count)]
        else:
            src, dst = SY.at[f], RY.at[f, 1 - d]
        step = 1 if d else -1
        return pltpu.make_async_remote_copy(
            src_ref=src, dst_ref=dst, send_sem=send_sem.at[f, a, d], recv_sem=recv_sem.at[f, a, d],
            device_id={AXES[a]: lax.rem(me[a] + step + sizes[a], sizes[a])}, device_id_type=MESH,
        )

    def dirs(f):
        return (0,) if f >= F0I else (0, 1)

    def can_send(a, d):
        return me[a] < sizes[a] - 1 if d else me[a] > 0

    def send(f, a):
        for d in dirs(f):
            pl.when(can_send(a, d))(lambda f=f, a=a, d=d: message(f, a, d).start())

    def receive(f, a):
        for d in dirs(f):
            pl.when(can_send(a, 1 - d))(lambda f=f, a=a, d=d: message(f, a, d).wait_recv())

    def faces_x(f, get, count):
        for i in range(count):
            SX[f, 0, i : i + 1] = get(i, 0)
            if f < F0I:
                SX[f, 1, i : i + 1] = get(i, n1 - 1)

    def rows_x(f, width):
        ref, count = field(f)
        for i in range(count):
            for w in range(width):
                ref[1 + i, PAD - 1 - w : PAD - w] = RX[f, 0, i : i + 1]
                ref[1 + i, PAD + n1 + w : PAD + n1 + w + 1] = RX[f, 1, i : i + 1]

    def exchange(f, p):
        ref, count = field(f)
        send(f, 0)
        faces_x(f, lambda i, r: ref[1 + i, PAD + r : PAD + r + 1], count)
        send(f, 1)
        pack(f, lambda i: ref[1 + i, rows], count, p)
        send(f, 2)

    def one(f, a):
        ref, count = field(f)
        if a == 1:
            faces_x(f, lambda i, r: ref[1 + i, PAD + r : PAD + r + 1], count)
        if a == 2:
            pack(f, lambda i: ref[1 + i, rows], count, 2)
        send(f, a)

    for pos, (k, a) in enumerate(((1, 1), (2, 2), (0, 0))):
        loads[2 * pos].wait()
        loads[2 * pos + 1].wait()
        for i in range(n0):
            inv = 1.0 / D[k, i]
            D[k, i] = inv
            S[k, 1 + i, rows] = R[k, i] * inv
        if pos == 0:
            pl.semaphore_wait(barrier, total)
        one(k, a)
    for f, a in ((0, 1), (2, 1), (1, 0), (2, 0), (0, 2), (1, 2)):
        one(f, a)

    loads[6].wait()
    for i in range(n0):
        NI[i] = 1.0 / (6.0 + NI[i])
    loads[7].wait()
    spread_rows = (
        lax.broadcasted_iota(jnp.int32, (n1, m1), 0) // 2 == lax.broadcasted_iota(jnp.int32, (n1, m1), 1)
    ).astype(jnp.float32)
    spread_cols = (
        lax.broadcasted_iota(jnp.int32, (m2, n2), 1) // 2 == lax.broadcasted_iota(jnp.int32, (m2, n2), 0)
    ).astype(jnp.float32)
    exact = functools.partial(
        jnp.dot, precision=lax.Precision.HIGHEST, preferred_element_type=jnp.float32
    )
    for i in range(m0):
        CI[i] = exact(spread_rows, exact(1.0 / (6.0 + CS[i]), spread_cols))

    for i in range(n0):
        x1, x2 = S[1, 1 + i, rows], S[2, 1 + i, rows]
        rhs = jnp.where(row_full >= 1, S[1, 1 + i, pl.ds(PAD - 1, n1)], 0.0) - x1
        rhs = rhs + (jnp.where(lane_full >= 1, pltpu.roll(x2, 1, 1), 0.0) - x2)
        rhs = rhs - S[0, 1 + i, rows]
        if i > 0:
            rhs = rhs + S[0, i, rows]
        F[0, i, 0:n1] = rhs
    receive(1, 1)
    receive(0, 0)
    receive(2, 2)
    ws = edges(2, 2)
    for i in range(n0):
        rhs = F[0, i, 0:n1] + jnp.where(lane_full < 1, halo(ws, i, 2), 0.0)
        if i == 0:
            rhs = rhs + S[0, 0, rows]
        first = rhs[0:8] + jnp.where(row8 < 1, RX[1, 0, i : i + 1], 0.0)
        FG[1 + i, rows] = jnp.concatenate([first, rhs[8:]], axis=0) * NI[i]
    exchange(FGI, 2)

    def smooth(k):
        for a in range(3):
            if (k, a) not in ((1, 1), (0, 0), (2, 2)):
                receive(k, a)
        rows_x(k, 1)
        w = arrived(k, 2)
        for i in range(n0):
            x = S[k, 1 + i, rows]
            near = S[k, i, rows] + S[k, i + 2, rows] + inplane(S.at[k, 1 + i], x, halo(w, i, 2), 1)
            OB[k, i] = x + near * D[k, i]

    for i in range(n0):
        F[0, i, 0:n1] = local_near(FG, i, n0, 1)
    smooth(0)

    for a in range(3):
        receive(FGI, a)
    ws = edges(FGI, 2)
    for c in range(m0):
        t = None
        for i in (2 * c, 2 * c + 1):
            near = outer_near(F[0, i, 0:n1], FG, FGI, ws, i, n0, 2)
            F[0, i, 0:n1] = near
            t = near if t is None else t + near
        t = t + jnp.where(lane_full % 2 == 0, pltpu.roll(t, n2 - 1, 1), pltpu.roll(t, 1, 1))
        T[c, rows] = t
        t = t + jnp.where(row_full % 2 == 0, T[c, pl.ds(PAD + 1, n1)], T[c, pl.ds(PAD - 1, n1)])
        CR[c] = t
        V1[1 + c, rows] = t * CI[c]
    exchange(V1I, 4)
    for c in range(m0):
        A1[c] = local_near(V1, c, m0, 2)

    def faces_f(j):
        f = F0I + j
        send(f, 0)
        faces_x(f, lambda i, r: F[j, i, r : r + 1], n0)
        send(f, 1)
        pack(f, lambda i: F[j, i, 0:n1], n0, 2)
        send(f, 2)

    for i in range(n0):
        F[0, i, 0:n1] = FG[1 + i, rows] + F[0, i, 0:n1] * NI[i]
    faces_f(0)
    smooth(1)

    for a in range(3):
        receive(V1I, a)
    ws = edges(V1I, 4)
    for c in range(m0):
        near = outer_near(A1[c], V1, V1I, ws, c, m0, 4)
        A1[c] = CR[c] - near
        V2[1 + c, rows] = V1[1 + c, rows] - near * CI[c]
    exchange(V2I, 4)

    def fold(x):
        acc = x[0:8]
        for g in range(1, groups):
            acc = acc + x[8 * g : 8 * g + 8]
        return acc

    def spread_near(j, V, w):
        for c in range(m0):
            x = V[1 + c, rows]
            near = x + inplane(V.at[1 + c], x, halo(w, c, 4), 1)
            F[j, 2 * c, 0:n1] = (near + V[c, rows]) * NI[2 * c]
            F[j, 2 * c + 1, 0:n1] = (near + V[c + 2, rows]) * NI[2 * c + 1]
        faces_f(j)

    sums = [jnp.zeros((8, n2), jnp.float32) for _ in range(5)]
    for c in range(m0):
        v1, v2, a1, cr = V1[1 + c, rows], V2[1 + c, rows], A1[c], CR[c]
        sums[0] = sums[0] + fold(v1 * cr)
        sums[1] = sums[1] + fold(v2 * cr)
        sums[2] = sums[2] + fold(v1 * a1)
        sums[3] = sums[3] + fold(v2 * a1)
        sums[4] = sums[4] + fold(v2 * (a1 - local_near(V2, c, m0, 2)))
    rows_x(V1I, 2)
    spread_near(1, V1, arrived(V1I, 4))

    for a in range(3):
        receive(V2I, a)
    outer = fold(V2[1, rows] * V2[0, rows] + V2[m0, rows] * V2[m0 + 1, rows])
    for v, w in enumerate(edges(V2I, 4)):
        outer = outer + SY[V2I, v] * w
    rim = SX[V2I, 0, 0:m0] * RX[V2I, 0, 0:m0] + SX[V2I, 1, 0:m0] * RX[V2I, 1, 0:m0]
    sums[4] = sums[4] - outer
    rim = 2.0 * jnp.sum(rim, axis=0, keepdims=True)
    sums[4] = sums[4] - jnp.where(row8 == 0, rim, 0.0)
    lane1 = lax.broadcasted_iota(jnp.int32, (1, n2), 1)
    part = jnp.zeros((1, n2), jnp.float32)
    for q, s in enumerate(sums):
        part = jnp.where(lane1 == q, jnp.sum(jnp.sum(s, axis=0, keepdims=True), axis=1, keepdims=True), part)

    def slot(axes, at):
        index = 0
        for a in axes:
            index = index * sizes[a] + at(a)
        return index

    def sum_message(p, offs, sign):
        axes, slots = phases[p], slots_of[p]
        other = partner(axes, offs, sign)
        index = slot(axes, (lambda a: me[a]) if sign > 0 else (lambda a: other[AXES[a]]))
        sem = p * slots_of[0].shape[0] + slot(axes, lambda a: offs[axes.index(a)])
        return pltpu.make_async_remote_copy(
            src_ref=slots.at[index], dst_ref=slots.at[index], send_sem=psend.at[sem], recv_sem=precv.at[sem],
            device_id=other, device_id_type=MESH,
        )

    def sum_start(p, value):
        slots_of[p][slot(phases[p], lambda a: me[a])] = value
        for offs in offsets(phases[p]):
            sum_message(p, offs, 1).start()

    def sum_end(p):
        for offs in offsets(phases[p]):
            sum_message(p, offs, -1).wait_recv()
        terms = [slots_of[p][d] for d in range(slots_of[p].shape[0])]
        while len(terms) > 1:
            terms = [functools.reduce(lambda x, y: x + y, terms[t : t + 2]) for t in range(0, len(terms), 2)]
        return terms[0]

    sum_start(0, part)
    rows_x(V2I, 2)
    spread_near(2, V2, arrived(V2I, 4))
    smooth(2)
    for j, G in enumerate((OB, G1, G2)):
        for a in range(3):
            receive(F0I + j, a)
        for i in range(n0):
            F[j, i, n1 : n1 + 1] = RX[F0I + j, 1, i : i + 1]
        wf = [RY[F0I + j, 1, v] for v in range(RY.shape[2])]
        for i in range(n0):
            x = F[j, i, 0:n1]
            grads = (F[j, i + 1, 0:n1] - x, F[j, i, 1 : n1 + 1] - x, from_high(x, halo(wf, i, 2)) - x)
            for k in range(3):
                G[k, i] = G[k, i] + grads[k] if j == 0 else grads[k]

    part = sum_end(0)
    for p in range(1, len(phases)):
        sum_start(p, part)
        part = sum_end(p)
    gone, gtwo, hone, hmix, htwo = [
        jnp.sum(jnp.where(lane1 == q, part, 0.0), axis=1, keepdims=True) for q in range(5)
    ]
    two = (gtwo - hmix * gone / hone) / (htwo - hmix * hmix / hone)
    oneco = (gone - hmix * two) / hone
    CO[0:1] = jnp.broadcast_to(oneco, (1, n2))
    CO[1:2] = jnp.broadcast_to(two, (1, n2))

    for p in range(len(phases)):
        for offs in offsets(phases[p]):
            sum_message(p, offs, 1).wait_send()
    for a in range(3):
        for d in (0, 1):
            def drain(a=a, d=d):
                for f in range(9):
                    if d in dirs(f):
                        message(f, a, d).wait_send()
            pl.when(can_send(a, d))(drain)


def combine(parts, OB, G1, G2, CO, out, W, sem):
    _, n0, n1, n2 = OB.shape
    one = jnp.broadcast_to(CO[0:1], (n1, n2))
    two = jnp.broadcast_to(CO[1:2], (n1, n2))
    step = n0 // parts
    copies = []
    for k in range(3):
        for h in range(parts):
            for i in range(h * step, (h + 1) * step):
                W[k, i] = OB[k, i] + one * G1[k, i] + two * G2[k, i]
            planes = pl.ds(h * step, step)
            copies.append(pltpu.make_async_copy(W.at[k, planes], out.at[k, planes], sem.at[k * parts + h]))
            copies[-1].start()
    for c in copies:
        c.wait()


def solution(mesh):
    sizes = tuple(mesh.shape[a] for a in AXES)

    def local(residual, edge_diag, node_shift, coarse_shift):
        n0, n1, n2 = node_shift.shape
        m0, m1, m2 = coarse_shift.shape
        vecs = max(-(-(n0 * (n1 // 8)) // (n2 // 2)), -(-(m0 * (n1 // 8)) // (n2 // 4)))
        f32 = jnp.float32
        counts = [math.prod(sizes[a] for a in axes) for axes in phases_of(sizes)]
        V = lambda *s: pltpu.VMEM(s, f32)
        scratch = [
            V(3, n0, n1, n2), V(3, n0, n1, n2), V(n0, n1, n2), V(m0, m1, m2),
            V(3, n0 + 2, n1 + 2 * PAD, n2), V(n0 + 2, n1 + 2 * PAD, n2),
            V(m0, n1, n2), V(m0, n1, n2), V(m0, n1, n2), V(m0, n1 + 2 * PAD, n2),
            V(m0 + 2, n1 + 2 * PAD, n2), V(m0 + 2, n1 + 2 * PAD, n2),
            V(3, n0 + 1, n1 + PAD, n2),
            V(9, 2, n0, n2), V(9, 2, n0, n2), V(9, vecs, 8, n2), V(9, 2, vecs, 8, n2),
            pltpu.SemaphoreType.DMA((8,)),
            pltpu.SemaphoreType.DMA((9, 3, 2)), pltpu.SemaphoreType.DMA((9, 3, 2)),
            pltpu.SemaphoreType.DMA((sum(counts),)), pltpu.SemaphoreType.DMA((sum(counts),)),
            *[V(c, 1, n2) for c in counts],
        ]
        field = pltpu.VMEM(residual.shape, f32)
        limit = 67_043_328 - 12 * math.prod(residual.shape) - 2**18
        fields = pl.pallas_call(
            functools.partial(kernel, sizes),
            out_shape=[field, field, field, pltpu.VMEM((8, n2), f32)],
            in_specs=[pl.BlockSpec(memory_space=pltpu.HBM)] * 4,
            out_specs=[pl.BlockSpec(memory_space=pltpu.VMEM)] * 4,
            scratch_shapes=scratch,
            compiler_params=pltpu.CompilerParams(collective_id=0, has_side_effects=True, vmem_limit_bytes=limit),
        )(residual, edge_diag, node_shift, coarse_shift)
        parts = 2 if n0 % 2 == 0 else 1
        return pl.pallas_call(
            functools.partial(combine, parts),
            out_shape=jax.ShapeDtypeStruct(residual.shape, f32),
            in_specs=[pl.BlockSpec(memory_space=pltpu.VMEM)] * 4,
            out_specs=pl.BlockSpec(memory_space=pltpu.HBM),
            scratch_shapes=[field, pltpu.SemaphoreType.DMA((3 * parts,))],
            compiler_params=pltpu.CompilerParams(vmem_limit_bytes=8 * math.prod(residual.shape)),
        )(*fields)

    placed = (
        P(None, "gz", "gx", "gy"),
        P(None, "gz", "gx", "gy"),
        P("gz", "gx", "gy"),
        P("gz", "gx", "gy"),
    )
    return jax.shard_map(
        local, mesh=mesh, in_specs=placed, out_specs=P(None, "gz", "gx", "gy"), check_vma=False
    )
```

```python
import functools
import itertools
import math

import jax
import jax.numpy as jnp
from jax import lax
from jax.experimental import pallas as pl
from jax.experimental.pallas import tpu as pltpu
from jax.sharding import PartitionSpec as P

MESH = pl.DeviceIdType.MESH
AXES = ("gz", "gx", "gy")
FGI, V1I, V2I, F0I = 3, 4, 5, 6
PAD = 8
FEW = 32


def phases_of(sizes):
    return ((0, 1, 2),) if math.prod(sizes) <= FEW else ((1, 2), (0,))


def greeted(sizes, rounds, moves):
    near = set(itertools.product((-1, 0, 1), repeat=3))
    known = set(near)
    for _ in range(rounds):
        known |= {tuple(p + q for p, q in zip(k, m)) for k in known for m in moves}
    needed = set()
    for axes in phases_of(sizes):
        spans = [range(1 - sizes[a], sizes[a]) if a in axes else (0,) for a in range(3)]
        needed |= set(itertools.product(*spans))
    every = near | (needed - known)
    return sorted(o for o in every if any(o) and all(abs(p) < n for p, n in zip(o, sizes)))


def kernel(
    sizes,
    res, dia, shf, csh, OB, G1, G2, CO,
    R, D, NI, CS, S, FG, CI, CR, A1, T, V1, V2, F,
    SX, RX, SY, RY,
    slots_of,
    in_sem, send_sem, recv_sem, psend, precv,
):
    phases = phases_of(sizes)
    n0, n1, n2 = NI.shape
    m0, m1, m2 = CS.shape
    groups = n1 // 8
    me = [lax.axis_index(a) for a in AXES]
    rows = pl.ds(PAD, n1)

    def offsets(axes):
        every = itertools.product(*[range(sizes[a]) for a in axes])
        return [offs for offs in every if any(offs)]

    def partner(axes, offs, sign):
        return {
            AXES[a]: lax.rem(me[a] + (o if sign > 0 else sizes[a] - o), sizes[a]) for a, o in zip(axes, offs)
        }

    loads = []
    for k in (1, 2, 0):
        for src, dst in ((res, R), (dia, D)):
            loads.append(pltpu.make_async_copy(src.at[k], dst.at[k], in_sem.at[len(loads)]))
    loads.append(pltpu.make_async_copy(shf, NI, in_sem.at[6]))
    loads.append(pltpu.make_async_copy(csh, CS, in_sem.at[7]))
    for c in loads:
        c.start()

    zplane = jnp.zeros((n1, n2), jnp.float32)
    for k in range(3):
        S[k, 0, rows] = zplane
        S[k, n0 + 1, rows] = zplane
        F[k, n0, 0:n1] = zplane
    FG[0, rows] = zplane
    FG[n0 + 1, rows] = zplane
    for V in (V1, V2):
        V[0, rows] = zplane
        V[m0 + 1, rows] = zplane
    RX[...] = jnp.zeros(RX.shape, jnp.float32)
    RY[...] = jnp.zeros(RY.shape, jnp.float32)
    barrier = pltpu.get_barrier_semaphore()
    faces = [tuple(d if b == a else 0 for b in range(3)) for a in range(3) for d in (-1, 1)]
    total = jnp.int32(0)
    for offs in greeted(sizes, 4, faces):
        there = functools.reduce(
            jnp.logical_and, [(me[a] + o >= 0) & (me[a] + o < sizes[a]) for a, o in enumerate(offs) if o]
        )
        peer = {AXES[a]: me[a] + o for a, o in enumerate(offs) if o}
        pl.when(there)(
            lambda peer=peer: pl.semaphore_signal(barrier, inc=1, device_id=peer, device_id_type=MESH)
        )
        total = total + there.astype(jnp.int32)

    lane = lax.broadcasted_iota(jnp.int32, (8, n2), 1)
    lane_full = lax.broadcasted_iota(jnp.int32, (n1, n2), 1)
    row_full = lax.broadcasted_iota(jnp.int32, (n1, n2), 0)
    row8 = lax.broadcasted_iota(jnp.int32, (8, n2), 0)
    keys = {p: ((lane + p // 2) // p) % (n2 // p) for p in (2, 4)}
    is_low = {p: (lane % p) >= p // 2 for p in (2, 4)}

    def place(i, g, p):
        k = i * groups + g
        per = n2 // p
        return k // per, k % per

    def pack(f, plane, count, p):
        accs = [jnp.zeros((8, n2), jnp.float32) for _ in range(place(count - 1, groups - 1, p)[0] + 1)]
        for i in range(count):
            x = plane(i)
            for g in range(groups):
                v, kk = place(i, g, p)
                part = x[8 * g : 8 * g + 8]
                if kk:
                    part = pltpu.roll(part, p * kk, 1)
                accs[v] = jnp.where(keys[p] == kk, part, accs[v])
        for v, acc in enumerate(accs):
            SY[f, v] = acc

    def arrived(f, p):
        return [jnp.where(is_low[p], RY[f, 0, v], RY[f, 1, v]) for v in range(RY.shape[2])]

    def halo(ws, i, p):
        parts = []
        for g in range(groups):
            v, kk = place(i, g, p)
            parts.append(pltpu.roll(ws[v], n2 - p * kk, 1) if kk else ws[v])
        return jnp.concatenate(parts, axis=0)

    def from_low(x, h, sh=1):
        return pltpu.roll(jnp.where(lane_full >= n2 - sh, h, x), sh, 1)

    def from_high(x, h, sh=1):
        return pltpu.roll(jnp.where(lane_full < sh, h, x), n2 - sh, 1)

    def inplane(ref, x, h, sh):
        near = ref[pl.ds(PAD - sh, n1)] + ref[pl.ds(PAD + sh, n1)]
        return near + from_low(x, h, sh) + from_high(x, h, sh)

    def local_near(ref, i, n, sh):
        x = ref[1 + i, rows]
        near = jnp.where(row_full >= sh, ref[1 + i, pl.ds(PAD - sh, n1)], 0.0)
        near = near + jnp.where(row_full < n1 - sh, ref[1 + i, pl.ds(PAD + sh, n1)], 0.0)
        near = near + jnp.where(lane_full >= sh, pltpu.roll(x, sh, 1), 0.0)
        near = near + jnp.where(lane_full < n2 - sh, pltpu.roll(x, n2 - sh, 1), 0.0)
        if i > 0:
            near = near + ref[i, rows]
        if i < n - 1:
            near = near + ref[i + 2, rows]
        return near

    def edges(f, p):
        sh = p // 2
        return [
            jnp.where(is_low[p], pltpu.roll(RY[f, 1, v], n2 - sh, 1), pltpu.roll(RY[f, 0, v], sh, 1))
            for v in range(RY.shape[2])
        ]

    def outer_near(near, ref, f, ws, i, n, p):
        sh = p // 2
        if i == 0:
            near = near + ref[0, rows]
        if i == n - 1:
            near = near + ref[n + 1, rows]
        side = (lane_full < sh) | (lane_full >= n2 - sh)
        near = near + jnp.where(side, halo(ws, i, p), 0.0)
        low = near[0:8] + jnp.where(row8 < sh, RX[f, 0, i : i + 1], 0.0)
        high = near[n1 - 8 : n1] + jnp.where(row8 >= 8 - sh, RX[f, 1, i : i + 1], 0.0)
        return jnp.concatenate([low, near[8 : n1 - 8], high], axis=0)

    def field(f):
        if f < 3:
            return S.at[f], n0
        return {FGI: (FG, n0), V1I: (V1, m0), V2I: (V2, m0)}[f]

    def message(f, a, d):
        if a == 0:
            if f >= F0I:
                src, dst = F.at[f - F0I, 0, pl.ds(0, n1)], F.at[f - F0I, n0, pl.ds(0, n1)]
            else:
                ref, n = field(f)
                src = ref.at[n if d else 1, rows]
                dst = ref.at[0 if d else n + 1, rows]
        elif a == 1:
            count = m0 if f in (V1I, V2I) else n0
            src, dst = SX.at[f, d, pl.ds(0, count)], RX.at[f, 1 - d, pl.ds(0, count)]
        else:
            src, dst = SY.at[f], RY.at[f, 1 - d]
        step = 1 if d else -1
        return pltpu.make_async_remote_copy(
            src_ref=src, dst_ref=dst, send_sem=send_sem.at[f, a, d], recv_sem=recv_sem.at[f, a, d],
            device_id={AXES[a]: lax.rem(me[a] + step + sizes[a], sizes[a])}, device_id_type=MESH,
        )

    def dirs(f):
        return (0,) if f >= F0I else (0, 1)

    def can_send(a, d):
        return me[a] < sizes[a] - 1 if d else me[a] > 0

    def send(f, a):
        for d in dirs(f):
            pl.when(can_send(a, d))(lambda f=f, a=a, d=d: message(f, a, d).start())

    def receive(f, a):
        for d in dirs(f):
            pl.when(can_send(a, 1 - d))(lambda f=f, a=a, d=d: message(f, a, d).wait_recv())

    def faces_x(f, get, count):
        for i in range(count):
            SX[f, 0, i : i + 1] = get(i, 0)
            if f < F0I:
                SX[f, 1, i : i + 1] = get(i, n1 - 1)

    def rows_x(f, width):
        ref, count = field(f)
        for i in range(count):
            for w in range(width):
                ref[1 + i, PAD - 1 - w : PAD - w] = RX[f, 0, i : i + 1]
                ref[1 + i, PAD + n1 + w : PAD + n1 + w + 1] = RX[f, 1, i : i + 1]

    def exchange(f, p):
        ref, count = field(f)
        send(f, 0)
        faces_x(f, lambda i, r: ref[1 + i, PAD + r : PAD + r + 1], count)
        send(f, 1)
        pack(f, lambda i: ref[1 + i, rows], count, p)
        send(f, 2)

    def one(f, a):
        ref, count = field(f)
        if a == 1:
            faces_x(f, lambda i, r: ref[1 + i, PAD + r : PAD + r + 1], count)
        if a == 2:
            pack(f, lambda i: ref[1 + i, rows], count, 2)
        send(f, a)

    for pos, (k, a) in enumerate(((1, 1), (2, 2), (0, 0))):
        loads[2 * pos].wait()
        loads[2 * pos + 1].wait()
        for i in range(n0):
            inv = 1.0 / D[k, i]
            D[k, i] = inv
            S[k, 1 + i, rows] = R[k, i] * inv
        if pos == 0:
            pl.semaphore_wait(barrier, total)
        one(k, a)
    for f, a in ((0, 1), (2, 1), (1, 0), (2, 0), (0, 2), (1, 2)):
        one(f, a)

    loads[6].wait()
    for i in range(n0):
        NI[i] = 1.0 / (6.0 + NI[i])
    loads[7].wait()
    spread_rows = (
        lax.broadcasted_iota(jnp.int32, (n1, m1), 0) // 2 == lax.broadcasted_iota(jnp.int32, (n1, m1), 1)
    ).astype(jnp.float32)
    spread_cols = (
        lax.broadcasted_iota(jnp.int32, (m2, n2), 1) // 2 == lax.broadcasted_iota(jnp.int32, (m2, n2), 0)
    ).astype(jnp.float32)
    exact = functools.partial(
        jnp.dot, precision=lax.Precision.HIGHEST, preferred_element_type=jnp.float32
    )
    for i in range(m0):
        CI[i] = exact(spread_rows, exact(1.0 / (6.0 + CS[i]), spread_cols))

    for i in range(n0):
        x1, x2 = S[1, 1 + i, rows], S[2, 1 + i, rows]
        rhs = jnp.where(row_full >= 1, S[1, 1 + i, pl.ds(PAD - 1, n1)], 0.0) - x1
        rhs = rhs + (jnp.where(lane_full >= 1, pltpu.roll(x2, 1, 1), 0.0) - x2)
        rhs = rhs - S[0, 1 + i, rows]
        if i > 0:
            rhs = rhs + S[0, i, rows]
        F[0, i, 0:n1] = rhs
    receive(1, 1)
    receive(0, 0)
    receive(2, 2)
    ws = edges(2, 2)
    for i in range(n0):
        rhs = F[0, i, 0:n1] + jnp.where(lane_full < 1, halo(ws, i, 2), 0.0)
        if i == 0:
            rhs = rhs + S[0, 0, rows]
        first = rhs[0:8] + jnp.where(row8 < 1, RX[1, 0, i : i + 1], 0.0)
        FG[1 + i, rows] = jnp.concatenate([first, rhs[8:]], axis=0) * NI[i]
    exchange(FGI, 2)

    def smooth(k):
        for a in range(3):
            if (k, a) not in ((1, 1), (0, 0), (2, 2)):
                receive(k, a)
        rows_x(k, 1)
        w = arrived(k, 2)
        for i in range(n0):
            x = S[k, 1 + i, rows]
            near = S[k, i, rows] + S[k, i + 2, rows] + inplane(S.at[k, 1 + i], x, halo(w, i, 2), 1)
            OB[k, i] = x + near * D[k, i]

    for i in range(n0):
        F[0, i, 0:n1] = local_near(FG, i, n0, 1)
    smooth(0)

    for a in range(3):
        receive(FGI, a)
    ws = edges(FGI, 2)
    for c in range(m0):
        t = None
        for i in (2 * c, 2 * c + 1):
            near = outer_near(F[0, i, 0:n1], FG, FGI, ws, i, n0, 2)
            F[0, i, 0:n1] = near
            t = near if t is None else t + near
        t = t + jnp.where(lane_full % 2 == 0, pltpu.roll(t, n2 - 1, 1), pltpu.roll(t, 1, 1))
        T[c, rows] = t
        t = t + jnp.where(row_full % 2 == 0, T[c, pl.ds(PAD + 1, n1)], T[c, pl.ds(PAD - 1, n1)])
        CR[c] = t
        V1[1 + c, rows] = t * CI[c]
    exchange(V1I, 4)
    for c in range(m0):
        A1[c] = local_near(V1, c, m0, 2)

    def faces_f(j):
        f = F0I + j
        send(f, 0)
        faces_x(f, lambda i, r: F[j, i, r : r + 1], n0)
        send(f, 1)
        pack(f, lambda i: F[j, i, 0:n1], n0, 2)
        send(f, 2)

    for i in range(n0):
        F[0, i, 0:n1] = FG[1 + i, rows] + F[0, i, 0:n1] * NI[i]
    faces_f(0)
    smooth(1)

    for a in range(3):
        receive(V1I, a)
    ws = edges(V1I, 4)
    for c in range(m0):
        near = outer_near(A1[c], V1, V1I, ws, c, m0, 4)
        A1[c] = CR[c] - near
        V2[1 + c, rows] = V1[1 + c, rows] - near * CI[c]
    exchange(V2I, 4)

    def fold(x):
        acc = x[0:8]
        for g in range(1, groups):
            acc = acc + x[8 * g : 8 * g + 8]
        return acc

    def spread_near(j, V, w):
        for c in range(m0):
            x = V[1 + c, rows]
            near = x + inplane(V.at[1 + c], x, halo(w, c, 4), 1)
            F[j, 2 * c, 0:n1] = (near + V[c, rows]) * NI[2 * c]
            F[j, 2 * c + 1, 0:n1] = (near + V[c + 2, rows]) * NI[2 * c + 1]
        faces_f(j)

    sums = [jnp.zeros((8, n2), jnp.float32) for _ in range(5)]
    for c in range(m0):
        v1, v2, a1, cr = V1[1 + c, rows], V2[1 + c, rows], A1[c], CR[c]
        sums[0] = sums[0] + fold(v1 * cr)
        sums[1] = sums[1] + fold(v2 * cr)
        sums[2] = sums[2] + fold(v1 * a1)
        sums[3] = sums[3] + fold(v2 * a1)
        sums[4] = sums[4] + fold(v2 * (a1 - local_near(V2, c, m0, 2)))
    rows_x(V1I, 2)
    spread_near(1, V1, arrived(V1I, 4))

    for a in range(3):
        receive(V2I, a)
    outer = fold(V2[1, rows] * V2[0, rows] + V2[m0, rows] * V2[m0 + 1, rows])
    for v, w in enumerate(edges(V2I, 4)):
        outer = outer + SY[V2I, v] * w
    rim = SX[V2I, 0, 0:m0] * RX[V2I, 0, 0:m0] + SX[V2I, 1, 0:m0] * RX[V2I, 1, 0:m0]
    sums[4] = sums[4] - outer
    rim = 2.0 * jnp.sum(rim, axis=0, keepdims=True)
    sums[4] = sums[4] - jnp.where(row8 == 0, rim, 0.0)
    lane1 = lax.broadcasted_iota(jnp.int32, (1, n2), 1)
    part = jnp.zeros((1, n2), jnp.float32)
    for q, s in enumerate(sums):
        part = jnp.where(lane1 == q, jnp.sum(jnp.sum(s, axis=0, keepdims=True), axis=1, keepdims=True), part)

    def slot(axes, at):
        index = 0
        for a in axes:
            index = index * sizes[a] + at(a)
        return index

    def sum_message(p, offs, sign):
        axes, slots = phases[p], slots_of[p]
        other = partner(axes, offs, sign)
        index = slot(axes, (lambda a: me[a]) if sign > 0 else (lambda a: other[AXES[a]]))
        sem = p * slots_of[0].shape[0] + slot(axes, lambda a: offs[axes.index(a)])
        return pltpu.make_async_remote_copy(
            src_ref=slots.at[index], dst_ref=slots.at[index], send_sem=psend.at[sem], recv_sem=precv.at[sem],
            device_id=other, device_id_type=MESH,
        )

    def sum_start(p, value):
        slots_of[p][slot(phases[p], lambda a: me[a])] = value
        for offs in offsets(phases[p]):
            sum_message(p, offs, 1).start()

    def sum_end(p):
        for offs in offsets(phases[p]):
            sum_message(p, offs, -1).wait_recv()
        terms = [slots_of[p][d] for d in range(slots_of[p].shape[0])]
        while len(terms) > 1:
            terms = [functools.reduce(lambda x, y: x + y, terms[t : t + 2]) for t in range(0, len(terms), 2)]
        return terms[0]

    sum_start(0, part)
    rows_x(V2I, 2)
    spread_near(2, V2, arrived(V2I, 4))
    smooth(2)
    for j, G in enumerate((OB, G1, G2)):
        for a in range(3):
            receive(F0I + j, a)
        for i in range(n0):
            F[j, i, n1 : n1 + 1] = RX[F0I + j, 1, i : i + 1]
        wf = [RY[F0I + j, 1, v] for v in range(RY.shape[2])]
        for i in range(n0):
            x = F[j, i, 0:n1]
            grads = (F[j, i + 1, 0:n1] - x, F[j, i, 1 : n1 + 1] - x, from_high(x, halo(wf, i, 2)) - x)
            for k in range(3):
                G[k, i] = G[k, i] + grads[k] if j == 0 else grads[k]

    part = sum_end(0)
    for p in range(1, len(phases)):
        sum_start(p, part)
        part = sum_end(p)
    gone, gtwo, hone, hmix, htwo = [
        jnp.sum(jnp.where(lane1 == q, part, 0.0), axis=1, keepdims=True) for q in range(5)
    ]
    two = (gtwo - hmix * gone / hone) / (htwo - hmix * hmix / hone)
    oneco = (gone - hmix * two) / hone
    CO[0:1] = jnp.broadcast_to(oneco, (1, n2))
    CO[1:2] = jnp.broadcast_to(two, (1, n2))

    for p in range(len(phases)):
        for offs in offsets(phases[p]):
            sum_message(p, offs, 1).wait_send()
    for a in range(3):
        for d in (0, 1):
            def drain(a=a, d=d):
                for f in range(9):
                    if d in dirs(f):
                        message(f, a, d).wait_send()
            pl.when(can_send(a, d))(drain)


def combine(parts, OB, G1, G2, CO, out, W, sem):
    _, n0, n1, n2 = OB.shape
    one = jnp.broadcast_to(CO[0:1], (n1, n2))
    two = jnp.broadcast_to(CO[1:2], (n1, n2))
    step = n0 // parts
    copies = []
    for k in range(3):
        for h in range(parts):
            for i in range(h * step, (h + 1) * step):
                W[k, i] = OB[k, i] + one * G1[k, i] + two * G2[k, i]
            planes = pl.ds(h * step, step)
            copies.append(pltpu.make_async_copy(W.at[k, planes], out.at[k, planes], sem.at[k * parts + h]))
            copies[-1].start()
    for c in copies:
        c.wait()


def solution(mesh):
    sizes = tuple(mesh.shape[a] for a in AXES)

    def local(residual, edge_diag, node_shift, coarse_shift):
        n0, n1, n2 = node_shift.shape
        m0, m1, m2 = coarse_shift.shape
        vecs = max(-(-(n0 * (n1 // 8)) // (n2 // 2)), -(-(m0 * (n1 // 8)) // (n2 // 4)))
        f32 = jnp.float32
        counts = [math.prod(sizes[a] for a in axes) for axes in phases_of(sizes)]
        V = lambda *s: pltpu.VMEM(s, f32)
        scratch = [
            V(3, n0, n1, n2), V(3, n0, n1, n2), V(n0, n1, n2), V(m0, m1, m2),
            V(3, n0 + 2, n1 + 2 * PAD, n2), V(n0 + 2, n1 + 2 * PAD, n2),
            V(m0, n1, n2), V(m0, n1, n2), V(m0, n1, n2), V(m0, n1 + 2 * PAD, n2),
            V(m0 + 2, n1 + 2 * PAD, n2), V(m0 + 2, n1 + 2 * PAD, n2),
            V(3, n0 + 1, n1 + PAD, n2),
            V(9, 2, n0, n2), V(9, 2, n0, n2), V(9, vecs, 8, n2), V(9, 2, vecs, 8, n2),
            *[V(c, 1, n2) for c in counts],
        ]
        sems = [pltpu.SemaphoreType.DMA(s) for s in ((8,), (9, 3, 2), (9, 3, 2), (sum(counts),), (sum(counts),))]

        def scoped(*refs):
            plain, slots_of = refs[: -len(counts)], refs[-len(counts) :]
            pl.run_scoped(functools.partial(kernel, sizes, *plain, slots_of), *sems)

        field = pltpu.VMEM(residual.shape, f32)
        limit = 67_043_328 - 12 * math.prod(residual.shape) - 2**18
        fields = pl.pallas_call(
            scoped,
            out_shape=[field, field, field, pltpu.VMEM((8, n2), f32)],
            in_specs=[pl.BlockSpec(memory_space=pltpu.HBM)] * 4,
            out_specs=[pl.BlockSpec(memory_space=pltpu.VMEM)] * 4,
            scratch_shapes=scratch,
            compiler_params=pltpu.CompilerParams(collective_id=0, has_side_effects=True, vmem_limit_bytes=limit),
        )(residual, edge_diag, node_shift, coarse_shift)
        parts = 2 if n0 % 2 == 0 else 1
        return pl.pallas_call(
            functools.partial(combine, parts),
            out_shape=jax.ShapeDtypeStruct(residual.shape, f32),
            in_specs=[pl.BlockSpec(memory_space=pltpu.VMEM)] * 4,
            out_specs=pl.BlockSpec(memory_space=pltpu.HBM),
            scratch_shapes=[field, pltpu.SemaphoreType.DMA((3 * parts,))],
            compiler_params=pltpu.CompilerParams(vmem_limit_bytes=8 * math.prod(residual.shape)),
        )(*fields)

    placed = (
        P(None, "gz", "gx", "gy"),
        P(None, "gz", "gx", "gy"),
        P("gz", "gx", "gy"),
        P("gz", "gx", "gy"),
    )
    return jax.shard_map(
        local, mesh=mesh, in_specs=placed, out_specs=P(None, "gz", "gx", "gy"), check_vma=False
    )
```

```python
import functools
import itertools
import math

import jax
import jax.numpy as jnp
from jax import lax
from jax.experimental import pallas as pl
from jax.experimental.pallas import tpu as pltpu
from jax.sharding import PartitionSpec as P

MESH = pl.DeviceIdType.MESH
AXES = ("gz", "gx", "gy")
FGI, V1I, V2I, F0I, NLI, CII = 3, 4, 5, 6, 9, 10
FIELDS = 11
FINAL = (F0I, F0I + 1, F0I + 2)
COARSE = (V1I, V2I, NLI, CII)
PAD = 8
FEW = 32


def phases_of(sizes):
    return ((0, 1, 2),) if math.prod(sizes) <= FEW else ((1, 2), (0,))


def greeted(sizes, rounds):
    near = set(itertools.product((-1, 0, 1), repeat=3))
    known = set(near)
    for moves in rounds:
        known |= {tuple(p + q for p, q in zip(k, m)) for k in known for m in moves}
    needed = set()
    for axes in phases_of(sizes):
        spans = [range(1 - sizes[a], sizes[a]) if a in axes else (0,) for a in range(3)]
        needed |= set(itertools.product(*spans))
    every = near | (needed - known)
    return sorted(o for o in every if any(o) and all(abs(p) < n for p, n in zip(o, sizes)))


def kernel(
    sizes,
    res, dia, shf, csh, OB, G1, G2, CO,
    R, D, NI, CS, S, FG, CI, CR, A1, NL, T, V1, V2, F,
    SX, RX, SY, RY, NZ, CZ, LZX, LXY, RZX, RZY, RXY,
    slots_of,
    in_sem, send_sem, recv_sem, psend, precv, lsend, lrecv,
):
    phases = phases_of(sizes)
    n0, n1, n2 = NI.shape
    m0, m1, m2 = CS.shape
    groups = n1 // 8
    me = [lax.axis_index(a) for a in AXES]
    rows = pl.ds(PAD, n1)

    def offsets(axes):
        every = itertools.product(*[range(sizes[a]) for a in axes])
        return [offs for offs in every if any(offs)]

    def partner(axes, offs, sign):
        return {
            AXES[a]: lax.rem(me[a] + (o if sign > 0 else sizes[a] - o), sizes[a]) for a, o in zip(axes, offs)
        }

    loads = []
    for k in (1, 2, 0):
        for src, dst in ((res, R), (dia, D)):
            loads.append(pltpu.make_async_copy(src.at[k], dst.at[k], in_sem.at[len(loads)]))
    loads.append(pltpu.make_async_copy(shf, NI, in_sem.at[6]))
    loads.append(pltpu.make_async_copy(csh, CS, in_sem.at[7]))
    for c in loads:
        c.start()

    zplane = jnp.zeros((n1, n2), jnp.float32)
    for k in range(3):
        S[k, 0, rows] = zplane
        S[k, n0 + 1, rows] = zplane
        F[k, n0, 0:n1] = zplane
    FG[0, rows] = zplane
    FG[n0 + 1, rows] = zplane
    for V in (V1, V2):
        V[0, rows] = zplane
        V[m0 + 1, rows] = zplane
    for buf in (RX, RY, NZ, CZ, RZX, RZY, RXY):
        buf[...] = jnp.zeros(buf.shape, jnp.float32)
    barrier = pltpu.get_barrier_semaphore()
    faces = [offs for offs in itertools.product((-1, 0, 1), repeat=3) if sum(map(abs, offs)) == 1]
    lines = [offs for offs in itertools.product((-1, 0, 1), repeat=3) if sum(map(abs, offs)) == 2]

    def exists(offs):
        inside = [(me[a] + o >= 0) & (me[a] + o < sizes[a]) for a, o in enumerate(offs) if o]
        return functools.reduce(jnp.logical_and, inside)

    def device(offs):
        return {AXES[a]: me[a] + o for a, o in enumerate(offs) if o}

    total = jnp.int32(0)
    for offs in greeted(sizes, (faces, faces, faces + lines)):
        there = exists(offs)
        pl.when(there)(
            lambda offs=offs: pl.semaphore_signal(
                barrier, inc=1, device_id=device(offs), device_id_type=MESH
            )
        )
        total = total + there.astype(jnp.int32)

    lane = lax.broadcasted_iota(jnp.int32, (8, n2), 1)
    lane_full = lax.broadcasted_iota(jnp.int32, (n1, n2), 1)
    row_full = lax.broadcasted_iota(jnp.int32, (n1, n2), 0)
    row8 = lax.broadcasted_iota(jnp.int32, (8, n2), 0)
    keys = {p: ((lane + p // 2) // p) % (n2 // p) for p in (2, 4)}
    is_low = {p: (lane % p) >= p // 2 for p in (2, 4)}

    def place(i, g, p):
        k = i * groups + g
        per = n2 // p
        return k // per, k % per

    def pack(f, plane, count, p):
        accs = [jnp.zeros((8, n2), jnp.float32) for _ in range(place(count - 1, groups - 1, p)[0] + 1)]
        for i in range(count):
            x = plane(i)
            for g in range(groups):
                v, kk = place(i, g, p)
                part = x[8 * g : 8 * g + 8]
                if kk:
                    part = pltpu.roll(part, p * kk, 1)
                accs[v] = jnp.where(keys[p] == kk, part, accs[v])
        for v, acc in enumerate(accs):
            SY[f, v] = acc

    def arrived(f, p):
        return [jnp.where(is_low[p], RY[f, 0, v], RY[f, 1, v]) for v in range(RY.shape[2])]

    def halo(ws, i, p):
        parts = []
        for g in range(groups):
            v, kk = place(i, g, p)
            parts.append(pltpu.roll(ws[v], n2 - p * kk, 1) if kk else ws[v])
        return jnp.concatenate(parts, axis=0)

    def from_low(x, h, sh=1):
        return pltpu.roll(jnp.where(lane_full >= n2 - sh, h, x), sh, 1)

    def from_high(x, h, sh=1):
        return pltpu.roll(jnp.where(lane_full < sh, h, x), n2 - sh, 1)

    def inplane(ref, x, h, sh):
        near = ref[pl.ds(PAD - sh, n1)] + ref[pl.ds(PAD + sh, n1)]
        return near + from_low(x, h, sh) + from_high(x, h, sh)

    def inplane_aligned(ref, x, h, sh):
        near = ref[pl.ds(PAD - sh, n1)] + ref[pl.ds(PAD + sh, n1)]
        near = near + jnp.where(lane_full < sh, h, pltpu.roll(x, sh, 1))
        return near + jnp.where(lane_full >= n2 - sh, h, pltpu.roll(x, n2 - sh, 1))

    def local_near(ref, i, n, sh):
        x = ref[1 + i, rows]
        near = jnp.where(row_full >= sh, ref[1 + i, pl.ds(PAD - sh, n1)], 0.0)
        near = near + jnp.where(row_full < n1 - sh, ref[1 + i, pl.ds(PAD + sh, n1)], 0.0)
        near = near + jnp.where(lane_full >= sh, pltpu.roll(x, sh, 1), 0.0)
        near = near + jnp.where(lane_full < n2 - sh, pltpu.roll(x, n2 - sh, 1), 0.0)
        if i > 0:
            near = near + ref[i, rows]
        if i < n - 1:
            near = near + ref[i + 2, rows]
        return near

    def edges(f, p):
        sh = p // 2
        return [
            jnp.where(is_low[p], pltpu.roll(RY[f, 1, v], n2 - sh, 1), pltpu.roll(RY[f, 0, v], sh, 1))
            for v in range(RY.shape[2])
        ]

    def outer_near(near, ref, f, ws, i, n, p):
        sh = p // 2
        if i == 0:
            near = near + ref[0, rows]
        if i == n - 1:
            near = near + ref[n + 1, rows]
        side = (lane_full < sh) | (lane_full >= n2 - sh)
        near = near + jnp.where(side, halo(ws, i, p), 0.0)
        low = near[0:8] + jnp.where(row8 < sh, RX[f, 0, i : i + 1], 0.0)
        high = near[n1 - 8 : n1] + jnp.where(row8 >= 8 - sh, RX[f, 1, i : i + 1], 0.0)
        return jnp.concatenate([low, near[8 : n1 - 8], high], axis=0)

    def field(f):
        if f < 3:
            return S.at[f], n0
        return {FGI: (FG, n0), V1I: (V1, m0)}[f]

    def message(f, a, d):
        if a == 0:
            if f in FINAL:
                src, dst = F.at[f - F0I, 0, pl.ds(0, n1)], F.at[f - F0I, n0, pl.ds(0, n1)]
            elif f in (NLI, CII):
                src, dst = {NLI: (NL, NZ), CII: (CI, CZ)}[f]
                src, dst = src.at[m0 - 1 if d else 0], dst.at[1 - d]
            else:
                ref, n = field(f)
                src = ref.at[n if d else 1, rows]
                dst = ref.at[0 if d else n + 1, rows]
        elif a == 1:
            count = m0 if f in COARSE else n0
            src, dst = SX.at[f, d, pl.ds(0, count)], RX.at[f, 1 - d, pl.ds(0, count)]
        else:
            src, dst = SY.at[f], RY.at[f, 1 - d]
        step = 1 if d else -1
        return pltpu.make_async_remote_copy(
            src_ref=src, dst_ref=dst, send_sem=send_sem.at[f, a, d], recv_sem=recv_sem.at[f, a, d],
            device_id={AXES[a]: lax.rem(me[a] + step + sizes[a], sizes[a])}, device_id_type=MESH,
        )

    def dirs(f):
        return (0,) if f in FINAL else (0, 1)

    def can_send(a, d):
        return me[a] < sizes[a] - 1 if d else me[a] > 0

    def send(f, a):
        for d in dirs(f):
            pl.when(can_send(a, d))(lambda f=f, a=a, d=d: message(f, a, d).start())

    def receive(f, a):
        for d in dirs(f):
            pl.when(can_send(a, 1 - d))(lambda f=f, a=a, d=d: message(f, a, d).wait_recv())

    def faces_x(f, get, count):
        for i in range(count):
            SX[f, 0, i : i + 1] = get(i, 0)
            if f not in FINAL:
                SX[f, 1, i : i + 1] = get(i, n1 - 1)

    def rows_x(f, ref):
        width = 2 if f in COARSE else 1
        for i in range(m0 if f in COARSE else n0):
            for w in range(width):
                ref[1 + i, PAD - 1 - w : PAD - w] = RX[f, 0, i : i + 1]
                ref[1 + i, PAD + n1 + w : PAD + n1 + w + 1] = RX[f, 1, i : i + 1]

    def line_message(offs, sign):
        z, x, y = [o * sign for o in offs]
        side = [0 if o > 0 else 1 for o in (z, x, y)]
        if not y:
            src, dst = LZX.at[1 - side[0], 1 - side[1]], RZX.at[side[0], side[1]]
        elif not x:
            plane = place(m0 - 1 if z > 0 else 0, 0, 4)[0]
            src, dst = SY.at[V1I, plane], RZY.at[side[0], side[2]]
        else:
            src, dst = LXY.at[1 - side[1]], RXY.at[side[1], side[2]]
        at = lines.index((z, x, y))
        return pltpu.make_async_remote_copy(
            src_ref=src, dst_ref=dst, send_sem=lsend.at[at], recv_sem=lrecv.at[at],
            device_id=device((z, x, y)), device_id_type=MESH,
        )

    def lines_send():
        for z in (0, 1):
            for x in (0, 1):
                c, r = (m0 - 1) * z, (n1 - 1) * x
                LZX[z, x] = V1[1 + c, PAD + r : PAD + r + 1]
        for x in (0, 1):
            for v in range(LXY.shape[1]):
                LXY[x, v] = SY[V1I, v, 7 * x : 7 * x + 1]
        for offs in lines:
            pl.when(exists(offs))(lambda offs=offs: line_message(offs, 1).start())

    def lines_receive():
        for offs in lines:
            pl.when(exists(offs))(lambda offs=offs: line_message(offs, -1).wait_recv())

    def align(low, high, p):
        return jnp.where(is_low[p], pltpu.roll(high, n2 - p // 2, 1), pltpu.roll(low, p // 2, 1))

    def halo_v2(ev, enl, eci):
        sh, kgroup = 2, [place(c, 0, 4) for c in (m0 - 1, 0)]
        col = [align(RZY[d, 0], RZY[d, 1], 4) for d in (0, 1)]
        for d, edge in ((0, 0), (1, m0 + 1)):
            v, kk = kgroup[d]
            near = NZ[d] + V1[1 if d == 0 else m0, rows]
            parts = [pltpu.roll(col[d], (n2 - 4 * (kk + g)) % n2, 1) for g in range(groups)]
            side = (lane_full < sh) | (lane_full >= n2 - sh)
            near = near + jnp.where(side, jnp.concatenate(parts, axis=0), 0.0)
            low = near[0:8] + jnp.where(row8 < sh, RZX[d, 0], 0.0)
            high = near[n1 - 8 : n1] + jnp.where(row8 >= 8 - sh, RZX[d, 1], 0.0)
            near = jnp.concatenate([low, near[8 : n1 - 8], high], axis=0)
            V2[edge, rows] = V1[edge, rows] - CZ[d] * near
        rowc = lax.broadcasted_iota(jnp.int32, (m0, n2), 0)
        lanec = lax.broadcasted_iota(jnp.int32, (m0, n2), 1)
        per = n2 // 4
        for d in (0, 1):
            near = RX[NLI, d, 0:m0] + SX[V1I, d, 0:m0]
            near = near + jnp.where(rowc == 0, RZX[0, d], 0.0) + jnp.where(rowc == m0 - 1, RZX[1, d], 0.0)
            for y in (0, 1):
                index = rowc * groups + (groups - 1 if d == 0 else 0)
                at = lax.rem(4 * lax.rem(index, per) + (n2 - 1 if y == 0 else 0), n2)
                got = jnp.zeros((m0, n2), jnp.float32)
                for v in range(RXY.shape[2]):
                    here = (lanec == at) & (index >= v * per) & (index < (v + 1) * per)
                    got = got + jnp.where(here, RXY[d, y, v], 0.0)
                got = jnp.sum(got, axis=1, keepdims=True)
                near = near + jnp.where((lanec < sh) if y == 0 else (lanec >= n2 - sh), got, 0.0)
            RX[V2I, d, 0:m0] = RX[V1I, d, 0:m0] - RX[CII, d, 0:m0] * near
        ws = []
        for v in range(len(ev)):
            near = enl[v] + SY[V1I, v]
            for d, c in ((0, 0), (1, m0 - 1)):
                into, k0 = place(c, 0, 4)
                if into == v:
                    shift = (4 * (k0 - kgroup[d][1])) % n2
                    moved = pltpu.roll(col[d], shift, 1) if shift else col[d]
                    near = near + jnp.where((keys[4] >= k0) & (keys[4] < k0 + groups), moved, 0.0)
            for d in (0, 1):
                line = align(
                    jnp.broadcast_to(RXY[d, 0, v], (8, n2)), jnp.broadcast_to(RXY[d, 1, v], (8, n2)), 4
                )
                jump = 4 * (groups - 1)
                line = pltpu.roll(line, n2 - jump if d == 0 else jump, 1)
                here = lax.rem(keys[4], groups) == (0 if d == 0 else groups - 1)
                here = here & ((row8 < sh) if d == 0 else (row8 >= 8 - sh))
                near = near + jnp.where(here, line, 0.0)
            ws.append(ev[v] - eci[v] * near)
        return ws

    def exchange(f, p):
        ref, count = field(f)
        send(f, 0)
        faces_x(f, lambda i, r: ref[1 + i, PAD + r : PAD + r + 1], count)
        send(f, 1)
        pack(f, lambda i: ref[1 + i, rows], count, p)
        send(f, 2)

    def one(f, a):
        ref, count = field(f)
        if a == 1:
            faces_x(f, lambda i, r: ref[1 + i, PAD + r : PAD + r + 1], count)
        if a == 2:
            pack(f, lambda i: ref[1 + i, rows], count, 2)
        send(f, a)

    def spread_faces(f, ref):
        send(f, 0)
        faces_x(f, lambda c, r: ref[c, r : r + 1], m0)
        send(f, 1)
        pack(f, lambda c: ref[c], m0, 4)
        send(f, 2)

    for pos, (k, a) in enumerate(((1, 1), (2, 2), (0, 0))):
        loads[2 * pos].wait()
        loads[2 * pos + 1].wait()
        for i in range(n0):
            inv = 1.0 / D[k, i]
            D[k, i] = inv
            S[k, 1 + i, rows] = R[k, i] * inv
        if pos == 0:
            pl.semaphore_wait(barrier, total)
        one(k, a)
    for f, a in ((0, 1), (2, 1), (1, 0), (2, 0), (0, 2), (1, 2)):
        one(f, a)

    loads[6].wait()
    for i in range(n0):
        NI[i] = 1.0 / (6.0 + NI[i])
    loads[7].wait()
    spread_rows = (
        lax.broadcasted_iota(jnp.int32, (n1, m1), 0) // 2 == lax.broadcasted_iota(jnp.int32, (n1, m1), 1)
    ).astype(jnp.float32)
    spread_cols = (
        lax.broadcasted_iota(jnp.int32, (m2, n2), 1) // 2 == lax.broadcasted_iota(jnp.int32, (m2, n2), 0)
    ).astype(jnp.float32)
    exact = functools.partial(
        jnp.dot, precision=lax.Precision.HIGHEST, preferred_element_type=jnp.float32
    )
    for i in range(m0):
        CI[i] = exact(spread_rows, exact(1.0 / (6.0 + CS[i]), spread_cols))
    spread_faces(CII, CI)

    for i in range(n0):
        x1, x2 = S[1, 1 + i, rows], S[2, 1 + i, rows]
        rhs = jnp.where(row_full >= 1, S[1, 1 + i, pl.ds(PAD - 1, n1)], 0.0) - x1
        rhs = rhs + (jnp.where(lane_full >= 1, pltpu.roll(x2, 1, 1), 0.0) - x2)
        rhs = rhs - S[0, 1 + i, rows]
        if i > 0:
            rhs = rhs + S[0, i, rows]
        F[0, i, 0:n1] = rhs
    receive(1, 1)
    receive(0, 0)
    receive(2, 2)
    ws = edges(2, 2)
    for i in range(n0):
        rhs = F[0, i, 0:n1] + jnp.where(lane_full < 1, halo(ws, i, 2), 0.0)
        if i == 0:
            rhs = rhs + S[0, 0, rows]
        first = rhs[0:8] + jnp.where(row8 < 1, RX[1, 0, i : i + 1], 0.0)
        FG[1 + i, rows] = jnp.concatenate([first, rhs[8:]], axis=0) * NI[i]
    exchange(FGI, 2)

    def smooth(k):
        for a in range(3):
            if (k, a) not in ((1, 1), (0, 0), (2, 2)):
                receive(k, a)
        rows_x(k, S.at[k])
        w = arrived(k, 2)
        for i in range(n0):
            x = S[k, 1 + i, rows]
            near = S[k, i, rows] + S[k, i + 2, rows] + inplane(S.at[k, 1 + i], x, halo(w, i, 2), 1)
            OB[k, i] = x + near * D[k, i]

    for i in range(n0):
        F[0, i, 0:n1] = local_near(FG, i, n0, 1)
    smooth(0)
    smooth(1)

    for a in range(3):
        receive(FGI, a)
    ws = edges(FGI, 2)
    for c in range(m0):
        t = None
        for i in (2 * c, 2 * c + 1):
            near = outer_near(F[0, i, 0:n1], FG, FGI, ws, i, n0, 2)
            F[0, i, 0:n1] = near
            t = near if t is None else t + near
        t = t + jnp.where(lane_full % 2 == 0, pltpu.roll(t, n2 - 1, 1), pltpu.roll(t, 1, 1))
        T[c, rows] = t
        t = t + jnp.where(row_full % 2 == 0, T[c, pl.ds(PAD + 1, n1)], T[c, pl.ds(PAD - 1, n1)])
        CR[c] = t
        V1[1 + c, rows] = t * CI[c]
    exchange(V1I, 4)
    lines_send()
    for c in range(m0):
        NL[c] = local_near(V1, c, m0, 2)
    spread_faces(NLI, NL)

    def faces_f(j):
        f = F0I + j
        send(f, 0)
        faces_x(f, lambda i, r: F[j, i, r : r + 1], n0)
        send(f, 1)
        pack(f, lambda i: F[j, i, 0:n1], n0, 2)
        send(f, 2)

    for i in range(n0):
        F[0, i, 0:n1] = FG[1 + i, rows] + F[0, i, 0:n1] * NI[i]
    faces_f(0)
    smooth(2)

    for f in (CII, V1I, NLI):
        for a in range(3):
            receive(f, a)
    ws = edges(V1I, 4)
    for c in range(m0):
        near = outer_near(NL[c], V1, V1I, ws, c, m0, 4)
        A1[c] = CR[c] - near
        V2[1 + c, rows] = V1[1 + c, rows] - near * CI[c]
    faces_x(V2I, lambda c, r: V2[1 + c, PAD + r : PAD + r + 1], m0)
    pack(V2I, lambda c: V2[1 + c, rows], m0, 4)
    lines_receive()
    w2 = halo_v2(ws, edges(NLI, 4), edges(CII, 4))

    def fold(x):
        acc = x[0:8]
        for g in range(1, groups):
            acc = acc + x[8 * g : 8 * g + 8]
        return acc

    def spread_near(j, V, w):
        for c in range(m0):
            x = V[1 + c, rows]
            near = x + inplane_aligned(V.at[1 + c], x, halo(w, c, 4), 1)
            F[j, 2 * c, 0:n1] = (near + V[c, rows]) * NI[2 * c]
            F[j, 2 * c + 1, 0:n1] = (near + V[c + 2, rows]) * NI[2 * c + 1]
        faces_f(j)

    sums = [jnp.zeros((8, n2), jnp.float32) for _ in range(5)]
    for c in range(m0):
        v1, v2, a1, cr = V1[1 + c, rows], V2[1 + c, rows], A1[c], CR[c]
        sums[0] = sums[0] + fold(v1 * cr)
        sums[1] = sums[1] + fold(v2 * cr)
        sums[2] = sums[2] + fold(v1 * a1)
        sums[3] = sums[3] + fold(v2 * a1)
        sums[4] = sums[4] + fold(v2 * (a1 - local_near(V2, c, m0, 2)))
    outer = fold(V2[1, rows] * V2[0, rows] + V2[m0, rows] * V2[m0 + 1, rows])
    for v, w in enumerate(w2):
        outer = outer + SY[V2I, v] * w
    rim = SX[V2I, 0, 0:m0] * RX[V2I, 0, 0:m0] + SX[V2I, 1, 0:m0] * RX[V2I, 1, 0:m0]
    sums[4] = sums[4] - outer
    rim = 2.0 * jnp.sum(rim, axis=0, keepdims=True)
    sums[4] = sums[4] - jnp.where(row8 == 0, rim, 0.0)
    lane1 = lax.broadcasted_iota(jnp.int32, (1, n2), 1)
    part = jnp.zeros((1, n2), jnp.float32)
    for q, s in enumerate(sums):
        part = jnp.where(lane1 == q, jnp.sum(jnp.sum(s, axis=0, keepdims=True), axis=1, keepdims=True), part)

    def slot(axes, at):
        index = 0
        for a in axes:
            index = index * sizes[a] + at(a)
        return index

    def sum_message(p, offs, sign):
        axes, slots = phases[p], slots_of[p]
        other = partner(axes, offs, sign)
        index = slot(axes, (lambda a: me[a]) if sign > 0 else (lambda a: other[AXES[a]]))
        sem = p * slots_of[0].shape[0] + slot(axes, lambda a: offs[axes.index(a)])
        return pltpu.make_async_remote_copy(
            src_ref=slots.at[index], dst_ref=slots.at[index], send_sem=psend.at[sem], recv_sem=precv.at[sem],
            device_id=other, device_id_type=MESH,
        )

    def sum_start(p, value):
        slots_of[p][slot(phases[p], lambda a: me[a])] = value
        for offs in offsets(phases[p]):
            sum_message(p, offs, 1).start()

    def sum_end(p):
        for offs in offsets(phases[p]):
            sum_message(p, offs, -1).wait_recv()
        terms = [slots_of[p][d] for d in range(slots_of[p].shape[0])]
        while len(terms) > 1:
            terms = [functools.reduce(lambda x, y: x + y, terms[t : t + 2]) for t in range(0, len(terms), 2)]
        return terms[0]

    sum_start(0, part)
    rows_x(V2I, V2)
    spread_near(2, V2, w2)
    rows_x(V1I, V1)
    spread_near(1, V1, ws)
    for j, G in enumerate((OB, G1, G2)):
        for a in range(3):
            receive(F0I + j, a)
        for i in range(n0):
            F[j, i, n1 : n1 + 1] = RX[F0I + j, 1, i : i + 1]
        wf = [RY[F0I + j, 1, v] for v in range(RY.shape[2])]
        for i in range(n0):
            x = F[j, i, 0:n1]
            grads = (F[j, i + 1, 0:n1] - x, F[j, i, 1 : n1 + 1] - x, from_high(x, halo(wf, i, 2)) - x)
            for k in range(3):
                G[k, i] = G[k, i] + grads[k] if j == 0 else grads[k]

    part = sum_end(0)
    for p in range(1, len(phases)):
        sum_start(p, part)
        part = sum_end(p)
    gone, gtwo, hone, hmix, htwo = [
        jnp.sum(jnp.where(lane1 == q, part, 0.0), axis=1, keepdims=True) for q in range(5)
    ]
    two = (gtwo - hmix * gone / hone) / (htwo - hmix * hmix / hone)
    oneco = (gone - hmix * two) / hone
    CO[0:1] = jnp.broadcast_to(oneco, (1, n2))
    CO[1:2] = jnp.broadcast_to(two, (1, n2))

    for p in range(len(phases)):
        for offs in offsets(phases[p]):
            sum_message(p, offs, 1).wait_send()
    for offs in lines:
        pl.when(exists(offs))(lambda offs=offs: line_message(offs, 1).wait_send())
    for a in range(3):
        for d in (0, 1):
            def drain(a=a, d=d):
                for f in range(FIELDS):
                    if f != V2I and d in dirs(f):
                        message(f, a, d).wait_send()
            pl.when(can_send(a, d))(drain)


def combine(parts, OB, G1, G2, CO, out, W, sem):
    _, n0, n1, n2 = OB.shape
    one = jnp.broadcast_to(CO[0:1], (n1, n2))
    two = jnp.broadcast_to(CO[1:2], (n1, n2))
    step = n0 // parts
    copies = []
    for k in range(3):
        for h in range(parts):
            for i in range(h * step, (h + 1) * step):
                W[k, i] = OB[k, i] + one * G1[k, i] + two * G2[k, i]
            planes = pl.ds(h * step, step)
            copies.append(pltpu.make_async_copy(W.at[k, planes], out.at[k, planes], sem.at[k * parts + h]))
            copies[-1].start()
    for c in copies:
        c.wait()


def solution(mesh):
    sizes = tuple(mesh.shape[a] for a in AXES)

    def local(residual, edge_diag, node_shift, coarse_shift):
        n0, n1, n2 = node_shift.shape
        m0, m1, m2 = coarse_shift.shape
        vecs = max(-(-(n0 * (n1 // 8)) // (n2 // 2)), -(-(m0 * (n1 // 8)) // (n2 // 4)))
        f32 = jnp.float32
        counts = [math.prod(sizes[a] for a in axes) for axes in phases_of(sizes)]
        V = lambda *s: pltpu.VMEM(s, f32)
        scratch = [
            V(3, n0, n1, n2), V(3, n0, n1, n2), V(n0, n1, n2), V(m0, m1, m2),
            V(3, n0 + 2, n1 + 2 * PAD, n2), V(n0 + 2, n1 + 2 * PAD, n2),
            V(m0, n1, n2), V(m0, n1, n2), V(m0, n1, n2), V(m0, n1, n2), V(m0, n1 + 2 * PAD, n2),
            V(m0 + 2, n1 + 2 * PAD, n2), V(m0 + 2, n1 + 2 * PAD, n2),
            V(3, n0 + 1, n1 + PAD, n2),
            V(FIELDS, 2, n0, n2), V(FIELDS, 2, n0, n2), V(FIELDS, vecs, 8, n2), V(FIELDS, 2, vecs, 8, n2),
            V(2, n1, n2), V(2, n1, n2), V(2, 2, 1, n2), V(2, vecs, 1, n2),
            V(2, 2, 1, n2), V(2, 2, 8, n2), V(2, 2, vecs, 1, n2),
            *[V(c, 1, n2) for c in counts],
        ]
        sems = [pltpu.SemaphoreType.DMA(s) for s in ((8,), *[(FIELDS, 3, 2)] * 2, *[(sum(counts),)] * 2, (12,), (12,))]

        def scoped(*refs):
            plain, slots_of = refs[: -len(counts)], refs[-len(counts) :]
            pl.run_scoped(functools.partial(kernel, sizes, *plain, slots_of), *sems)

        field = pltpu.VMEM(residual.shape, f32)
        limit = 67_043_328 - 12 * math.prod(residual.shape) - 2**18
        fields = pl.pallas_call(
            scoped,
            out_shape=[field, field, field, pltpu.VMEM((8, n2), f32)],
            in_specs=[pl.BlockSpec(memory_space=pltpu.HBM)] * 4,
            out_specs=[pl.BlockSpec(memory_space=pltpu.VMEM)] * 4,
            scratch_shapes=scratch,
            compiler_params=pltpu.CompilerParams(collective_id=0, has_side_effects=True, vmem_limit_bytes=limit),
        )(residual, edge_diag, node_shift, coarse_shift)
        parts = 2 if n0 % 2 == 0 else 1
        return pl.pallas_call(
            functools.partial(combine, parts),
            out_shape=jax.ShapeDtypeStruct(residual.shape, f32),
            in_specs=[pl.BlockSpec(memory_space=pltpu.VMEM)] * 4,
            out_specs=pl.BlockSpec(memory_space=pltpu.HBM),
            scratch_shapes=[field, pltpu.SemaphoreType.DMA((3 * parts,))],
            compiler_params=pltpu.CompilerParams(vmem_limit_bytes=8 * math.prod(residual.shape)),
        )(*fields)

    placed = (
        P(None, "gz", "gx", "gy"),
        P(None, "gz", "gx", "gy"),
        P("gz", "gx", "gy"),
        P("gz", "gx", "gy"),
    )
    return jax.shard_map(
        local, mesh=mesh, in_specs=placed, out_specs=P(None, "gz", "gx", "gy"), check_vma=False
    )
```

```python
import functools
import itertools
import math

import jax
import jax.numpy as jnp
from jax import lax
from jax.experimental import pallas as pl
from jax.experimental.pallas import tpu as pltpu
from jax.sharding import PartitionSpec as P

MESH = pl.DeviceIdType.MESH
AXES = ("gz", "gx", "gy")
FGI, V1I, V2I, F0I, NLI, CII = 3, 4, 5, 6, 9, 10
FIELDS = 11
FINAL = (F0I, F0I + 1, F0I + 2)
COARSE = (V1I, V2I, NLI, CII)
PAD = 8
FEW = 32


def phases_of(sizes):
    return ((0, 1, 2),) if math.prod(sizes) <= FEW else ((1, 2), (0,))


def greeted(sizes, rounds):
    near = set(itertools.product((-1, 0, 1), repeat=3))
    known = set(near)
    for moves in rounds:
        known |= {tuple(p + q for p, q in zip(k, m)) for k in known for m in moves}
    needed = set()
    for axes in phases_of(sizes):
        spans = [range(1 - sizes[a], sizes[a]) if a in axes else (0,) for a in range(3)]
        needed |= set(itertools.product(*spans))
    every = near | (needed - known)
    return sorted(o for o in every if any(o) and all(abs(p) < n for p, n in zip(o, sizes)))


def kernel(
    sizes,
    res, dia, shf, csh, OB, G1, G2, CO, MZ, MX, MY,
    R, D, NI, CS, S, FG, CI, CR, A1, NL, T, V1, V2, F,
    SX, RX, SY, RY, NZ, CZ, LZX, LXY, RZX, RZY, RXY,
    slots_of,
    in_sem, send_sem, recv_sem, psend, precv, lsend, lrecv,
):
    phases = phases_of(sizes)
    n0, n1, n2 = NI.shape
    m0, m1, m2 = CS.shape
    groups = n1 // 8
    me = [lax.axis_index(a) for a in AXES]
    rows = pl.ds(PAD, n1)

    def offsets(axes):
        every = itertools.product(*[range(sizes[a]) for a in axes])
        return [offs for offs in every if any(offs)]

    def partner(axes, offs, sign):
        return {
            AXES[a]: lax.rem(me[a] + (o if sign > 0 else sizes[a] - o), sizes[a]) for a, o in zip(axes, offs)
        }

    loads = []
    for k in (1, 2, 0):
        for src, dst in ((res, R), (dia, D)):
            loads.append(pltpu.make_async_copy(src.at[k], dst.at[k], in_sem.at[len(loads)]))
    loads.append(pltpu.make_async_copy(shf, NI, in_sem.at[6]))
    loads.append(pltpu.make_async_copy(csh, CS, in_sem.at[7]))
    for c in loads:
        c.start()

    zplane = jnp.zeros((n1, n2), jnp.float32)
    for k in range(3):
        S[k, 0, rows] = zplane
        S[k, n0 + 1, rows] = zplane
        F[k, n0, 0:n1] = zplane
        for i in range(n0):
            F[k, i, n1 : n1 + 1] = jnp.zeros((1, n2), jnp.float32)
    FG[0, rows] = zplane
    FG[n0 + 1, rows] = zplane
    for V in (V1, V2):
        V[0, rows] = zplane
        V[m0 + 1, rows] = zplane
    for buf in (RX, RY, NZ, CZ, RZX, RZY, RXY):
        buf[...] = jnp.zeros(buf.shape, jnp.float32)
    barrier = pltpu.get_barrier_semaphore()
    faces = [offs for offs in itertools.product((-1, 0, 1), repeat=3) if sum(map(abs, offs)) == 1]
    lines = [offs for offs in itertools.product((-1, 0, 1), repeat=3) if sum(map(abs, offs)) == 2]

    def exists(offs):
        inside = [(me[a] + o >= 0) & (me[a] + o < sizes[a]) for a, o in enumerate(offs) if o]
        return functools.reduce(jnp.logical_and, inside)

    def device(offs):
        return {AXES[a]: me[a] + o for a, o in enumerate(offs) if o}

    total = jnp.int32(0)
    for offs in greeted(sizes, (faces, faces, faces + lines)):
        there = exists(offs)
        pl.when(there)(
            lambda offs=offs: pl.semaphore_signal(
                barrier, inc=1, device_id=device(offs), device_id_type=MESH
            )
        )
        total = total + there.astype(jnp.int32)

    lane = lax.broadcasted_iota(jnp.int32, (8, n2), 1)
    lane_full = lax.broadcasted_iota(jnp.int32, (n1, n2), 1)
    row_full = lax.broadcasted_iota(jnp.int32, (n1, n2), 0)
    row8 = lax.broadcasted_iota(jnp.int32, (8, n2), 0)
    keys = {p: ((lane + p // 2) // p) % (n2 // p) for p in (2, 4)}
    is_low = {p: (lane % p) >= p // 2 for p in (2, 4)}

    def place(i, g, p):
        k = i * groups + g
        per = n2 // p
        return k // per, k % per

    def pack(f, plane, count, p):
        accs = [jnp.zeros((8, n2), jnp.float32) for _ in range(place(count - 1, groups - 1, p)[0] + 1)]
        for i in range(count):
            x = plane(i)
            for g in range(groups):
                v, kk = place(i, g, p)
                part = x[8 * g : 8 * g + 8]
                if kk:
                    part = pltpu.roll(part, p * kk, 1)
                accs[v] = jnp.where(keys[p] == kk, part, accs[v])
        for v, acc in enumerate(accs):
            SY[f, v] = acc

    def halo(ws, i, p):
        parts = []
        for g in range(groups):
            v, kk = place(i, g, p)
            parts.append(pltpu.roll(ws[v], n2 - p * kk, 1) if kk else ws[v])
        return jnp.concatenate(parts, axis=0)

    def inplane(ref, x, h, sh):
        near = ref[pl.ds(PAD - sh, n1)] + ref[pl.ds(PAD + sh, n1)]
        near = near + jnp.where(lane_full < sh, h, pltpu.roll(x, sh, 1))
        return near + jnp.where(lane_full >= n2 - sh, h, pltpu.roll(x, n2 - sh, 1))

    def local_near(ref, i, n, sh):
        x = ref[1 + i, rows]
        near = jnp.where(row_full >= sh, ref[1 + i, pl.ds(PAD - sh, n1)], 0.0)
        near = near + jnp.where(row_full < n1 - sh, ref[1 + i, pl.ds(PAD + sh, n1)], 0.0)
        near = near + jnp.where(lane_full >= sh, pltpu.roll(x, sh, 1), 0.0)
        near = near + jnp.where(lane_full < n2 - sh, pltpu.roll(x, n2 - sh, 1), 0.0)
        if i > 0:
            near = near + ref[i, rows]
        if i < n - 1:
            near = near + ref[i + 2, rows]
        return near

    def edges(f, p):
        sh = p // 2
        return [
            jnp.where(is_low[p], pltpu.roll(RY[f, 1, v], n2 - sh, 1), pltpu.roll(RY[f, 0, v], sh, 1))
            for v in range(RY.shape[2])
        ]

    def outer_near(near, ref, f, ws, i, n, p):
        sh = p // 2
        if i == 0:
            near = near + ref[0, rows]
        if i == n - 1:
            near = near + ref[n + 1, rows]
        side = (lane_full < sh) | (lane_full >= n2 - sh)
        near = near + jnp.where(side, halo(ws, i, p), 0.0)
        low = near[0:8] + jnp.where(row8 < sh, RX[f, 0, i : i + 1], 0.0)
        high = near[n1 - 8 : n1] + jnp.where(row8 >= 8 - sh, RX[f, 1, i : i + 1], 0.0)
        return jnp.concatenate([low, near[8 : n1 - 8], high], axis=0)

    def field(f):
        if f < 3:
            return S.at[f], n0
        return {FGI: (FG, n0), V1I: (V1, m0)}[f]

    def message(f, a, d):
        if a == 0:
            if f in FINAL:
                src, dst = F.at[f - F0I, 0, pl.ds(0, n1)], F.at[f - F0I, n0, pl.ds(0, n1)]
            elif f in (NLI, CII):
                src, dst = {NLI: (NL, NZ), CII: (CI, CZ)}[f]
                src, dst = src.at[m0 - 1 if d else 0], dst.at[1 - d]
            else:
                ref, n = field(f)
                src = ref.at[n if d else 1, rows]
                dst = ref.at[0 if d else n + 1, rows]
        elif a == 1:
            count = m0 if f in COARSE else n0
            src, dst = SX.at[f, d, pl.ds(0, count)], RX.at[f, 1 - d, pl.ds(0, count)]
        else:
            src, dst = SY.at[f], RY.at[f, 1 - d]
        step = 1 if d else -1
        return pltpu.make_async_remote_copy(
            src_ref=src, dst_ref=dst, send_sem=send_sem.at[f, a, d], recv_sem=recv_sem.at[f, a, d],
            device_id={AXES[a]: lax.rem(me[a] + step + sizes[a], sizes[a])}, device_id_type=MESH,
        )

    def dirs(f):
        return (0,) if f in FINAL else (0, 1)

    def can_send(a, d):
        return me[a] < sizes[a] - 1 if d else me[a] > 0

    def send(f, a):
        for d in dirs(f):
            pl.when(can_send(a, d))(lambda f=f, a=a, d=d: message(f, a, d).start())

    def receive(f, a):
        for d in dirs(f):
            pl.when(can_send(a, 1 - d))(lambda f=f, a=a, d=d: message(f, a, d).wait_recv())

    def faces_x(f, get, count):
        for i in range(count):
            SX[f, 0, i : i + 1] = get(i, 0)
            if f not in FINAL:
                SX[f, 1, i : i + 1] = get(i, n1 - 1)

    def rows_x(f, ref):
        width = 2 if f in COARSE else 1
        for i in range(m0 if f in COARSE else n0):
            for w in range(width):
                ref[1 + i, PAD - 1 - w : PAD - w] = RX[f, 0, i : i + 1]
                ref[1 + i, PAD + n1 + w : PAD + n1 + w + 1] = RX[f, 1, i : i + 1]

    def line_message(offs, sign):
        z, x, y = [o * sign for o in offs]
        side = [0 if o > 0 else 1 for o in (z, x, y)]
        if not y:
            src, dst = LZX.at[1 - side[0], 1 - side[1]], RZX.at[side[0], side[1]]
        elif not x:
            plane = place(m0 - 1 if z > 0 else 0, 0, 4)[0]
            src, dst = SY.at[V1I, plane], RZY.at[side[0], side[2]]
        else:
            src, dst = LXY.at[1 - side[1]], RXY.at[side[1], side[2]]
        at = lines.index((z, x, y))
        return pltpu.make_async_remote_copy(
            src_ref=src, dst_ref=dst, send_sem=lsend.at[at], recv_sem=lrecv.at[at],
            device_id=device((z, x, y)), device_id_type=MESH,
        )

    def lines_send():
        for z in (0, 1):
            for x in (0, 1):
                c, r = (m0 - 1) * z, (n1 - 1) * x
                LZX[z, x] = V1[1 + c, PAD + r : PAD + r + 1]
        for x in (0, 1):
            for v in range(LXY.shape[1]):
                LXY[x, v] = SY[V1I, v, 7 * x : 7 * x + 1]
        for offs in lines:
            pl.when(exists(offs))(lambda offs=offs: line_message(offs, 1).start())

    def lines_receive():
        for offs in lines:
            pl.when(exists(offs))(lambda offs=offs: line_message(offs, -1).wait_recv())

    def align(low, high, p):
        return jnp.where(is_low[p], pltpu.roll(high, n2 - p // 2, 1), pltpu.roll(low, p // 2, 1))

    def halo_v2(ev, enl, eci):
        sh, kgroup = 2, [place(c, 0, 4) for c in (m0 - 1, 0)]
        col = [align(RZY[d, 0], RZY[d, 1], 4) for d in (0, 1)]
        for d, edge in ((0, 0), (1, m0 + 1)):
            v, kk = kgroup[d]
            near = NZ[d] + V1[1 if d == 0 else m0, rows]
            parts = [pltpu.roll(col[d], (n2 - 4 * (kk + g)) % n2, 1) for g in range(groups)]
            side = (lane_full < sh) | (lane_full >= n2 - sh)
            near = near + jnp.where(side, jnp.concatenate(parts, axis=0), 0.0)
            low = near[0:8] + jnp.where(row8 < sh, RZX[d, 0], 0.0)
            high = near[n1 - 8 : n1] + jnp.where(row8 >= 8 - sh, RZX[d, 1], 0.0)
            near = jnp.concatenate([low, near[8 : n1 - 8], high], axis=0)
            V2[edge, rows] = V1[edge, rows] - CZ[d] * near
        rowc = lax.broadcasted_iota(jnp.int32, (m0, n2), 0)
        lanec = lax.broadcasted_iota(jnp.int32, (m0, n2), 1)
        per = n2 // 4
        for d in (0, 1):
            near = RX[NLI, d, 0:m0] + SX[V1I, d, 0:m0]
            near = near + jnp.where(rowc == 0, RZX[0, d], 0.0) + jnp.where(rowc == m0 - 1, RZX[1, d], 0.0)
            for y in (0, 1):
                index = rowc * groups + (groups - 1 if d == 0 else 0)
                at = lax.rem(4 * lax.rem(index, per) + (n2 - 1 if y == 0 else 0), n2)
                got = jnp.zeros((m0, n2), jnp.float32)
                for v in range(RXY.shape[2]):
                    here = (lanec == at) & (index >= v * per) & (index < (v + 1) * per)
                    got = got + jnp.where(here, RXY[d, y, v], 0.0)
                got = jnp.sum(got, axis=1, keepdims=True)
                near = near + jnp.where((lanec < sh) if y == 0 else (lanec >= n2 - sh), got, 0.0)
            RX[V2I, d, 0:m0] = RX[V1I, d, 0:m0] - RX[CII, d, 0:m0] * near
        ws = []
        for v in range(len(ev)):
            near = enl[v] + SY[V1I, v]
            for d, c in ((0, 0), (1, m0 - 1)):
                into, k0 = place(c, 0, 4)
                if into == v:
                    shift = (4 * (k0 - kgroup[d][1])) % n2
                    moved = pltpu.roll(col[d], shift, 1) if shift else col[d]
                    near = near + jnp.where((keys[4] >= k0) & (keys[4] < k0 + groups), moved, 0.0)
            for d in (0, 1):
                line = align(
                    jnp.broadcast_to(RXY[d, 0, v], (8, n2)), jnp.broadcast_to(RXY[d, 1, v], (8, n2)), 4
                )
                jump = 4 * (groups - 1)
                line = pltpu.roll(line, n2 - jump if d == 0 else jump, 1)
                here = lax.rem(keys[4], groups) == (0 if d == 0 else groups - 1)
                here = here & ((row8 < sh) if d == 0 else (row8 >= 8 - sh))
                near = near + jnp.where(here, line, 0.0)
            ws.append(ev[v] - eci[v] * near)
        return ws

    def exchange(f, p):
        ref, count = field(f)
        send(f, 0)
        faces_x(f, lambda i, r: ref[1 + i, PAD + r : PAD + r + 1], count)
        send(f, 1)
        pack(f, lambda i: ref[1 + i, rows], count, p)
        send(f, 2)

    def one(f, a):
        ref, count = field(f)
        if a == 1:
            faces_x(f, lambda i, r: ref[1 + i, PAD + r : PAD + r + 1], count)
        if a == 2:
            pack(f, lambda i: ref[1 + i, rows], count, 2)
        send(f, a)

    def spread_faces(f, ref):
        send(f, 0)
        faces_x(f, lambda c, r: ref[c, r : r + 1], m0)
        send(f, 1)
        pack(f, lambda c: ref[c], m0, 4)
        send(f, 2)

    for pos, (k, a) in enumerate(((1, 1), (2, 2), (0, 0))):
        loads[2 * pos].wait()
        loads[2 * pos + 1].wait()
        for i in range(n0):
            inv = 1.0 / D[k, i]
            D[k, i] = inv
            S[k, 1 + i, rows] = R[k, i] * inv
        if pos == 0:
            pl.semaphore_wait(barrier, total)
        one(k, a)
    for f, a in ((0, 1), (2, 1), (1, 0), (2, 0), (0, 2), (1, 2)):
        one(f, a)

    loads[6].wait()
    for i in range(n0):
        NI[i] = 1.0 / (6.0 + NI[i])
    loads[7].wait()
    spread_rows = (
        lax.broadcasted_iota(jnp.int32, (n1, m1), 0) // 2 == lax.broadcasted_iota(jnp.int32, (n1, m1), 1)
    ).astype(jnp.float32)
    spread_cols = (
        lax.broadcasted_iota(jnp.int32, (m2, n2), 1) // 2 == lax.broadcasted_iota(jnp.int32, (m2, n2), 0)
    ).astype(jnp.float32)
    exact = functools.partial(
        jnp.dot, precision=lax.Precision.HIGHEST, preferred_element_type=jnp.float32
    )
    for i in range(m0):
        CI[i] = exact(spread_rows, exact(1.0 / (6.0 + CS[i]), spread_cols))
    spread_faces(CII, CI)

    for i in range(n0):
        x1, x2 = S[1, 1 + i, rows], S[2, 1 + i, rows]
        rhs = jnp.where(row_full >= 1, S[1, 1 + i, pl.ds(PAD - 1, n1)], 0.0) - x1
        rhs = rhs + (jnp.where(lane_full >= 1, pltpu.roll(x2, 1, 1), 0.0) - x2)
        rhs = rhs - S[0, 1 + i, rows]
        if i > 0:
            rhs = rhs + S[0, i, rows]
        F[0, i, 0:n1] = rhs
    receive(1, 1)
    receive(0, 0)
    receive(2, 2)
    ws = edges(2, 2)
    for i in range(n0):
        rhs = F[0, i, 0:n1] + jnp.where(lane_full < 1, halo(ws, i, 2), 0.0)
        if i == 0:
            rhs = rhs + S[0, 0, rows]
        first = rhs[0:8] + jnp.where(row8 < 1, RX[1, 0, i : i + 1], 0.0)
        FG[1 + i, rows] = jnp.concatenate([first, rhs[8:]], axis=0) * NI[i]
    def gradients(j, G):
        for i in range(n0):
            x = F[j, i, 0:n1]
            above = F[j, i + 1, 0:n1] - x if i < n0 - 1 else -x
            ahead = jnp.where(lane_full >= n2 - 1, 0.0, pltpu.roll(x, n2 - 1, 1)) - x
            for k, grad in enumerate((above, F[j, i, 1 : n1 + 1] - x, ahead)):
                G[k, i] = G[k, i] + grad if j == 0 else grad

    exchange(FGI, 2)

    def smooth(k):
        for a in range(3):
            if (k, a) not in ((1, 1), (0, 0), (2, 2)):
                receive(k, a)
        rows_x(k, S.at[k])
        w = edges(k, 2)
        for i in range(n0):
            x = S[k, 1 + i, rows]
            near = S[k, i, rows] + S[k, i + 2, rows] + inplane(S.at[k, 1 + i], x, halo(w, i, 2), 1)
            OB[k, i] = x + near * D[k, i]

    for i in range(n0):
        F[0, i, 0:n1] = local_near(FG, i, n0, 1)
    smooth(0)
    smooth(1)

    for a in range(3):
        receive(FGI, a)
    ws = edges(FGI, 2)
    for c in range(m0):
        t = None
        for i in (2 * c, 2 * c + 1):
            near = outer_near(F[0, i, 0:n1], FG, FGI, ws, i, n0, 2)
            F[0, i, 0:n1] = near
            t = near if t is None else t + near
        t = t + jnp.where(lane_full % 2 == 0, pltpu.roll(t, n2 - 1, 1), pltpu.roll(t, 1, 1))
        T[c, rows] = t
        t = t + jnp.where(row_full % 2 == 0, T[c, pl.ds(PAD + 1, n1)], T[c, pl.ds(PAD - 1, n1)])
        CR[c] = t
        V1[1 + c, rows] = t * CI[c]
    exchange(V1I, 4)
    lines_send()
    for c in range(m0):
        NL[c] = local_near(V1, c, m0, 2)
    spread_faces(NLI, NL)

    def faces_f(j):
        f = F0I + j
        send(f, 0)
        faces_x(f, lambda i, r: F[j, i, r : r + 1], n0)
        send(f, 1)
        pack(f, lambda i: F[j, i, 0:n1], n0, 2)
        send(f, 2)

    for i in range(n0):
        F[0, i, 0:n1] = FG[1 + i, rows] + F[0, i, 0:n1] * NI[i]
    faces_f(0)
    smooth(2)
    gradients(0, OB)

    for f in (CII, V1I, NLI):
        for a in range(3):
            receive(f, a)
    ws = edges(V1I, 4)
    for c in range(m0):
        near = outer_near(NL[c], V1, V1I, ws, c, m0, 4)
        A1[c] = CR[c] - near
        V2[1 + c, rows] = V1[1 + c, rows] - near * CI[c]
    faces_x(V2I, lambda c, r: V2[1 + c, PAD + r : PAD + r + 1], m0)
    pack(V2I, lambda c: V2[1 + c, rows], m0, 4)
    lines_receive()
    w2 = halo_v2(ws, edges(NLI, 4), edges(CII, 4))

    def fold(x):
        acc = x[0:8]
        for g in range(1, groups):
            acc = acc + x[8 * g : 8 * g + 8]
        return acc

    def spread_near(j, V, w):
        for c in range(m0):
            x = V[1 + c, rows]
            near = x + inplane(V.at[1 + c], x, halo(w, c, 4), 1)
            F[j, 2 * c, 0:n1] = (near + V[c, rows]) * NI[2 * c]
            F[j, 2 * c + 1, 0:n1] = (near + V[c + 2, rows]) * NI[2 * c + 1]
        faces_f(j)

    sums = [jnp.zeros((8, n2), jnp.float32) for _ in range(5)]
    for c in range(m0):
        v1, v2, a1, cr = V1[1 + c, rows], V2[1 + c, rows], A1[c], CR[c]
        sums[0] = sums[0] + fold(v1 * cr)
        sums[1] = sums[1] + fold(v2 * cr)
        sums[2] = sums[2] + fold(v1 * a1)
        sums[3] = sums[3] + fold(v2 * a1)
        sums[4] = sums[4] + fold(v2 * (a1 - local_near(V2, c, m0, 2)))
    outer = fold(V2[1, rows] * V2[0, rows] + V2[m0, rows] * V2[m0 + 1, rows])
    for v, w in enumerate(w2):
        outer = outer + SY[V2I, v] * w
    rim = SX[V2I, 0, 0:m0] * RX[V2I, 0, 0:m0] + SX[V2I, 1, 0:m0] * RX[V2I, 1, 0:m0]
    sums[4] = sums[4] - outer
    rim = 2.0 * jnp.sum(rim, axis=0, keepdims=True)
    sums[4] = sums[4] - jnp.where(row8 == 0, rim, 0.0)
    lane1 = lax.broadcasted_iota(jnp.int32, (1, n2), 1)
    part = jnp.zeros((1, n2), jnp.float32)
    for q, s in enumerate(sums):
        part = jnp.where(lane1 == q, jnp.sum(jnp.sum(s, axis=0, keepdims=True), axis=1, keepdims=True), part)

    def slot(axes, at):
        index = 0
        for a in axes:
            index = index * sizes[a] + at(a)
        return index

    def sum_message(p, offs, sign):
        axes, slots = phases[p], slots_of[p]
        other = partner(axes, offs, sign)
        index = slot(axes, (lambda a: me[a]) if sign > 0 else (lambda a: other[AXES[a]]))
        sem = p * slots_of[0].shape[0] + slot(axes, lambda a: offs[axes.index(a)])
        return pltpu.make_async_remote_copy(
            src_ref=slots.at[index], dst_ref=slots.at[index], send_sem=psend.at[sem], recv_sem=precv.at[sem],
            device_id=other, device_id_type=MESH,
        )

    def sum_start(p, value):
        slots_of[p][slot(phases[p], lambda a: me[a])] = value
        for offs in offsets(phases[p]):
            sum_message(p, offs, 1).start()

    def sum_end(p):
        for offs in offsets(phases[p]):
            sum_message(p, offs, -1).wait_recv()
        terms = [slots_of[p][d] for d in range(slots_of[p].shape[0])]
        while len(terms) > 1:
            terms = [functools.reduce(lambda x, y: x + y, terms[t : t + 2]) for t in range(0, len(terms), 2)]
        return terms[0]

    sum_start(0, part)
    rows_x(V2I, V2)
    spread_near(2, V2, w2)
    rows_x(V1I, V1)
    spread_near(1, V1, ws)
    gradients(1, G1)
    gradients(2, G2)

    part = sum_end(0)
    for p in range(1, len(phases)):
        sum_start(p, part)
        part = sum_end(p)
    gone, gtwo, hone, hmix, htwo = [
        jnp.sum(jnp.where(lane1 == q, part, 0.0), axis=1, keepdims=True) for q in range(5)
    ]
    two = (gtwo - hmix * gone / hone) / (htwo - hmix * hmix / hone)
    oneco = (gone - hmix * two) / hone
    CO[0:1] = jnp.broadcast_to(oneco, (1, n2))
    CO[1:2] = jnp.broadcast_to(two, (1, n2))
    for f in FINAL:
        for a in range(3):
            receive(f, a)

    def mix(get):
        a = get(0)
        return a + jnp.broadcast_to(oneco, a.shape) * get(1) + jnp.broadcast_to(two, a.shape) * get(2)

    MZ[...] = mix(lambda j: F[j, n0, 0:n1])
    MX[...] = mix(lambda j: RX[F0I + j, 1])
    for v in range(RY.shape[2]):
        MY[v] = pltpu.roll(mix(lambda j: RY[F0I + j, 1, v]), n2 - 1, 1)

    for p in range(len(phases)):
        for offs in offsets(phases[p]):
            sum_message(p, offs, 1).wait_send()
    for offs in lines:
        pl.when(exists(offs))(lambda offs=offs: line_message(offs, 1).wait_send())
    for a in range(3):
        for d in (0, 1):
            def drain(a=a, d=d):
                for f in range(FIELDS):
                    if f != V2I and d in dirs(f):
                        message(f, a, d).wait_send()
            pl.when(can_send(a, d))(drain)


def combine(parts, OB, G1, G2, CO, MZ, MX, MY, out, W, sem):
    _, n0, n1, n2 = OB.shape
    one = jnp.broadcast_to(CO[0:1], (n1, n2))
    two = jnp.broadcast_to(CO[1:2], (n1, n2))
    groups, per, step = n1 // 8, n2 // 2, n0 // parts
    row8 = lax.broadcasted_iota(jnp.int32, (8, n2), 0)
    lane_full = lax.broadcasted_iota(jnp.int32, (n1, n2), 1)

    def edge(k, i, x):
        if k == 0:
            return x + MZ[...] if i == n0 - 1 else x
        if k == 1:
            last = x[n1 - 8 : n1] + jnp.where(row8 == 7, MX[i : i + 1], 0.0)
            return jnp.concatenate([x[0 : n1 - 8], last], axis=0)
        ats = [divmod(i * groups + g, per) for g in range(groups)]
        parts = [pltpu.roll(MY[v], (n2 - 2 * kk) % n2, 1) for v, kk in ats]
        return x + jnp.where(lane_full >= n2 - 1, jnp.concatenate(parts, axis=0), 0.0)

    copies = []
    for k in range(3):
        for h in range(parts):
            for i in range(h * step, (h + 1) * step):
                W[k, i] = edge(k, i, OB[k, i] + one * G1[k, i] + two * G2[k, i])
            planes = pl.ds(h * step, step)
            copies.append(pltpu.make_async_copy(W.at[k, planes], out.at[k, planes], sem.at[k * parts + h]))
            copies[-1].start()
    for c in copies:
        c.wait()


def solution(mesh):
    sizes = tuple(mesh.shape[a] for a in AXES)

    def local(residual, edge_diag, node_shift, coarse_shift):
        n0, n1, n2 = node_shift.shape
        m0, m1, m2 = coarse_shift.shape
        vecs = max(-(-(n0 * (n1 // 8)) // (n2 // 2)), -(-(m0 * (n1 // 8)) // (n2 // 4)))
        f32 = jnp.float32
        counts = [math.prod(sizes[a] for a in axes) for axes in phases_of(sizes)]
        V = lambda *s: pltpu.VMEM(s, f32)
        scratch = [
            V(3, n0, n1, n2), V(3, n0, n1, n2), V(n0, n1, n2), V(m0, m1, m2),
            V(3, n0 + 2, n1 + 2 * PAD, n2), V(n0 + 2, n1 + 2 * PAD, n2),
            V(m0, n1, n2), V(m0, n1, n2), V(m0, n1, n2), V(m0, n1, n2), V(m0, n1 + 2 * PAD, n2),
            V(m0 + 2, n1 + 2 * PAD, n2), V(m0 + 2, n1 + 2 * PAD, n2),
            V(3, n0 + 1, n1 + PAD, n2),
            V(FIELDS, 2, n0, n2), V(FIELDS, 2, n0, n2), V(FIELDS, vecs, 8, n2), V(FIELDS, 2, vecs, 8, n2),
            V(2, n1, n2), V(2, n1, n2), V(2, 2, 1, n2), V(2, vecs, 1, n2),
            V(2, 2, 1, n2), V(2, 2, 8, n2), V(2, 2, vecs, 1, n2),
            *[V(c, 1, n2) for c in counts],
        ]
        sems = [pltpu.SemaphoreType.DMA(s) for s in ((8,), *[(FIELDS, 3, 2)] * 2, *[(sum(counts),)] * 2, (12,), (12,))]

        def scoped(*refs):
            plain, slots_of = refs[: -len(counts)], refs[-len(counts) :]
            pl.run_scoped(functools.partial(kernel, sizes, *plain, slots_of), *sems)

        field = pltpu.VMEM(residual.shape, f32)
        limit = 67_043_328 - 12 * math.prod(residual.shape) - 2**18
        fields = pl.pallas_call(
            scoped,
            out_shape=[field] * 3 + [pltpu.VMEM(s, f32) for s in ((8, n2), (n1, n2), (n0, n2), (vecs, 8, n2))],
            in_specs=[pl.BlockSpec(memory_space=pltpu.HBM)] * 4,
            out_specs=[pl.BlockSpec(memory_space=pltpu.VMEM)] * 7,
            scratch_shapes=scratch,
            compiler_params=pltpu.CompilerParams(collective_id=0, has_side_effects=True, vmem_limit_bytes=limit),
        )(residual, edge_diag, node_shift, coarse_shift)
        parts = 2 if n0 % 2 == 0 else 1
        return pl.pallas_call(
            functools.partial(combine, parts),
            out_shape=jax.ShapeDtypeStruct(residual.shape, f32),
            in_specs=[pl.BlockSpec(memory_space=pltpu.VMEM)] * 7,
            out_specs=pl.BlockSpec(memory_space=pltpu.HBM),
            scratch_shapes=[field, pltpu.SemaphoreType.DMA((3 * parts,))],
            compiler_params=pltpu.CompilerParams(vmem_limit_bytes=8 * math.prod(residual.shape)),
        )(*fields)

    placed = (
        P(None, "gz", "gx", "gy"),
        P(None, "gz", "gx", "gy"),
        P("gz", "gx", "gy"),
        P("gz", "gx", "gy"),
    )
    return jax.shard_map(
        local, mesh=mesh, in_specs=placed, out_specs=P(None, "gz", "gx", "gy"), check_vma=False
    )
```

```python
import functools
import itertools
import math

import jax
import jax.numpy as jnp
from jax import lax
from jax.experimental import pallas as pl
from jax.experimental.pallas import tpu as pltpu
from jax.sharding import PartitionSpec as P

MESH = pl.DeviceIdType.MESH
AXES = ("gz", "gx", "gy")
PI, V1I, V2I, F0I, NLI, CII, NII, FGI = 3, 4, 5, 6, 9, 10, 11, 12
FIELDS = 13
FINAL = (F0I, F0I + 1, F0I + 2)
COARSE = (V1I, V2I, NLI, CII)
LOCAL = (V2I, FGI)
CROSS = [(a, b, d) for a in range(3) for b in range(3) if a != b for d in (0, 1)]
PAD = 8
FEW = 32


def phases_of(sizes):
    return ((0, 1, 2),) if math.prod(sizes) <= FEW else ((1, 2), (0,))


def greeted(sizes, rounds):
    near = set(itertools.product(range(-1, 2), range(-2, 3), range(-2, 3)))
    known = set(near)
    for moves in rounds:
        known |= {tuple(p + q for p, q in zip(k, m)) for k in known for m in moves}
    needed = set()
    for axes in phases_of(sizes):
        spans = [range(1 - sizes[a], sizes[a]) if a in axes else (0,) for a in range(3)]
        needed |= set(itertools.product(*spans))
    every = near | (needed - known)
    return sorted(o for o in every if any(o) and all(abs(p) < n for p, n in zip(o, sizes)))


def kernel(
    sizes,
    res, dia, shf, csh, OB, G1, G2, CO, MZ, MX, MY,
    R, D, NI, CS, S, FG, CI, CR, A1, NL, T, V1, V2, F,
    SX, RX, SY, RY, NZ, CZ, LZX, LXY, RZX, RZY, RXY,
    P, PZ, NZI, LRZ, LRX, LY2, LY1, LP0, RRZ, RRX, RZ2, RZ0, RX2, RX1,
    slots_of,
    in_sem, send_sem, recv_sem, psend, precv, lsend, lrecv, csend, crecv,
):
    phases = phases_of(sizes)
    n0, n1, n2 = NI.shape
    m0, m1, m2 = CS.shape
    groups = n1 // 8
    me = [lax.axis_index(a) for a in AXES]
    rows = pl.ds(PAD, n1)

    def offsets(axes):
        every = itertools.product(*[range(sizes[a]) for a in axes])
        return [offs for offs in every if any(offs)]

    def partner(axes, offs, sign):
        return {
            AXES[a]: lax.rem(me[a] + (o if sign > 0 else sizes[a] - o), sizes[a]) for a, o in zip(axes, offs)
        }

    loads = [pltpu.make_async_copy(shf, NI, in_sem.at[0])]
    for k in (1, 2, 0):
        for src, dst in ((res, R), (dia, D)):
            loads.append(pltpu.make_async_copy(src.at[k], dst.at[k], in_sem.at[len(loads)]))
    loads.append(pltpu.make_async_copy(csh, CS, in_sem.at[7]))
    for c in loads:
        c.start()

    zplane = jnp.zeros((n1, n2), jnp.float32)
    for k in range(3):
        S[k, 0, rows] = zplane
        S[k, n0 + 1, rows] = zplane
        F[k, n0, 0:n1] = zplane
        for i in range(n0):
            F[k, i, n1 : n1 + 1] = jnp.zeros((1, n2), jnp.float32)
    for V in (V1, V2):
        V[0, rows] = zplane
        V[m0 + 1, rows] = zplane
    for buf in (RX, RY, NZ, CZ, RZX, RZY, RXY, PZ, NZI, RRZ, RRX, RZ2, RZ0, RX2, RX1):
        buf[...] = jnp.zeros(buf.shape, jnp.float32)
    barrier = pltpu.get_barrier_semaphore()
    faces = [offs for offs in itertools.product((-1, 0, 1), repeat=3) if sum(map(abs, offs)) == 1]
    lines = [offs for offs in itertools.product((-1, 0, 1), repeat=3) if sum(map(abs, offs)) == 2]

    def exists(offs):
        inside = [(me[a] + o >= 0) & (me[a] + o < sizes[a]) for a, o in enumerate(offs) if o]
        return functools.reduce(jnp.logical_and, inside)

    def device(offs):
        return {AXES[a]: me[a] + o for a, o in enumerate(offs) if o}

    total = jnp.int32(0)
    for offs in greeted(sizes, (faces + [m for m in lines if min(m) < 0], faces + lines)):
        there = exists(offs)
        pl.when(there)(
            lambda offs=offs: pl.semaphore_signal(
                barrier, inc=1, device_id=device(offs), device_id_type=MESH
            )
        )
        total = total + there.astype(jnp.int32)

    lane = lax.broadcasted_iota(jnp.int32, (8, n2), 1)
    lane_full = lax.broadcasted_iota(jnp.int32, (n1, n2), 1)
    row_full = lax.broadcasted_iota(jnp.int32, (n1, n2), 0)
    row8 = lax.broadcasted_iota(jnp.int32, (8, n2), 0)
    keys = {p: ((lane + p // 2) // p) % (n2 // p) for p in (2, 4)}
    is_low = {p: (lane % p) >= p // 2 for p in (2, 4)}

    def place(i, g, p):
        k = i * groups + g
        per = n2 // p
        return k // per, k % per

    def gather(blocks, p):
        accs = {}
        for (i, g), part in blocks:
            v, kk = place(i, g, p)
            if kk:
                part = pltpu.roll(part, p * kk, 1)
            accs[v] = jnp.where(keys[p] == kk, part, accs.get(v, 0.0))
        return accs

    def pack(f, plane, count, p):
        at = [(i, g) for i in range(count) for g in range(groups)]
        planes = [plane(i) for i in range(count)]
        accs = gather([((i, g), planes[i][8 * g : 8 * g + 8]) for i, g in at], p)
        for v, acc in accs.items():
            SY[f, v] = acc

    def halo(ws, i, p):
        parts = []
        for g in range(groups):
            v, kk = place(i, g, p)
            parts.append(pltpu.roll(ws[v], n2 - p * kk, 1) if kk else ws[v])
        return jnp.concatenate(parts, axis=0)

    def inplane(ref, x, h, sh):
        near = ref[pl.ds(PAD - sh, n1)] + ref[pl.ds(PAD + sh, n1)]
        near = near + jnp.where(lane_full < sh, h, pltpu.roll(x, sh, 1))
        return near + jnp.where(lane_full >= n2 - sh, h, pltpu.roll(x, n2 - sh, 1))

    def local_near(ref, i, n, sh):
        x = ref[1 + i, rows]
        near = jnp.where(row_full >= sh, ref[1 + i, pl.ds(PAD - sh, n1)], 0.0)
        near = near + jnp.where(row_full < n1 - sh, ref[1 + i, pl.ds(PAD + sh, n1)], 0.0)
        near = near + jnp.where(lane_full >= sh, pltpu.roll(x, sh, 1), 0.0)
        near = near + jnp.where(lane_full < n2 - sh, pltpu.roll(x, n2 - sh, 1), 0.0)
        if i > 0:
            near = near + ref[i, rows]
        if i < n - 1:
            near = near + ref[i + 2, rows]
        return near

    def edges(f, p):
        sh = p // 2
        return [
            jnp.where(is_low[p], pltpu.roll(RY[f, 1, v], n2 - sh, 1), pltpu.roll(RY[f, 0, v], sh, 1))
            for v in range(RY.shape[2])
        ]

    def outer_near(near, ref, f, ws, i, n, p):
        sh = p // 2
        if i == 0:
            near = near + ref[0, rows]
        if i == n - 1:
            near = near + ref[n + 1, rows]
        side = (lane_full < sh) | (lane_full >= n2 - sh)
        near = near + jnp.where(side, halo(ws, i, p), 0.0)
        low = near[0:8] + jnp.where(row8 < sh, RX[f, 0, i : i + 1], 0.0)
        high = near[n1 - 8 : n1] + jnp.where(row8 >= 8 - sh, RX[f, 1, i : i + 1], 0.0)
        return jnp.concatenate([low, near[8 : n1 - 8], high], axis=0)

    def field(f):
        if f < 3:
            return S.at[f], n0
        return {V1I: (V1, m0)}[f]

    ZBUF = {NLI: (NL, NZ, m0), CII: (CI, CZ, m0), PI: (P, PZ, n0), NII: (NI, NZI, n0)}

    def message(f, a, d):
        if a == 0:
            if f in FINAL:
                src, dst = F.at[f - F0I, 0, pl.ds(0, n1)], F.at[f - F0I, n0, pl.ds(0, n1)]
            elif f in ZBUF:
                src, dst, n = ZBUF[f]
                src, dst = src.at[n - 1 if d else 0], dst.at[1 - d]
            else:
                ref, n = field(f)
                src = ref.at[n if d else 1, rows]
                dst = ref.at[0 if d else n + 1, rows]
        elif a == 1:
            count = m0 if f in COARSE else n0
            src, dst = SX.at[f, d, pl.ds(0, count)], RX.at[f, 1 - d, pl.ds(0, count)]
        else:
            src, dst = SY.at[f], RY.at[f, 1 - d]
        step = 1 if d else -1
        return pltpu.make_async_remote_copy(
            src_ref=src, dst_ref=dst, send_sem=send_sem.at[f, a, d], recv_sem=recv_sem.at[f, a, d],
            device_id={AXES[a]: lax.rem(me[a] + step + sizes[a], sizes[a])}, device_id_type=MESH,
        )

    def dirs(f):
        return (0,) if f in FINAL else (0, 1)

    def can_send(a, d):
        return me[a] < sizes[a] - 1 if d else me[a] > 0

    def send(f, a):
        for d in dirs(f):
            pl.when(can_send(a, d))(lambda f=f, a=a, d=d: message(f, a, d).start())

    def receive(f, a):
        for d in dirs(f):
            pl.when(can_send(a, 1 - d))(lambda f=f, a=a, d=d: message(f, a, d).wait_recv())

    def faces_x(f, get, count):
        for i in range(count):
            SX[f, 0, i : i + 1] = get(i, 0)
            if f not in FINAL:
                SX[f, 1, i : i + 1] = get(i, n1 - 1)

    def rows_x(f, ref):
        width = 2 if f in COARSE else 1
        for i in range(m0 if f in COARSE else n0):
            for w in range(width):
                ref[1 + i, PAD - 1 - w : PAD - w] = RX[f, 0, i : i + 1]
                ref[1 + i, PAD + n1 + w : PAD + n1 + w + 1] = RX[f, 1, i : i + 1]

    def line_message(offs, sign):
        z, x, y = [o * sign for o in offs]
        side = [0 if o > 0 else 1 for o in (z, x, y)]
        if not y:
            src, dst = LZX.at[1 - side[0], 1 - side[1]], RZX.at[side[0], side[1]]
        elif not x:
            plane = place(m0 - 1 if z > 0 else 0, 0, 4)[0]
            src, dst = SY.at[V1I, plane], RZY.at[side[0], side[2]]
        else:
            src, dst = LXY.at[1 - side[1]], RXY.at[side[1], side[2]]
        at = lines.index((z, x, y))
        return pltpu.make_async_remote_copy(
            src_ref=src, dst_ref=dst, send_sem=lsend.at[at], recv_sem=lrecv.at[at],
            device_id=device((z, x, y)), device_id_type=MESH,
        )

    def cross_message(a, b, d, sign):
        src, dst = {
            (0, 1): (LRZ.at[d], RRZ.at[d]),
            (1, 0): (LRX.at[d], RRX.at[d]),
            (0, 2): (SY.at[2, place(0 if d else n0 - 1, 0, 2)[0]], RZ2.at[d]),
            (2, 0): (LP0, RZ0.at[d]),
            (1, 2): (LY2.at[d], RX2.at[d]),
            (2, 1): (LY1, RX1.at[d]),
        }[a, b]
        at = CROSS.index((a, b, d))
        return pltpu.make_async_remote_copy(
            src_ref=src, dst_ref=dst, send_sem=csend.at[at], recv_sem=crecv.at[at],
            device_id=device(cross_offs(a, b, d, sign)), device_id_type=MESH,
        )

    def cross_offs(a, b, d, sign):
        offs = [0, 0, 0]
        offs[a], offs[b] = (-sign if d else sign), sign
        return tuple(offs)

    def cross_rows():
        for d in (0, 1):
            i, r = (0 if d else n0 - 1), (0 if d else n1 - 1)
            LRZ[d] = S[1, 1 + i, PAD + n1 - 1 : PAD + n1]
            LRX[d] = S[0, n0, PAD + r : PAD + r + 1]
            for v in range(LY2.shape[1]):
                LY2[d, v] = SY[2, v, (0 if d else 7) : (1 if d else 8)]
        top = [((n0 - 1, g), S[0, n0, PAD + 8 * g : PAD + 8 * g + 8]) for g in range(groups)]
        for acc in gather(top, 2).values():
            LP0[...] = acc
        last = [((i, groups - 1), S[1, 1 + i, PAD + n1 - 8 : PAD + n1]) for i in range(n0)]
        for v, acc in gather(last, 2).items():
            LY1[v] = acc[7:8]

    def cross_send():
        for at in CROSS:
            pl.when(exists(cross_offs(*at, 1)))(lambda at=at: cross_message(*at, 1).start())

    def cross_receive():
        for at in CROSS:
            pl.when(exists(cross_offs(*at, -1)))(lambda at=at: cross_message(*at, -1).wait_recv())

    def halo_fg():
        for d in (0, 1):
            kk = place(0 if d else n0 - 1, 0, 2)[1]
            rhs = PZ[d] + S[0, n0, rows] if d else PZ[d]
            col = [pltpu.roll(RZ2[d], (2 * n2 - 2 * (kk + g) + 1) % n2, 1) for g in range(groups)]
            rhs = rhs + jnp.where(lane_full < 1, jnp.concatenate(col, axis=0), 0.0)
            first = rhs[0:8] + jnp.where(row8 < 1, RRZ[d], 0.0)
            FG[(n0 + 1) * d, rows] = jnp.concatenate([first, rhs[8:]], axis=0) * NZI[d]
        rowi = lax.broadcasted_iota(jnp.int32, (n0, n2), 0)
        lanei = lax.broadcasted_iota(jnp.int32, (n0, n2), 1)
        per = n2 // 2
        for d in (0, 1):
            rhs = RX[PI, d] + SX[1, 1] if d else RX[PI, d]
            rhs = rhs + jnp.where(rowi == 0, RRX[d], 0.0)
            index = rowi * groups + (0 if d else groups - 1)
            at = lax.rem(2 * lax.rem(index, per) + n2 - 1, n2)
            got = jnp.zeros((n0, n2), jnp.float32)
            for v in range(RX2.shape[1]):
                here = (lanei == at) & (index >= v * per) & (index < (v + 1) * per)
                got = got + jnp.where(here, RX2[d, v], 0.0)
            rhs = rhs + jnp.where(lanei < 1, jnp.sum(got, axis=1, keepdims=True), 0.0)
            RX[FGI, d] = rhs * RX[NII, d]
        ws = []
        for v, (ep, en) in enumerate(zip(edges(PI, 2), edges(NII, 2))):
            rhs = ep + jnp.where(is_low[2], SY[2, v], 0.0)
            if v == 0:
                k0 = place(n0 - 1, 0, 2)[1]
                moved = pltpu.roll(align(RZ0[0], RZ0[1], 2), (n2 - 2 * k0) % n2, 1)
                rhs = rhs + jnp.where(keys[2] < groups, moved, 0.0)
            line = align(jnp.broadcast_to(RX1[0, v], (8, n2)), jnp.broadcast_to(RX1[1, v], (8, n2)), 2)
            line = pltpu.roll(line, n2 - 2 * (groups - 1), 1)
            here = (lax.rem(keys[2], groups) == 0) & (row8 < 1)
            ws.append((rhs + jnp.where(here, line, 0.0)) * en)
        return ws

    def lines_send():
        for z in (0, 1):
            for x in (0, 1):
                c, r = (m0 - 1) * z, (n1 - 1) * x
                LZX[z, x] = V1[1 + c, PAD + r : PAD + r + 1]
        for x in (0, 1):
            for v in range(LXY.shape[1]):
                LXY[x, v] = SY[V1I, v, 7 * x : 7 * x + 1]
        for offs in lines:
            pl.when(exists(offs))(lambda offs=offs: line_message(offs, 1).start())

    def lines_receive():
        for offs in lines:
            pl.when(exists(offs))(lambda offs=offs: line_message(offs, -1).wait_recv())

    def align(low, high, p):
        return jnp.where(is_low[p], pltpu.roll(high, n2 - p // 2, 1), pltpu.roll(low, p // 2, 1))

    def halo_v2(ev, enl, eci):
        sh, kgroup = 2, [place(c, 0, 4) for c in (m0 - 1, 0)]
        col = [align(RZY[d, 0], RZY[d, 1], 4) for d in (0, 1)]
        for d, edge in ((0, 0), (1, m0 + 1)):
            v, kk = kgroup[d]
            near = NZ[d] + V1[1 if d == 0 else m0, rows]
            parts = [pltpu.roll(col[d], (n2 - 4 * (kk + g)) % n2, 1) for g in range(groups)]
            side = (lane_full < sh) | (lane_full >= n2 - sh)
            near = near + jnp.where(side, jnp.concatenate(parts, axis=0), 0.0)
            low = near[0:8] + jnp.where(row8 < sh, RZX[d, 0], 0.0)
            high = near[n1 - 8 : n1] + jnp.where(row8 >= 8 - sh, RZX[d, 1], 0.0)
            near = jnp.concatenate([low, near[8 : n1 - 8], high], axis=0)
            V2[edge, rows] = V1[edge, rows] - CZ[d] * near
        rowc = lax.broadcasted_iota(jnp.int32, (m0, n2), 0)
        lanec = lax.broadcasted_iota(jnp.int32, (m0, n2), 1)
        per = n2 // 4
        for d in (0, 1):
            near = RX[NLI, d, 0:m0] + SX[V1I, d, 0:m0]
            near = near + jnp.where(rowc == 0, RZX[0, d], 0.0) + jnp.where(rowc == m0 - 1, RZX[1, d], 0.0)
            for y in (0, 1):
                index = rowc * groups + (groups - 1 if d == 0 else 0)
                at = lax.rem(4 * lax.rem(index, per) + (n2 - 1 if y == 0 else 0), n2)
                got = jnp.zeros((m0, n2), jnp.float32)
                for v in range(RXY.shape[2]):
                    here = (lanec == at) & (index >= v * per) & (index < (v + 1) * per)
                    got = got + jnp.where(here, RXY[d, y, v], 0.0)
                got = jnp.sum(got, axis=1, keepdims=True)
                near = near + jnp.where((lanec < sh) if y == 0 else (lanec >= n2 - sh), got, 0.0)
            RX[V2I, d, 0:m0] = RX[V1I, d, 0:m0] - RX[CII, d, 0:m0] * near
        ws = []
        for v in range(len(ev)):
            near = enl[v] + SY[V1I, v]
            for d, c in ((0, 0), (1, m0 - 1)):
                into, k0 = place(c, 0, 4)
                if into == v:
                    shift = (4 * (k0 - kgroup[d][1])) % n2
                    moved = pltpu.roll(col[d], shift, 1) if shift else col[d]
                    near = near + jnp.where((keys[4] >= k0) & (keys[4] < k0 + groups), moved, 0.0)
            for d in (0, 1):
                line = align(
                    jnp.broadcast_to(RXY[d, 0, v], (8, n2)), jnp.broadcast_to(RXY[d, 1, v], (8, n2)), 4
                )
                jump = 4 * (groups - 1)
                line = pltpu.roll(line, n2 - jump if d == 0 else jump, 1)
                here = lax.rem(keys[4], groups) == (0 if d == 0 else groups - 1)
                here = here & ((row8 < sh) if d == 0 else (row8 >= 8 - sh))
                near = near + jnp.where(here, line, 0.0)
            ws.append(ev[v] - eci[v] * near)
        return ws

    def exchange(f, p):
        ref, count = field(f)
        send(f, 0)
        faces_x(f, lambda i, r: ref[1 + i, PAD + r : PAD + r + 1], count)
        send(f, 1)
        pack(f, lambda i: ref[1 + i, rows], count, p)
        send(f, 2)

    def one(f, a):
        ref, count = field(f)
        if a == 1:
            faces_x(f, lambda i, r: ref[1 + i, PAD + r : PAD + r + 1], count)
        if a == 2:
            pack(f, lambda i: ref[1 + i, rows], count, 2)
        send(f, a)

    def spread_faces(f, ref, n, p):
        send(f, 0)
        faces_x(f, lambda c, r: ref[c, r : r + 1], n)
        send(f, 1)
        pack(f, lambda c: ref[c], n, p)
        send(f, 2)

    def partial_rhs():
        for i in range(n0):
            x1, x2 = S[1, 1 + i, rows], S[2, 1 + i, rows]
            rhs = jnp.where(row_full >= 1, S[1, 1 + i, pl.ds(PAD - 1, n1)], 0.0) - x1
            rhs = rhs + (jnp.where(lane_full >= 1, pltpu.roll(x2, 1, 1), 0.0) - x2)
            rhs = rhs - S[0, 1 + i, rows]
            if i > 0:
                rhs = rhs + S[0, i, rows]
            P[i] = rhs

    loads[0].wait()
    for i in range(n0):
        NI[i] = 1.0 / (6.0 + NI[i])
    for pos, (k, a) in enumerate(((1, 1), (2, 2), (0, 0))):
        loads[1 + 2 * pos].wait()
        loads[2 + 2 * pos].wait()
        for i in range(n0):
            inv = 1.0 / D[k, i]
            D[k, i] = inv
            S[k, 1 + i, rows] = R[k, i] * inv
        if pos == 0:
            pl.semaphore_wait(barrier, total)
            spread_faces(NII, NI, n0, 2)
        one(k, a)
    partial_rhs()
    cross_rows()
    cross_send()
    spread_faces(PI, P, n0, 2)
    for f, a in ((0, 1), (2, 1), (1, 0), (2, 0), (0, 2), (1, 2)):
        one(f, a)

    loads[7].wait()
    spread_rows = (
        lax.broadcasted_iota(jnp.int32, (n1, m1), 0) // 2 == lax.broadcasted_iota(jnp.int32, (n1, m1), 1)
    ).astype(jnp.float32)
    spread_cols = (
        lax.broadcasted_iota(jnp.int32, (m2, n2), 1) // 2 == lax.broadcasted_iota(jnp.int32, (m2, n2), 0)
    ).astype(jnp.float32)
    exact = functools.partial(
        jnp.dot, precision=lax.Precision.HIGHEST, preferred_element_type=jnp.float32
    )
    for i in range(m0):
        CI[i] = exact(spread_rows, exact(1.0 / (6.0 + CS[i]), spread_cols))
    spread_faces(CII, CI, m0, 4)

    receive(1, 1)
    receive(0, 0)
    receive(2, 2)
    ws = edges(2, 2)
    for i in range(n0):
        rhs = P[i] + jnp.where(lane_full < 1, halo(ws, i, 2), 0.0)
        if i == 0:
            rhs = rhs + S[0, 0, rows]
        first = rhs[0:8] + jnp.where(row8 < 1, RX[1, 0, i : i + 1], 0.0)
        FG[1 + i, rows] = jnp.concatenate([first, rhs[8:]], axis=0) * NI[i]
    def gradients(j, G):
        for i in range(n0):
            x = F[j, i, 0:n1]
            above = F[j, i + 1, 0:n1] - x if i < n0 - 1 else -x
            ahead = jnp.where(lane_full >= n2 - 1, 0.0, pltpu.roll(x, n2 - 1, 1)) - x
            for k, grad in enumerate((above, F[j, i, 1 : n1 + 1] - x, ahead)):
                G[k, i] = G[k, i] + grad if j == 0 else grad


    def smooth(k):
        for a in range(3):
            if (k, a) not in ((1, 1), (0, 0), (2, 2)):
                receive(k, a)
        rows_x(k, S.at[k])
        w = edges(k, 2)
        for i in range(n0):
            x = S[k, 1 + i, rows]
            near = S[k, i, rows] + S[k, i + 2, rows] + inplane(S.at[k, 1 + i], x, halo(w, i, 2), 1)
            OB[k, i] = x + near * D[k, i]

    for i in range(n0):
        F[0, i, 0:n1] = local_near(FG, i, n0, 1)

    for f in (NII, PI):
        for a in range(3):
            receive(f, a)
    cross_receive()
    ws = halo_fg()
    for c in range(m0):
        t = None
        for i in (2 * c, 2 * c + 1):
            near = outer_near(F[0, i, 0:n1], FG, FGI, ws, i, n0, 2)
            F[0, i, 0:n1] = near
            t = near if t is None else t + near
        t = t + jnp.where(lane_full % 2 == 0, pltpu.roll(t, n2 - 1, 1), pltpu.roll(t, 1, 1))
        T[c, rows] = t
        t = t + jnp.where(row_full % 2 == 0, T[c, pl.ds(PAD + 1, n1)], T[c, pl.ds(PAD - 1, n1)])
        CR[c] = t
        V1[1 + c, rows] = t * CI[c]
    exchange(V1I, 4)
    lines_send()
    for c in range(m0):
        NL[c] = local_near(V1, c, m0, 2)
    spread_faces(NLI, NL, m0, 4)

    def faces_f(j):
        f = F0I + j
        send(f, 0)
        faces_x(f, lambda i, r: F[j, i, r : r + 1], n0)
        send(f, 1)
        pack(f, lambda i: F[j, i, 0:n1], n0, 2)
        send(f, 2)

    for i in range(n0):
        F[0, i, 0:n1] = FG[1 + i, rows] + F[0, i, 0:n1] * NI[i]
    faces_f(0)
    for k in (1, 2, 0):
        smooth(k)
    gradients(0, OB)

    for f in (CII, V1I, NLI):
        for a in range(3):
            receive(f, a)
    ws = edges(V1I, 4)
    for c in range(m0):
        near = outer_near(NL[c], V1, V1I, ws, c, m0, 4)
        A1[c] = CR[c] - near
        V2[1 + c, rows] = V1[1 + c, rows] - near * CI[c]
    faces_x(V2I, lambda c, r: V2[1 + c, PAD + r : PAD + r + 1], m0)
    pack(V2I, lambda c: V2[1 + c, rows], m0, 4)
    lines_receive()
    w2 = halo_v2(ws, edges(NLI, 4), edges(CII, 4))

    def fold(x):
        acc = x[0:8]
        for g in range(1, groups):
            acc = acc + x[8 * g : 8 * g + 8]
        return acc

    def spread_near(j, V, w):
        for c in range(m0):
            x = V[1 + c, rows]
            near = x + inplane(V.at[1 + c], x, halo(w, c, 4), 1)
            F[j, 2 * c, 0:n1] = (near + V[c, rows]) * NI[2 * c]
            F[j, 2 * c + 1, 0:n1] = (near + V[c + 2, rows]) * NI[2 * c + 1]
        faces_f(j)

    sums = [jnp.zeros((8, n2), jnp.float32) for _ in range(5)]
    for c in range(m0):
        v1, v2, a1, cr = V1[1 + c, rows], V2[1 + c, rows], A1[c], CR[c]
        sums[0] = sums[0] + fold(v1 * cr)
        sums[1] = sums[1] + fold(v2 * cr)
        sums[2] = sums[2] + fold(v1 * a1)
        sums[3] = sums[3] + fold(v2 * a1)
        sums[4] = sums[4] + fold(v2 * (a1 - local_near(V2, c, m0, 2)))
    outer = fold(V2[1, rows] * V2[0, rows] + V2[m0, rows] * V2[m0 + 1, rows])
    for v, w in enumerate(w2):
        outer = outer + SY[V2I, v] * w
    rim = SX[V2I, 0, 0:m0] * RX[V2I, 0, 0:m0] + SX[V2I, 1, 0:m0] * RX[V2I, 1, 0:m0]
    sums[4] = sums[4] - outer
    rim = 2.0 * jnp.sum(rim, axis=0, keepdims=True)
    sums[4] = sums[4] - jnp.where(row8 == 0, rim, 0.0)
    lane1 = lax.broadcasted_iota(jnp.int32, (1, n2), 1)
    part = jnp.zeros((1, n2), jnp.float32)
    for q, s in enumerate(sums):
        part = jnp.where(lane1 == q, jnp.sum(jnp.sum(s, axis=0, keepdims=True), axis=1, keepdims=True), part)

    def slot(axes, at):
        index = 0
        for a in axes:
            index = index * sizes[a] + at(a)
        return index

    def sum_message(p, offs, sign):
        axes, slots = phases[p], slots_of[p]
        other = partner(axes, offs, sign)
        index = slot(axes, (lambda a: me[a]) if sign > 0 else (lambda a: other[AXES[a]]))
        sem = p * slots_of[0].shape[0] + slot(axes, lambda a: offs[axes.index(a)])
        return pltpu.make_async_remote_copy(
            src_ref=slots.at[index], dst_ref=slots.at[index], send_sem=psend.at[sem], recv_sem=precv.at[sem],
            device_id=other, device_id_type=MESH,
        )

    def sum_start(p, value):
        slots_of[p][slot(phases[p], lambda a: me[a])] = value
        for offs in offsets(phases[p]):
            sum_message(p, offs, 1).start()

    def sum_end(p):
        for offs in offsets(phases[p]):
            sum_message(p, offs, -1).wait_recv()
        terms = [slots_of[p][d] for d in range(slots_of[p].shape[0])]
        while len(terms) > 1:
            terms = [functools.reduce(lambda x, y: x + y, terms[t : t + 2]) for t in range(0, len(terms), 2)]
        return terms[0]

    sum_start(0, part)
    rows_x(V2I, V2)
    spread_near(2, V2, w2)
    rows_x(V1I, V1)
    spread_near(1, V1, ws)
    gradients(1, G1)
    gradients(2, G2)

    part = sum_end(0)
    for p in range(1, len(phases)):
        sum_start(p, part)
        part = sum_end(p)
    gone, gtwo, hone, hmix, htwo = [
        jnp.sum(jnp.where(lane1 == q, part, 0.0), axis=1, keepdims=True) for q in range(5)
    ]
    two = (gtwo - hmix * gone / hone) / (htwo - hmix * hmix / hone)
    oneco = (gone - hmix * two) / hone
    CO[0:1] = jnp.broadcast_to(oneco, (1, n2))
    CO[1:2] = jnp.broadcast_to(two, (1, n2))
    for f in FINAL:
        for a in range(3):
            receive(f, a)

    def mix(get):
        a = get(0)
        return a + jnp.broadcast_to(oneco, a.shape) * get(1) + jnp.broadcast_to(two, a.shape) * get(2)

    MZ[...] = mix(lambda j: F[j, n0, 0:n1])
    MX[...] = mix(lambda j: RX[F0I + j, 1])
    for v in range(RY.shape[2]):
        MY[v] = pltpu.roll(mix(lambda j: RY[F0I + j, 1, v]), n2 - 1, 1)

    for p in range(len(phases)):
        for offs in offsets(phases[p]):
            sum_message(p, offs, 1).wait_send()
    for offs in lines:
        pl.when(exists(offs))(lambda offs=offs: line_message(offs, 1).wait_send())
    for at in CROSS:
        pl.when(exists(cross_offs(*at, 1)))(lambda at=at: cross_message(*at, 1).wait_send())
    for a in range(3):
        for d in (0, 1):
            def drain(a=a, d=d):
                for f in range(FIELDS):
                    if f not in LOCAL and d in dirs(f):
                        message(f, a, d).wait_send()
            pl.when(can_send(a, d))(drain)


def combine(parts, OB, G1, G2, CO, MZ, MX, MY, out, W, sem):
    _, n0, n1, n2 = OB.shape
    one = jnp.broadcast_to(CO[0:1], (n1, n2))
    two = jnp.broadcast_to(CO[1:2], (n1, n2))
    groups, per, step = n1 // 8, n2 // 2, n0 // parts
    row8 = lax.broadcasted_iota(jnp.int32, (8, n2), 0)
    lane_full = lax.broadcasted_iota(jnp.int32, (n1, n2), 1)

    def edge(k, i, x):
        if k == 0:
            return x + MZ[...] if i == n0 - 1 else x
        if k == 1:
            last = x[n1 - 8 : n1] + jnp.where(row8 == 7, MX[i : i + 1], 0.0)
            return jnp.concatenate([x[0 : n1 - 8], last], axis=0)
        ats = [divmod(i * groups + g, per) for g in range(groups)]
        parts = [pltpu.roll(MY[v], (n2 - 2 * kk) % n2, 1) for v, kk in ats]
        return x + jnp.where(lane_full >= n2 - 1, jnp.concatenate(parts, axis=0), 0.0)

    copies = []
    for k in range(3):
        for h in range(parts):
            for i in range(h * step, (h + 1) * step):
                W[k, i] = edge(k, i, OB[k, i] + one * G1[k, i] + two * G2[k, i])
            planes = pl.ds(h * step, step)
            copies.append(pltpu.make_async_copy(W.at[k, planes], out.at[k, planes], sem.at[k * parts + h]))
            copies[-1].start()
    for c in copies:
        c.wait()


def solution(mesh):
    sizes = tuple(mesh.shape[a] for a in AXES)

    def local(residual, edge_diag, node_shift, coarse_shift):
        n0, n1, n2 = node_shift.shape
        m0, m1, m2 = coarse_shift.shape
        vecs = max(-(-(n0 * (n1 // 8)) // (n2 // 2)), -(-(m0 * (n1 // 8)) // (n2 // 4)))
        f32 = jnp.float32
        counts = [math.prod(sizes[a] for a in axes) for axes in phases_of(sizes)]
        V = lambda *s: pltpu.VMEM(s, f32)
        scratch = [
            V(3, n0, n1, n2), V(3, n0, n1, n2), V(n0, n1, n2), V(m0, m1, m2),
            V(3, n0 + 2, n1 + 2 * PAD, n2), V(n0 + 2, n1 + 2 * PAD, n2),
            V(m0, n1, n2), V(m0, n1, n2), V(m0, n1, n2), V(m0, n1, n2), V(m0, n1 + 2 * PAD, n2),
            V(m0 + 2, n1 + 2 * PAD, n2), V(m0 + 2, n1 + 2 * PAD, n2),
            V(3, n0 + 1, n1 + PAD, n2),
            V(FIELDS, 2, n0, n2), V(FIELDS, 2, n0, n2), V(FIELDS, vecs, 8, n2), V(FIELDS, 2, vecs, 8, n2),
            V(2, n1, n2), V(2, n1, n2), V(2, 2, 1, n2), V(2, vecs, 1, n2),
            V(2, 2, 1, n2), V(2, 2, 8, n2), V(2, 2, vecs, 1, n2),
            V(n0, n1, n2), V(2, n1, n2), V(2, n1, n2), V(2, 1, n2), V(2, 1, n2), V(2, vecs, 1, n2), V(vecs, 1, n2),
            V(8, n2), V(2, 1, n2), V(2, 1, n2), V(2, 8, n2), V(2, 8, n2), V(2, vecs, 1, n2), V(2, vecs, 1, n2),
            *[V(c, 1, n2) for c in counts],
        ]
        sems = [pltpu.SemaphoreType.DMA(s) for s in ((8,), *[(FIELDS, 3, 2)] * 2, *[(sum(counts),)] * 2, *[(12,)] * 4)]

        def scoped(*refs):
            plain, slots_of = refs[: -len(counts)], refs[-len(counts) :]
            pl.run_scoped(functools.partial(kernel, sizes, *plain, slots_of), *sems)

        field = pltpu.VMEM(residual.shape, f32)
        limit = 67_043_328 - 12 * math.prod(residual.shape) - 2**18
        fields = pl.pallas_call(
            scoped,
            out_shape=[field] * 3 + [pltpu.VMEM(s, f32) for s in ((8, n2), (n1, n2), (n0, n2), (vecs, 8, n2))],
            in_specs=[pl.BlockSpec(memory_space=pltpu.HBM)] * 4,
            out_specs=[pl.BlockSpec(memory_space=pltpu.VMEM)] * 7,
            scratch_shapes=scratch,
            compiler_params=pltpu.CompilerParams(collective_id=0, has_side_effects=True, vmem_limit_bytes=limit),
        )(residual, edge_diag, node_shift, coarse_shift)
        parts = 2 if n0 % 2 == 0 else 1
        return pl.pallas_call(
            functools.partial(combine, parts),
            out_shape=jax.ShapeDtypeStruct(residual.shape, f32),
            in_specs=[pl.BlockSpec(memory_space=pltpu.VMEM)] * 7,
            out_specs=pl.BlockSpec(memory_space=pltpu.HBM),
            scratch_shapes=[field, pltpu.SemaphoreType.DMA((3 * parts,))],
            compiler_params=pltpu.CompilerParams(vmem_limit_bytes=8 * math.prod(residual.shape)),
        )(*fields)

    placed = (
        P(None, "gz", "gx", "gy"),
        P(None, "gz", "gx", "gy"),
        P("gz", "gx", "gy"),
        P("gz", "gx", "gy"),
    )
    return jax.shard_map(
        local, mesh=mesh, in_specs=placed, out_specs=P(None, "gz", "gx", "gy"), check_vma=False
    )
```

```python
import functools
import itertools
import math

import jax
import jax.numpy as jnp
from jax import lax
from jax.experimental import pallas as pl
from jax.experimental.pallas import tpu as pltpu
from jax.sharding import PartitionSpec as P

MESH = pl.DeviceIdType.MESH
AXES = ("gz", "gx", "gy")
PI, V1I, V2I, F0I, NLI, CII, NII, FGI = 3, 4, 5, 6, 9, 10, 11, 12
FIELDS = 13
FINAL = (F0I, F0I + 1, F0I + 2)
COARSE = (V1I, V2I, NLI, CII)
LOCAL = (V2I, FGI)
CROSS = [(a, b, d) for a in range(3) for b in range(3) if a != b for d in (0, 1)]
PAD = 8
FEW = 32


def phases_of(sizes):
    return ((0, 1, 2),) if math.prod(sizes) <= FEW else ((1, 2), (0,))


def greeted(sizes, rounds):
    near = set(itertools.product(range(-1, 2), range(-2, 3), range(-2, 3)))
    known = set(near)
    for moves in rounds:
        known |= {tuple(p + q for p, q in zip(k, m)) for k in known for m in moves}
    needed = set()
    for axes in phases_of(sizes):
        spans = [range(1 - sizes[a], sizes[a]) if a in axes else (0,) for a in range(3)]
        needed |= set(itertools.product(*spans))
    every = near | (needed - known)
    return sorted(o for o in every if any(o) and all(abs(p) < n for p, n in zip(o, sizes)))


def kernel(
    sizes,
    res, dia, shf, csh, OB, G1, G2, CO, MZ, MX, MY,
    R, D, NI, CS, S, FG, CI, CR, A1, NL, T, V1, V2, F,
    SX, RX, SY, RY, NZ, CZ, LZX, LXY, RZX, RZY, RXY,
    P, PZ, NZI, LRZ, LRX, LY2, LY1, LP0, RRZ, RRX, RZ2, RZ0, RX2, RX1, DX,
    slots_of,
    in_sem, send_sem, recv_sem, psend, precv, lsend, lrecv, csend, crecv,
):
    phases = phases_of(sizes)
    n0, n1, n2 = NI.shape
    m0, m1, m2 = CS.shape
    groups = n1 // 8
    me = [lax.axis_index(a) for a in AXES]
    rows = pl.ds(PAD, n1)

    def offsets(axes):
        every = itertools.product(*[range(sizes[a]) for a in axes])
        return [offs for offs in every if any(offs)]

    def partner(axes, offs, sign):
        return {
            AXES[a]: lax.rem(me[a] + (o if sign > 0 else sizes[a] - o), sizes[a]) for a, o in zip(axes, offs)
        }

    barrier = pltpu.get_barrier_semaphore()
    faces = [offs for offs in itertools.product((-1, 0, 1), repeat=3) if sum(map(abs, offs)) == 1]
    lines = [offs for offs in itertools.product((-1, 0, 1), repeat=3) if sum(map(abs, offs)) == 2]

    def exists(offs):
        inside = [(me[a] + o >= 0) & (me[a] + o < sizes[a]) for a, o in enumerate(offs) if o]
        return functools.reduce(jnp.logical_and, inside)

    def device(offs):
        return {AXES[a]: me[a] + o for a, o in enumerate(offs) if o}

    total = jnp.int32(0)
    for offs in greeted(sizes, (faces + [m for m in lines if min(m) < 0], faces + lines)):
        there = exists(offs)
        pl.when(there)(
            lambda offs=offs: pl.semaphore_signal(
                barrier, inc=1, device_id=device(offs), device_id_type=MESH
            )
        )
        total = total + there.astype(jnp.int32)

    bands = (0, n1 - 8)
    loads = {}

    def load(key, src, dst):
        loads[key] = pltpu.make_async_copy(src, dst, in_sem.at[len(loads)])
        loads[key].start()

    for first, count in [(r, 8) for r in bands] + [(8, n1 - 16)]:
        at = pl.ds(first, count)
        load((3, first), shf.at[:, at], NI.at[:, at])
        for k in (1, 2, 0):
            load((k, first, 0), res.at[k, :, at], R.at[k, :, at])
            load((k, first, 1), dia.at[k, :, at], D.at[k, :, at])
    load(4, csh, CS)

    for k in range(3):
        for i in range(n0):
            F[k, i, n1 : n1 + 1] = jnp.zeros((1, n2), jnp.float32)
    DX[...] = jnp.zeros(DX.shape, jnp.float32)

    def clear(offs, *refs):
        @pl.when(jnp.logical_not(exists(offs)))
        def _():
            for ref in refs:
                ref[...] = jnp.zeros(ref.shape, jnp.float32)

    for d in (0, 1):
        step, i, c = (1, n0 + 1, m0 + 1) if d else (-1, 0, 0)
        planes = [S.at[k, i, rows] for k in range(3)] + [V1.at[c, rows], NZ.at[d], CZ.at[d], PZ.at[d], NZI.at[d]]
        clear((step, 0, 0), *planes, *([F.at[k, n0, pl.ds(0, n1)] for k in range(3)] if d else []))
        clear((0, step, 0), *[RX.at[f, d] for f in range(FIELDS) if f not in LOCAL])
        clear((0, 0, step), *[RY.at[f, d] for f in range(FIELDS) if f not in LOCAL])
    for offs in lines:
        z, x, y = [int(o > 0) for o in offs]
        clear(offs, RXY.at[x, y] if not offs[0] else RZY.at[z, y] if not offs[1] else RZX.at[z, x])

    lane = lax.broadcasted_iota(jnp.int32, (8, n2), 1)
    lane_full = lax.broadcasted_iota(jnp.int32, (n1, n2), 1)
    row_full = lax.broadcasted_iota(jnp.int32, (n1, n2), 0)
    row8 = lax.broadcasted_iota(jnp.int32, (8, n2), 0)
    keys = {p: ((lane + p // 2) // p) % (n2 // p) for p in (2, 4)}
    is_low = {p: (lane % p) >= p // 2 for p in (2, 4)}

    def place(i, g, p):
        k = i * groups + g
        per = n2 // p
        return k // per, k % per

    def gather(blocks, p):
        accs = {}
        for (i, g), part in blocks:
            v, kk = place(i, g, p)
            if kk:
                part = pltpu.roll(part, p * kk, 1)
            accs[v] = jnp.where(keys[p] == kk, part, accs.get(v, 0.0))
        return accs

    def pack(f, plane, count, p):
        at = [(i, g) for i in range(count) for g in range(groups)]
        planes = [plane(i) for i in range(count)]
        accs = gather([((i, g), planes[i][8 * g : 8 * g + 8]) for i, g in at], p)
        for v, acc in accs.items():
            SY[f, v] = acc

    def halo(ws, i, p):
        parts = []
        for g in range(groups):
            v, kk = place(i, g, p)
            parts.append(pltpu.roll(ws[v], n2 - p * kk, 1) if kk else ws[v])
        return jnp.concatenate(parts, axis=0)

    def inplane(ref, x, h, sh):
        near = ref[pl.ds(PAD - sh, n1)] + ref[pl.ds(PAD + sh, n1)]
        near = near + jnp.where(lane_full < sh, h, pltpu.roll(x, sh, 1))
        return near + jnp.where(lane_full >= n2 - sh, h, pltpu.roll(x, n2 - sh, 1))

    def local_near(ref, i, n, sh):
        x = ref[1 + i, rows]
        near = jnp.where(row_full >= sh, ref[1 + i, pl.ds(PAD - sh, n1)], 0.0)
        near = near + jnp.where(row_full < n1 - sh, ref[1 + i, pl.ds(PAD + sh, n1)], 0.0)
        near = near + jnp.where(lane_full >= sh, pltpu.roll(x, sh, 1), 0.0)
        near = near + jnp.where(lane_full < n2 - sh, pltpu.roll(x, n2 - sh, 1), 0.0)
        if i > 0:
            near = near + ref[i, rows]
        if i < n - 1:
            near = near + ref[i + 2, rows]
        return near

    def edges(f, p):
        sh = p // 2
        return [
            jnp.where(is_low[p], pltpu.roll(RY[f, 1, v], n2 - sh, 1), pltpu.roll(RY[f, 0, v], sh, 1))
            for v in range(RY.shape[2])
        ]

    def outer_near(near, ref, f, ws, i, n, p):
        sh = p // 2
        if i == 0:
            near = near + ref[0, rows]
        if i == n - 1:
            near = near + ref[n + 1, rows]
        side = (lane_full < sh) | (lane_full >= n2 - sh)
        near = near + jnp.where(side, halo(ws, i, p), 0.0)
        low = near[0:8] + jnp.where(row8 < sh, RX[f, 0, i : i + 1], 0.0)
        high = near[n1 - 8 : n1] + jnp.where(row8 >= 8 - sh, RX[f, 1, i : i + 1], 0.0)
        return jnp.concatenate([low, near[8 : n1 - 8], high], axis=0)

    def field(f):
        if f < 3:
            return S.at[f], n0
        return {V1I: (V1, m0)}[f]

    ZBUF = {NLI: (NL, NZ, m0), CII: (CI, CZ, m0), PI: (P, PZ, n0), NII: (NI, NZI, n0)}

    def message(f, a, d):
        if a == 0:
            if f in FINAL:
                src, dst = F.at[f - F0I, 0, pl.ds(0, n1)], F.at[f - F0I, n0, pl.ds(0, n1)]
            elif f in ZBUF:
                src, dst, n = ZBUF[f]
                src, dst = src.at[n - 1 if d else 0], dst.at[1 - d]
            else:
                ref, n = field(f)
                src = ref.at[n if d else 1, rows]
                dst = ref.at[0 if d else n + 1, rows]
        elif a == 1:
            count = m0 if f in COARSE else n0
            src, dst = SX.at[f, d, pl.ds(0, count)], RX.at[f, 1 - d, pl.ds(0, count)]
        else:
            src, dst = SY.at[f], RY.at[f, 1 - d]
        step = 1 if d else -1
        return pltpu.make_async_remote_copy(
            src_ref=src, dst_ref=dst, send_sem=send_sem.at[f, a, d], recv_sem=recv_sem.at[f, a, d],
            device_id={AXES[a]: lax.rem(me[a] + step + sizes[a], sizes[a])}, device_id_type=MESH,
        )

    def dirs(f):
        return (0,) if f in FINAL else (0, 1)

    def can_send(a, d):
        return me[a] < sizes[a] - 1 if d else me[a] > 0

    def send(f, a, only=(0, 1)):
        for d in [d for d in dirs(f) if d in only]:
            pl.when(can_send(a, d))(lambda f=f, a=a, d=d: message(f, a, d).start())

    def receive(f, a, only=(0, 1)):
        for d in [d for d in dirs(f) if d in only]:
            pl.when(can_send(a, 1 - d))(lambda f=f, a=a, d=d: message(f, a, d).wait_recv())

    def faces_x(f, get, count):
        for i in range(count):
            SX[f, 0, i : i + 1] = get(i, 0)
            if f not in FINAL:
                SX[f, 1, i : i + 1] = get(i, n1 - 1)

    def rows_x(f, ref):
        width = 2 if f in COARSE else 1
        for i in range(m0 if f in COARSE else n0):
            for w in range(width):
                ref[1 + i, PAD - 1 - w : PAD - w] = RX[f, 0, i : i + 1]
                ref[1 + i, PAD + n1 + w : PAD + n1 + w + 1] = RX[f, 1, i : i + 1]

    def line_message(offs, sign):
        z, x, y = [o * sign for o in offs]
        side = [0 if o > 0 else 1 for o in (z, x, y)]
        if not y:
            src, dst = LZX.at[1 - side[0], 1 - side[1]], RZX.at[side[0], side[1]]
        elif not x:
            plane = place(m0 - 1 if z > 0 else 0, 0, 4)[0]
            src, dst = SY.at[V1I, plane], RZY.at[side[0], side[2]]
        else:
            src, dst = LXY.at[1 - side[1]], RXY.at[side[1], side[2]]
        at = lines.index((z, x, y))
        return pltpu.make_async_remote_copy(
            src_ref=src, dst_ref=dst, send_sem=lsend.at[at], recv_sem=lrecv.at[at],
            device_id=device((z, x, y)), device_id_type=MESH,
        )

    def cross_message(a, b, d, sign):
        src, dst = {
            (0, 1): (LRZ.at[d], RRZ.at[d]),
            (1, 0): (LRX.at[d], RRX.at[d]),
            (0, 2): (SY.at[2, place(0 if d else n0 - 1, 0, 2)[0]], RZ2.at[d]),
            (2, 0): (LP0, RZ0.at[d]),
            (1, 2): (LY2.at[d], RX2.at[d]),
            (2, 1): (LY1, RX1.at[d]),
        }[a, b]
        at = CROSS.index((a, b, d))
        return pltpu.make_async_remote_copy(
            src_ref=src, dst_ref=dst, send_sem=csend.at[at], recv_sem=crecv.at[at],
            device_id=device(cross_offs(a, b, d, sign)), device_id_type=MESH,
        )

    def cross_offs(a, b, d, sign):
        offs = [0, 0, 0]
        offs[a], offs[b] = (-sign if d else sign), sign
        return tuple(offs)

    CROSS_INTO = {(0, 1): RRZ, (1, 0): RRX, (0, 2): RZ2, (2, 0): RZ0, (1, 2): RX2, (2, 1): RX1}
    for a, b, d in CROSS:
        clear(cross_offs(a, b, d, -1), CROSS_INTO[a, b].at[d])

    def cross_rows():
        for d in (0, 1):
            i, r = (0 if d else n0 - 1), (0 if d else n1 - 1)
            LRZ[d] = S[1, 1 + i, PAD + n1 - 1 : PAD + n1]
            LRX[d] = S[0, n0, PAD + r : PAD + r + 1]
        for k, g in ((2, groups - 1), (2, 0), (1, groups - 1)):
            top = [((i, g), S[k, 1 + i, PAD + 8 * g : PAD + 8 * g + 8]) for i in range(n0)]
            for v, acc in gather(top, 2).items():
                line = acc[7:8] if g else acc[0:1]
                if k == 2:
                    LY2[0 if g else 1, v] = line
                else:
                    LY1[v] = line

    def cross_plane():
        top = [((n0 - 1, g), S[0, n0, PAD + 8 * g : PAD + 8 * g + 8]) for g in range(groups)]
        for acc in gather(top, 2).values():
            LP0[...] = acc

    def rows_rhs():
        rowi = lax.broadcasted_iota(jnp.int32, (n0, n2), 0)
        lanei = lax.broadcasted_iota(jnp.int32, (n0, n2), 1)
        inner = [S[1, 1 + i, PAD + n1 - 2 : PAD + n1 - 1] for i in range(n0)]
        for d in (0, 1):
            x = jnp.where(rowi >= 1, pltpu.roll(SX[0, d], 1, 0), 0.0) - SX[0, d]
            x = x + jnp.where(lanei >= 1, pltpu.roll(SX[2, d], 1, 1), 0.0) - SX[2, d]
            SX[PI, d] = x - SX[1, d] + jnp.concatenate(inner, axis=0) if d else x - SX[1, d]

    def cross_send(which):
        for at in [at for at in CROSS if (at[:2] in ((0, 2), (2, 0))) == which]:
            pl.when(exists(cross_offs(*at, 1)))(lambda at=at: cross_message(*at, 1).start())

    def cross_receive():
        for at in CROSS:
            pl.when(exists(cross_offs(*at, -1)))(lambda at=at: cross_message(*at, -1).wait_recv())

    def halo_fg():
        for d in (0, 1):
            kk = place(0 if d else n0 - 1, 0, 2)[1]
            rhs = PZ[d] + S[0, n0, rows] if d else PZ[d]
            col = [pltpu.roll(RZ2[d], (2 * n2 - 2 * (kk + g) + 1) % n2, 1) for g in range(groups)]
            rhs = rhs + jnp.where(lane_full < 1, jnp.concatenate(col, axis=0), 0.0)
            first = rhs[0:8] + jnp.where(row8 < 1, RRZ[d], 0.0)
            FG[(n0 + 1) * d, rows] = jnp.concatenate([first, rhs[8:]], axis=0) * NZI[d]
        rowi = lax.broadcasted_iota(jnp.int32, (n0, n2), 0)
        lanei = lax.broadcasted_iota(jnp.int32, (n0, n2), 1)
        per = n2 // 2
        for d in (0, 1):
            rhs = RX[PI, d] + SX[1, 1] if d else RX[PI, d]
            rhs = rhs + jnp.where(rowi == 0, RRX[d], 0.0)
            index = rowi * groups + (0 if d else groups - 1)
            at = lax.rem(2 * lax.rem(index, per) + n2 - 1, n2)
            got = jnp.zeros((n0, n2), jnp.float32)
            for v in range(RX2.shape[1]):
                here = (lanei == at) & (index >= v * per) & (index < (v + 1) * per)
                got = got + jnp.where(here, RX2[d, v], 0.0)
            rhs = rhs + jnp.where(lanei < 1, jnp.sum(got, axis=1, keepdims=True), 0.0)
            RX[FGI, d] = rhs * RX[NII, d]
        ws = []
        for v, (ep, en) in enumerate(zip(edges(PI, 2), edges(NII, 2))):
            rhs = ep + jnp.where(is_low[2], SY[2, v], 0.0)
            if v == 0:
                k0 = place(n0 - 1, 0, 2)[1]
                moved = pltpu.roll(align(RZ0[0], RZ0[1], 2), (n2 - 2 * k0) % n2, 1)
                rhs = rhs + jnp.where(keys[2] < groups, moved, 0.0)
            line = align(jnp.broadcast_to(RX1[0, v], (8, n2)), jnp.broadcast_to(RX1[1, v], (8, n2)), 2)
            line = pltpu.roll(line, n2 - 2 * (groups - 1), 1)
            here = (lax.rem(keys[2], groups) == 0) & (row8 < 1)
            ws.append((rhs + jnp.where(here, line, 0.0)) * en)
        return ws

    def lines_send(which):
        for offs in [offs for offs in lines if which(offs)]:
            pl.when(exists(offs))(lambda offs=offs: line_message(offs, 1).start())

    def lines_receive():
        for offs in lines:
            pl.when(exists(offs))(lambda offs=offs: line_message(offs, -1).wait_recv())

    def align(low, high, p):
        return jnp.where(is_low[p], pltpu.roll(high, n2 - p // 2, 1), pltpu.roll(low, p // 2, 1))

    def halo_v2(ev, enl, eci):
        sh, kgroup = 2, [place(c, 0, 4) for c in (m0 - 1, 0)]
        col = [align(RZY[d, 0], RZY[d, 1], 4) for d in (0, 1)]
        for d, edge in ((0, 0), (1, m0 + 1)):
            v, kk = kgroup[d]
            near = NZ[d] + V1[1 if d == 0 else m0, rows]
            parts = [pltpu.roll(col[d], (n2 - 4 * (kk + g)) % n2, 1) for g in range(groups)]
            side = (lane_full < sh) | (lane_full >= n2 - sh)
            near = near + jnp.where(side, jnp.concatenate(parts, axis=0), 0.0)
            low = near[0:8] + jnp.where(row8 < sh, RZX[d, 0], 0.0)
            high = near[n1 - 8 : n1] + jnp.where(row8 >= 8 - sh, RZX[d, 1], 0.0)
            near = jnp.concatenate([low, near[8 : n1 - 8], high], axis=0)
            V2[edge, rows] = V1[edge, rows] - CZ[d] * near
        rowc = lax.broadcasted_iota(jnp.int32, (m0, n2), 0)
        lanec = lax.broadcasted_iota(jnp.int32, (m0, n2), 1)
        per = n2 // 4
        for d in (0, 1):
            near = RX[NLI, d, 0:m0] + SX[V1I, d, 0:m0]
            near = near + jnp.where(rowc == 0, RZX[0, d], 0.0) + jnp.where(rowc == m0 - 1, RZX[1, d], 0.0)
            for y in (0, 1):
                index = rowc * groups + (groups - 1 if d == 0 else 0)
                at = lax.rem(4 * lax.rem(index, per) + (n2 - 1 if y == 0 else 0), n2)
                got = jnp.zeros((m0, n2), jnp.float32)
                for v in range(RXY.shape[2]):
                    here = (lanec == at) & (index >= v * per) & (index < (v + 1) * per)
                    got = got + jnp.where(here, RXY[d, y, v], 0.0)
                got = jnp.sum(got, axis=1, keepdims=True)
                near = near + jnp.where((lanec < sh) if y == 0 else (lanec >= n2 - sh), got, 0.0)
            RX[V2I, d, 0:m0] = RX[V1I, d, 0:m0] - RX[CII, d, 0:m0] * near
        ws = []
        for v in range(len(ev)):
            near = enl[v] + SY[V1I, v]
            for d, c in ((0, 0), (1, m0 - 1)):
                into, k0 = place(c, 0, 4)
                if into == v:
                    shift = (4 * (k0 - kgroup[d][1])) % n2
                    moved = pltpu.roll(col[d], shift, 1) if shift else col[d]
                    near = near + jnp.where((keys[4] >= k0) & (keys[4] < k0 + groups), moved, 0.0)
            for d in (0, 1):
                line = align(
                    jnp.broadcast_to(RXY[d, 0, v], (8, n2)), jnp.broadcast_to(RXY[d, 1, v], (8, n2)), 4
                )
                jump = 4 * (groups - 1)
                line = pltpu.roll(line, n2 - jump if d == 0 else jump, 1)
                here = lax.rem(keys[4], groups) == (0 if d == 0 else groups - 1)
                here = here & ((row8 < sh) if d == 0 else (row8 >= 8 - sh))
                near = near + jnp.where(here, line, 0.0)
            ws.append(ev[v] - eci[v] * near)
        return ws

    def one(f, a, only=(0, 1)):
        ref, count = field(f)
        if a == 2:
            pack(f, lambda i: ref[1 + i, rows], count, 2)
        send(f, a, only)

    def spread_faces(f, ref, n, p):
        send(f, 0)
        faces_x(f, lambda c, r: ref[c, r : r + 1], n)
        send(f, 1)
        pack(f, lambda c: ref[c], n, p)
        send(f, 2)

    def partial_rhs():
        for i in range(n0):
            x1, x2 = S[1, 1 + i, rows], S[2, 1 + i, rows]
            rhs = jnp.where(row_full >= 1, S[1, 1 + i, pl.ds(PAD - 1, n1)], 0.0) - x1
            rhs = rhs + (jnp.where(lane_full >= 1, pltpu.roll(x2, 1, 1), 0.0) - x2)
            rhs = rhs - S[0, 1 + i, rows]
            if i > 0:
                rhs = rhs + S[0, i, rows]
            P[i] = rhs

    def invert(first, count):
        at = pl.ds(first, count)
        loads[3, first].wait()
        NI[:, at] = 1.0 / (6.0 + NI[:, at])

    def scale(k, first, count):
        at = pl.ds(first, count)
        for part in (0, 1):
            loads[k, first, part].wait()
        inv = 1.0 / D[k, :, at]
        D[k, :, at] = inv
        S[k, pl.ds(1, n0), pl.ds(PAD + first, count)] = R[k, :, at] * inv

    for first in bands:
        invert(first, 8)
    faces_x(NII, lambda i, r: NI[i, r : r + 1], n0)
    for k in (1, 2, 0):
        for first in bands:
            scale(k, first, 8)
        faces_x(k, lambda i, r: S[k, 1 + i, PAD + r : PAD + r + 1], n0)
    cross_rows()
    rows_rhs()
    pl.semaphore_wait(barrier, total)
    cross_send(False)
    send(1, 1, (1,))
    send(PI, 1)
    send(NII, 1)
    invert(8, n1 - 16)
    send(NII, 0)
    pack(NII, lambda i: NI[i], n0, 2)
    send(NII, 2)
    for k in (1, 2, 0):
        scale(k, 8, n1 - 16)
        if k == 2:
            pack(2, lambda i: S[2, 1 + i, rows], n0, 2)
            send(2, 2, (1,))
    send(0, 0, (1,))
    cross_plane()
    cross_send(True)
    partial_rhs()
    send(PI, 0)
    pack(PI, lambda i: P[i], n0, 2)
    send(PI, 2)
    loads[4].wait()
    spread_cols = (
        lax.broadcasted_iota(jnp.int32, (m2, n2), 1) // 2 == lax.broadcasted_iota(jnp.int32, (m2, n2), 0)
    ).astype(jnp.float32)
    inverse = (1.0 / (6.0 + CS[...])).reshape(m0 * m1, m2)
    inverse = jnp.dot(
        inverse, spread_cols, precision=lax.Precision.HIGHEST, preferred_element_type=jnp.float32
    ).reshape(m0, m1, n2)
    for c in range(m0):
        for r in (0, 1):
            CI[c, pl.ds(r, m1, stride=2)] = inverse[c]
    spread_faces(CII, CI, m0, 4)

    for i in range(n0):
        FG[1 + i, rows] = P[i] * NI[i]

    def gradients(j, G):
        for i in range(n0):
            x = F[j, i, 0:n1]
            above = F[j, i + 1, 0:n1] - x if i < n0 - 1 else -x
            ahead = jnp.where(lane_full >= n2 - 1, 0.0, pltpu.roll(x, n2 - 1, 1)) - x
            for k, grad in enumerate((above, F[j, i, 1 : n1 + 1] - x, ahead)):
                G[k, i] = G[k, i] + grad if j == 0 else grad


    def smooth(k):
        for a in range(3):
            receive(k, a, (0,) if (k, a) in from_low else (0, 1))
        rows_x(k, S.at[k])
        w = edges(k, 2)
        for i in range(n0):
            x = S[k, 1 + i, rows]
            near = S[k, i, rows] + S[k, i + 2, rows] + inplane(S.at[k, 1 + i], x, halo(w, i, 2), 1)
            OB[k, i] = x + near * D[k, i]

    for i in range(n0):
        F[0, i, 0:n1] = local_near(FG, i, n0, 1)

    def pair_rows(t, slot):
        t = t + jnp.where(lane_full % 2 == 0, pltpu.roll(t, n2 - 1, 1), pltpu.roll(t, 1, 1))
        T[slot, rows] = t
        return t + jnp.where(row_full % 2 == 0, T[slot, pl.ds(PAD + 1, n1)], T[slot, pl.ds(PAD - 1, n1)])

    for c in range(m0):
        CR[c] = pair_rows(F[0, 2 * c, 0:n1] + F[0, 2 * c + 1, 0:n1], c)
    from_low = ((0, 0), (1, 1), (2, 2))
    for f, a in from_low:
        receive(f, a, (1,))
    low2 = [jnp.where(is_low[2], 0.0, pltpu.roll(RY[2, 0, v], 1, 1)) for v in range(RY.shape[2])]
    add = S[0, 0, rows] * NI[0]
    T[2, rows] = add
    t = add + jnp.where(row_full >= 1, T[2, pl.ds(PAD - 1, n1)], 0.0)
    t = t + jnp.where(row_full < n1 - 1, T[2, pl.ds(PAD + 1, n1)], 0.0)
    t = t + jnp.where(lane_full >= 1, pltpu.roll(add, 1, 1), 0.0)
    t = t + jnp.where(lane_full < n2 - 1, pltpu.roll(add, n2 - 1, 1), 0.0)
    A1[0] = t
    lanei = lax.broadcasted_iota(jnp.int32, (n0, n2), 1)
    add = RX[1, 0] * SX[NII, 0]
    DX[pl.ds(PAD, n0)] = add
    x = add + DX[pl.ds(PAD - 1, n0)] + DX[pl.ds(PAD + 1, n0)]
    x = x + jnp.where(lanei >= 1, pltpu.roll(add, 1, 1), 0.0)
    SX[FGI, 0] = x + jnp.where(lanei < n2 - 1, pltpu.roll(add, n2 - 1, 1), 0.0)
    adds = [e * SY[NII, v] for v, e in enumerate(low2)]
    group, hop, per = lax.rem(keys[2], groups), 2 * groups, n2 // 2
    source = 2 * (2 * groups * (keys[4] // groups) + keys[4] % groups) + n2 - is_low[4].astype(jnp.int32)
    source = lax.rem(source, n2)
    spread = []
    for v, add in enumerate(adds):
        ahead = jnp.where(group < groups - 1, pltpu.roll(pltpu.roll(add, n2 - 2, 1), 7, 0), 0.0)
        behind = jnp.where(group > 0, pltpu.roll(pltpu.roll(add, 2, 1), 1, 0), 0.0)
        w = add + jnp.where(row8 < 7, pltpu.roll(add, 7, 0), ahead)
        w = w + jnp.where(row8 > 0, pltpu.roll(add, 1, 0), behind)
        ahead = pltpu.roll(adds[v + 1], n2 - hop, 1) if v + 1 < len(adds) else 0.0
        behind = pltpu.roll(adds[v - 1], hop, 1) if v else 0.0
        w = w + jnp.where(keys[2] < per - groups, pltpu.roll(add, n2 - hop, 1), ahead)
        w = w + jnp.where(keys[2] >= groups, pltpu.roll(add, hop, 1), behind)
        spread.append(w)
    for f in (NII, PI):
        for a in range(3):
            receive(f, a)
    cross_receive()
    ws = halo_fg()
    CR[0] = CR[0] + pair_rows(FG[0, rows] + A1[0], 0)
    CR[m0 - 1] = CR[m0 - 1] + pair_rows(FG[n0 + 1, rows], 1)
    SX[FGI, 0] = SX[FGI, 0] + RX[FGI, 0]
    SX[FGI, 1] = RX[FGI, 1]
    even = lax.broadcasted_iota(jnp.int32, (m0, n2), 1) % 2 == 0
    for d in (0, 1):
        x = SX[FGI, d, pl.ds(0, m0, stride=2)] + SX[FGI, d, pl.ds(1, m0, stride=2)]
        RX[V2I, d, 0:m0] = x + jnp.where(even, pltpu.roll(x, n2 - 1, 1), pltpu.roll(x, 1, 1))
    blocks = []
    for v, (w, add) in enumerate(zip(ws, spread)):
        w = w + add
        w = w + pltpu.roll(w, n2 - hop, 1)
        w = w + jnp.where(row8 % 2 == 0, pltpu.roll(w, 7, 0), pltpu.roll(w, 1, 0))
        blocks.append(jnp.take_along_axis(w, source, axis=1))
    side = (lane_full < 2) | (lane_full >= n2 - 2)
    for c in range(m0):
        t = CR[c] + jnp.where(side, halo(blocks, c, 4), 0.0)
        low = t[0:8] + jnp.where(row8 < 2, RX[V2I, 0, c : c + 1], 0.0)
        high = t[n1 - 8 : n1] + jnp.where(row8 >= 6, RX[V2I, 1, c : c + 1], 0.0)
        t = jnp.concatenate([low, t[8 : n1 - 8], high], axis=0)
        CR[c] = t
        V1[1 + c, rows] = t * CI[c]
    rowc = lax.broadcasted_iota(jnp.int32, (m0, n2), 0)
    lanec = lax.broadcasted_iota(jnp.int32, (m0, n2), 1)
    faces_x(V1I, lambda c, r: V1[1 + c, PAD + r : PAD + r + 1], m0)
    for z in (0, 1):
        for x in (0, 1):
            c = (m0 - 1) * z
            LZX[z, x] = SX[V1I, x, c : c + 1]
    for x in (0, 1):
        g = (groups - 1) * x
        ends = [((c, g), V1[1 + c, PAD + 8 * g : PAD + 8 * g + 8]) for c in range(m0)]
        for v, acc in gather(ends, 4).items():
            LXY[x, v] = acc[7 * x : 7 * x + 1]
    lines_send(lambda offs: offs[1] != 0)
    send(V1I, 1)
    for d, r in ((0, 2), (1, n1 - 3)):
        x = SX[V1I, d, 0:m0]
        near = jnp.concatenate([V1[1 + c, PAD + r : PAD + r + 1] for c in range(m0)], axis=0)
        near = near + jnp.where(rowc >= 1, pltpu.roll(x, 1, 0), 0.0)
        near = near + jnp.where(rowc < m0 - 1, pltpu.roll(x, m0 - 1, 0), 0.0)
        near = near + jnp.where(lanec >= 2, pltpu.roll(x, 2, 1), 0.0)
        SX[NLI, d, 0:m0] = near + jnp.where(lanec < n2 - 2, pltpu.roll(x, n2 - 2, 1), 0.0)
    send(NLI, 1)
    send(V1I, 0)
    pack(V1I, lambda c: V1[1 + c, rows], m0, 4)
    lines_send(lambda offs: offs[1] == 0)
    send(V1I, 2)
    for c in range(m0):
        NL[c] = local_near(V1, c, m0, 2)
    send(NLI, 0)
    pack(NLI, lambda c: NL[c], m0, 4)
    send(NLI, 2)

    def faces_f(j):
        f = F0I + j
        send(f, 0)
        faces_x(f, lambda i, r: F[j, i, r : r + 1], n0)
        send(f, 1)
        pack(f, lambda i: F[j, i, 0:n1], n0, 2)
        send(f, 2)

    for f, a in ((0, 1), (2, 1), (1, 0), (2, 0), (0, 2), (1, 2)):
        one(f, a)
    for f, a in from_low:
        send(f, a, (0,))
    for i in range(n0):
        rhs = P[i] + jnp.where(lane_full < 1, halo(low2, i, 2), 0.0)
        if i == 0:
            rhs = rhs + S[0, 0, rows]
        first = rhs[0:8] + jnp.where(row8 < 1, RX[1, 0, i : i + 1], 0.0)
        FG[1 + i, rows] = jnp.concatenate([first, rhs[8:]], axis=0) * NI[i]
    for i in range(n0):
        near = outer_near(local_near(FG, i, n0, 1), FG, FGI, ws, i, n0, 2)
        F[0, i, 0:n1] = FG[1 + i, rows] + near * NI[i]
    faces_f(0)

    def fold(x):
        acc = x[0:8]
        for g in range(1, groups):
            acc = acc + x[8 * g : 8 * g + 8]
        return acc

    sums = [jnp.zeros((8, n2), jnp.float32) for _ in range(4)]
    for c in range(m0):
        sums[0] = sums[0] + fold(V1[1 + c, rows] * CR[c])

    for f in (CII, V1I, NLI):
        for a in range(3):
            receive(f, a)
    lines_receive()
    ws = edges(V1I, 4)
    for c in range(m0):
        near = outer_near(NL[c], V1, V1I, ws, c, m0, 4)
        A1[c] = CR[c] - near
        V2[1 + c, rows] = V1[1 + c, rows] - near * CI[c]
    faces_x(V2I, lambda c, r: V2[1 + c, PAD + r : PAD + r + 1], m0)
    pack(V2I, lambda c: V2[1 + c, rows], m0, 4)
    w2 = halo_v2(ws, edges(NLI, 4), edges(CII, 4))

    def spread_near(j, V, w):
        for c in range(m0):
            x = V[1 + c, rows]
            near = x + inplane(V.at[1 + c], x, halo(w, c, 4), 1)
            F[j, 2 * c, 0:n1] = (near + V[c, rows]) * NI[2 * c]
            F[j, 2 * c + 1, 0:n1] = (near + V[c + 2, rows]) * NI[2 * c + 1]
        faces_f(j)

    for c in range(m0):
        v1, v2, a1 = V1[1 + c, rows], V2[1 + c, rows], A1[c]
        near = jnp.where(row_full < n1 - 2, V2[1 + c, pl.ds(PAD + 2, n1)], 0.0)
        near = near + jnp.where(lane_full < n2 - 2, pltpu.roll(v2, n2 - 2, 1), 0.0)
        if c < m0 - 1:
            near = near + V2[2 + c, rows]
        sums[1] = sums[1] + fold(v1 * a1)
        sums[2] = sums[2] + fold(v2 * a1)
        sums[3] = sums[3] + fold(v2 * (a1 - 2.0 * near))
    outer = fold(V2[1, rows] * V2[0, rows] + V2[m0, rows] * V2[m0 + 1, rows])
    for v, w in enumerate(w2):
        outer = outer + SY[V2I, v] * w
    rim = SX[V2I, 0, 0:m0] * RX[V2I, 0, 0:m0] + SX[V2I, 1, 0:m0] * RX[V2I, 1, 0:m0]
    sums[3] = sums[3] - outer
    rim = 2.0 * jnp.sum(rim, axis=0, keepdims=True)
    sums[3] = sums[3] - jnp.where(row8 == 0, rim, 0.0)
    lane1 = lax.broadcasted_iota(jnp.int32, (1, n2), 1)
    part = jnp.zeros((1, n2), jnp.float32)
    for q, s in enumerate(sums):
        part = jnp.where(lane1 == q, jnp.sum(jnp.sum(s, axis=0, keepdims=True), axis=1, keepdims=True), part)

    def slot(axes, at):
        index = 0
        for a in axes:
            index = index * sizes[a] + at(a)
        return index

    def sum_message(p, offs, sign):
        axes, slots = phases[p], slots_of[p]
        other = partner(axes, offs, sign)
        index = slot(axes, (lambda a: me[a]) if sign > 0 else (lambda a: other[AXES[a]]))
        sem = p * slots_of[0].shape[0] + slot(axes, lambda a: offs[axes.index(a)])
        return pltpu.make_async_remote_copy(
            src_ref=slots.at[index], dst_ref=slots.at[index], send_sem=psend.at[sem], recv_sem=precv.at[sem],
            device_id=other, device_id_type=MESH,
        )

    def sum_start(p, value):
        slots_of[p][slot(phases[p], lambda a: me[a])] = value
        for offs in offsets(phases[p]):
            sum_message(p, offs, 1).start()

    def sum_end(p):
        for offs in offsets(phases[p]):
            sum_message(p, offs, -1).wait_recv()
        terms = [slots_of[p][d] for d in range(slots_of[p].shape[0])]
        while len(terms) > 1:
            terms = [functools.reduce(lambda x, y: x + y, terms[t : t + 2]) for t in range(0, len(terms), 2)]
        return terms[0]

    sum_start(0, part)
    rows_x(V2I, V2)
    spread_near(2, V2, w2)
    rows_x(V1I, V1)
    spread_near(1, V1, ws)
    gradients(1, G1)
    gradients(2, G2)
    for k in (1, 2, 0):
        smooth(k)
    gradients(0, OB)

    def drain(fields):
        for a in range(3):
            for d in (0, 1):
                def over(a=a, d=d):
                    for f in fields:
                        if f not in LOCAL and d in dirs(f):
                            message(f, a, d).wait_send()
                pl.when(can_send(a, d))(over)

    drain([f for f in range(FIELDS) if f not in FINAL])
    for offs in lines:
        pl.when(exists(offs))(lambda offs=offs: line_message(offs, 1).wait_send())
    for at in CROSS:
        pl.when(exists(cross_offs(*at, 1)))(lambda at=at: cross_message(*at, 1).wait_send())

    part = sum_end(0)
    for p in range(1, len(phases)):
        sum_start(p, part)
        part = sum_end(p)
    gone, hone, hmix, htwo = [
        jnp.sum(jnp.where(lane1 == q, part, 0.0), axis=1, keepdims=True) for q in range(4)
    ]
    two = (hone - hmix * gone / hone) / (htwo - hmix * hmix / hone)
    oneco = (gone - hmix * two) / hone
    CO[0:1] = jnp.broadcast_to(oneco, (1, n2))
    CO[1:2] = jnp.broadcast_to(two, (1, n2))
    for f in FINAL:
        for a in range(3):
            receive(f, a)

    def mix(get):
        a = get(0)
        return a + jnp.broadcast_to(oneco, a.shape) * get(1) + jnp.broadcast_to(two, a.shape) * get(2)

    MZ[...] = mix(lambda j: F[j, n0, 0:n1])
    MX[...] = mix(lambda j: RX[F0I + j, 1])
    for v in range(RY.shape[2]):
        MY[v] = pltpu.roll(mix(lambda j: RY[F0I + j, 1, v]), n2 - 1, 1)

    for p in range(len(phases)):
        for offs in offsets(phases[p]):
            sum_message(p, offs, 1).wait_send()
    drain(FINAL)


def combine(parts, OB, G1, G2, CO, MZ, MX, MY, out, W, sem):
    _, n0, n1, n2 = OB.shape
    one = jnp.broadcast_to(CO[0:1], (n1, n2))
    two = jnp.broadcast_to(CO[1:2], (n1, n2))
    groups, per, step = n1 // 8, n2 // 2, n0 // parts
    row8 = lax.broadcasted_iota(jnp.int32, (8, n2), 0)
    lane_full = lax.broadcasted_iota(jnp.int32, (n1, n2), 1)

    def edge(k, i, x):
        if k == 0:
            return x + MZ[...] if i == n0 - 1 else x
        if k == 1:
            last = x[n1 - 8 : n1] + jnp.where(row8 == 7, MX[i : i + 1], 0.0)
            return jnp.concatenate([x[0 : n1 - 8], last], axis=0)
        ats = [divmod(i * groups + g, per) for g in range(groups)]
        parts = [pltpu.roll(MY[v], (n2 - 2 * kk) % n2, 1) for v, kk in ats]
        return x + jnp.where(lane_full >= n2 - 1, jnp.concatenate(parts, axis=0), 0.0)

    copies = []
    for k in range(3):
        for h in range(parts):
            for i in range(h * step, (h + 1) * step):
                W[k, i] = edge(k, i, OB[k, i] + one * G1[k, i] + two * G2[k, i])
            planes = pl.ds(h * step, step)
            copies.append(pltpu.make_async_copy(W.at[k, planes], out.at[k, planes], sem.at[k * parts + h]))
            copies[-1].start()
    for c in copies:
        c.wait()


def solution(mesh):
    sizes = tuple(mesh.shape[a] for a in AXES)

    def local(residual, edge_diag, node_shift, coarse_shift):
        n0, n1, n2 = node_shift.shape
        m0, m1, m2 = coarse_shift.shape
        vecs = max(-(-(n0 * (n1 // 8)) // (n2 // 2)), -(-(m0 * (n1 // 8)) // (n2 // 4)))
        f32 = jnp.float32
        counts = [math.prod(sizes[a] for a in axes) for axes in phases_of(sizes)]
        V = lambda *s: pltpu.VMEM(s, f32)
        scratch = [
            V(3, n0, n1, n2), V(3, n0, n1, n2), V(n0, n1, n2), V(m0, m1, m2),
            V(3, n0 + 2, n1 + 2 * PAD, n2), V(n0 + 2, n1 + 2 * PAD, n2),
            V(m0, n1, n2), V(m0, n1, n2), V(m0, n1, n2), V(m0, n1, n2), V(m0, n1 + 2 * PAD, n2),
            V(m0 + 2, n1 + 2 * PAD, n2), V(m0 + 2, n1 + 2 * PAD, n2),
            V(3, n0 + 1, n1 + PAD, n2),
            V(FIELDS, 2, n0, n2), V(FIELDS, 2, n0, n2), V(FIELDS, vecs, 8, n2), V(FIELDS, 2, vecs, 8, n2),
            V(2, n1, n2), V(2, n1, n2), V(2, 2, 1, n2), V(2, vecs, 1, n2),
            V(2, 2, 1, n2), V(2, 2, 8, n2), V(2, 2, vecs, 1, n2),
            V(n0, n1, n2), V(2, n1, n2), V(2, n1, n2), V(2, 1, n2), V(2, 1, n2), V(2, vecs, 1, n2), V(vecs, 1, n2),
            V(8, n2), V(2, 1, n2), V(2, 1, n2), V(2, 8, n2), V(2, 8, n2), V(2, vecs, 1, n2), V(2, vecs, 1, n2), V(n0 + 2 * PAD, n2),
            *[V(c, 1, n2) for c in counts],
        ]
        sems = [pltpu.SemaphoreType.DMA(s) for s in ((22,), *[(FIELDS, 3, 2)] * 2, *[(sum(counts),)] * 2, *[(12,)] * 4)]

        def scoped(*refs):
            plain, slots_of = refs[: -len(counts)], refs[-len(counts) :]
            pl.run_scoped(functools.partial(kernel, sizes, *plain, slots_of), *sems)

        field = pltpu.VMEM(residual.shape, f32)
        limit = 67_043_328 - 12 * math.prod(residual.shape) - 2**18
        fields = pl.pallas_call(
            scoped,
            out_shape=[field] * 3 + [pltpu.VMEM(s, f32) for s in ((8, n2), (n1, n2), (n0, n2), (vecs, 8, n2))],
            in_specs=[pl.BlockSpec(memory_space=pltpu.HBM)] * 4,
            out_specs=[pl.BlockSpec(memory_space=pltpu.VMEM)] * 7,
            scratch_shapes=scratch,
            compiler_params=pltpu.CompilerParams(collective_id=0, has_side_effects=True, vmem_limit_bytes=limit),
        )(residual, edge_diag, node_shift, coarse_shift)
        parts = 2 if n0 % 2 == 0 else 1
        return pl.pallas_call(
            functools.partial(combine, parts),
            out_shape=jax.ShapeDtypeStruct(residual.shape, f32),
            in_specs=[pl.BlockSpec(memory_space=pltpu.VMEM)] * 7,
            out_specs=pl.BlockSpec(memory_space=pltpu.HBM),
            scratch_shapes=[field, pltpu.SemaphoreType.DMA((3 * parts,))],
            compiler_params=pltpu.CompilerParams(vmem_limit_bytes=8 * math.prod(residual.shape)),
        )(*fields)

    placed = (
        P(None, "gz", "gx", "gy"),
        P(None, "gz", "gx", "gy"),
        P("gz", "gx", "gy"),
        P("gz", "gx", "gy"),
    )
    return jax.shard_map(
        local, mesh=mesh, in_specs=placed, out_specs=P(None, "gz", "gx", "gy"), check_vma=False
    )
```

```python
import functools
import itertools
import math

import jax
import jax.numpy as jnp
from jax import lax
from jax.experimental import pallas as pl
from jax.experimental.pallas import tpu as pltpu
from jax.sharding import PartitionSpec as P

MESH = pl.DeviceIdType.MESH
AXES = ("gz", "gx", "gy")
PI, V1I, V2I, F0I, NLI, CII, NII, FGI = 3, 4, 5, 6, 9, 10, 11, 12
FIELDS = 13
FINAL = (F0I, F0I + 1, F0I + 2)
COARSE = (V1I, V2I, NLI, CII)
LOCAL = (V2I, FGI)
CROSS = [(a, b, d) for a in range(3) for b in range(3) if a != b for d in (0, 1)]
GREET = [(a, b, 2) for a in range(3) for b in range(a)]
PAD = 8
FEW = 32


def fence():
    pl.delay(1)


def phases_of(sizes):
    return ((0, 1, 2),) if math.prod(sizes) <= FEW else ((1, 2), (0,))


def greeted(sizes, rounds):
    near = set(itertools.product((-1, 0, 1), repeat=3))
    known = set(near)
    for moves in rounds:
        known |= {tuple(p + q for p, q in zip(k, m)) for k in known for m in moves}
    needed = set()
    for axes in phases_of(sizes):
        spans = [range(1 - sizes[a], sizes[a]) if a in axes else (0,) for a in range(3)]
        needed |= set(itertools.product(*spans))
    every = near | (needed - known)
    return sorted(o for o in every if any(o) and all(abs(p) < n for p, n in zip(o, sizes)))


def kernel(
    sizes,
    res, dia, shf, csh, OB, G1, G2, CO, MZ, MX, MY,
    R, D, NI, CS, S, FG, CI, CR, A1, NL, T, V1, V2, F,
    SX, RX, SY, RY, NZ, CZ, LZX, LXY, RZX, RZY, RXY,
    P, PZ, NZI, LRZ, LRX, LY2, LY1, LP0, RRZ, RRX, RZ2, RZ0, RX2, RX1, DX, HELLO,
    slots_of,
    in_sem, send_sem, recv_sem, psend, precv, lsend, lrecv, csend, crecv,
):
    phases = phases_of(sizes)
    n0, n1, n2 = NI.shape
    m0, m1, m2 = CS.shape
    groups = n1 // 8
    me = [lax.axis_index(a) for a in AXES]
    rows = pl.ds(PAD, n1)

    def offsets(axes):
        every = itertools.product(*[range(sizes[a]) for a in axes])
        return [offs for offs in every if any(offs)]

    def partner(axes, offs, sign):
        return {
            AXES[a]: lax.rem(me[a] + (o if sign > 0 else sizes[a] - o), sizes[a]) for a, o in zip(axes, offs)
        }

    barrier = pltpu.get_barrier_semaphore()
    faces = [offs for offs in itertools.product((-1, 0, 1), repeat=3) if sum(map(abs, offs)) == 1]
    lines = [offs for offs in itertools.product((-1, 0, 1), repeat=3) if sum(map(abs, offs)) == 2]

    def exists(offs):
        inside = [(me[a] + o >= 0) & (me[a] + o < sizes[a]) for a, o in enumerate(offs) if o]
        return functools.reduce(jnp.logical_and, inside)

    def device(offs):
        return {AXES[a]: me[a] + o for a, o in enumerate(offs) if o}

    total = jnp.int32(0)
    for offs in greeted(sizes, (faces + lines, faces + lines)):
        there = exists(offs)
        pl.when(there)(
            lambda offs=offs: pl.semaphore_signal(
                barrier, inc=1, device_id=device(offs), device_id_type=MESH
            )
        )
        total = total + there.astype(jnp.int32)

    bands = (0, n1 - 8)
    loads = {}

    def load(key, src, dst):
        loads[key] = pltpu.make_async_copy(src, dst, in_sem.at[len(loads)])
        loads[key].start()

    load(3, shf, NI)
    for first, count in [(r, 8) for r in bands] + [(8, n1 - 16)]:
        at = pl.ds(first, count)
        for k in (1, 2, 0):
            load((k, first, 0), res.at[k, :, at], R.at[k, :, at])
            load((k, first, 1), dia.at[k, :, at], D.at[k, :, at])
    load(4, csh, CS)

    for k in range(3):
        for i in range(n0):
            F[k, i, n1 : n1 + 1] = jnp.zeros((1, n2), jnp.float32)
    DX[...] = jnp.zeros(DX.shape, jnp.float32)

    def clear(offs, *refs):
        @pl.when(jnp.logical_not(exists(offs)))
        def _():
            for ref in refs:
                ref[...] = jnp.zeros(ref.shape, jnp.float32)

    for d in (0, 1):
        step, i, c = (1, n0 + 1, m0 + 1) if d else (-1, 0, 0)
        planes = [S.at[k, i, rows] for k in range(3)] + [V1.at[c, rows], NZ.at[d], CZ.at[d], PZ.at[d], NZI.at[d]]
        clear((step, 0, 0), *planes, *([F.at[k, n0, pl.ds(0, n1)] for k in range(3)] if d else []))
        clear((0, step, 0), *[RX.at[f, d] for f in range(FIELDS) if f not in LOCAL])
        clear((0, 0, step), *[RY.at[f, d] for f in range(FIELDS) if f not in LOCAL])
    for offs in lines:
        z, x, y = [int(o > 0) for o in offs]
        clear(offs, RXY.at[x, y] if not offs[0] else RZY.at[z, y] if not offs[1] else RZX.at[z, x])

    lane = lax.broadcasted_iota(jnp.int32, (8, n2), 1)
    lane_full = lax.broadcasted_iota(jnp.int32, (n1, n2), 1)
    row_full = lax.broadcasted_iota(jnp.int32, (n1, n2), 0)
    row8 = lax.broadcasted_iota(jnp.int32, (8, n2), 0)
    keys = {p: ((lane + p // 2) // p) % (n2 // p) for p in (2, 4)}
    is_low = {p: (lane % p) >= p // 2 for p in (2, 4)}

    def place(i, g, p):
        k = i * groups + g
        per = n2 // p
        return k // per, k % per

    def gather(blocks, p):
        accs = {}
        for (i, g), part in blocks:
            v, kk = place(i, g, p)
            if kk:
                part = pltpu.roll(part, p * kk, 1)
            accs[v] = jnp.where(keys[p] == kk, part, accs.get(v, 0.0))
        return accs

    def pack(f, plane, count, p):
        at = [(i, g) for i in range(count) for g in range(groups)]
        planes = [plane(i) for i in range(count)]
        accs = gather([((i, g), planes[i][8 * g : 8 * g + 8]) for i, g in at], p)
        for v, acc in accs.items():
            SY[f, v] = acc

    def halo(ws, i, p):
        parts = []
        for g in range(groups):
            v, kk = place(i, g, p)
            parts.append(pltpu.roll(ws[v], n2 - p * kk, 1) if kk else ws[v])
        return jnp.concatenate(parts, axis=0)

    def inplane(ref, x, h, sh):
        near = ref[pl.ds(PAD - sh, n1)] + ref[pl.ds(PAD + sh, n1)]
        near = near + jnp.where(lane_full < sh, h, pltpu.roll(x, sh, 1))
        return near + jnp.where(lane_full >= n2 - sh, h, pltpu.roll(x, n2 - sh, 1))

    def local_near(ref, i, n, sh):
        x = ref[1 + i, rows]
        near = jnp.where(row_full >= sh, ref[1 + i, pl.ds(PAD - sh, n1)], 0.0)
        near = near + jnp.where(row_full < n1 - sh, ref[1 + i, pl.ds(PAD + sh, n1)], 0.0)
        near = near + jnp.where(lane_full >= sh, pltpu.roll(x, sh, 1), 0.0)
        near = near + jnp.where(lane_full < n2 - sh, pltpu.roll(x, n2 - sh, 1), 0.0)
        if i > 0:
            near = near + ref[i, rows]
        if i < n - 1:
            near = near + ref[i + 2, rows]
        return near

    def edges(f, p):
        sh = p // 2
        return [
            jnp.where(is_low[p], pltpu.roll(RY[f, 1, v], n2 - sh, 1), pltpu.roll(RY[f, 0, v], sh, 1))
            for v in range(RY.shape[2])
        ]

    def outer_near(near, ref, f, ws, i, n, p):
        sh = p // 2
        if i == 0:
            near = near + ref[0, rows]
        if i == n - 1:
            near = near + ref[n + 1, rows]
        side = (lane_full < sh) | (lane_full >= n2 - sh)
        near = near + jnp.where(side, halo(ws, i, p), 0.0)
        low = near[0:8] + jnp.where(row8 < sh, RX[f, 0, i : i + 1], 0.0)
        high = near[n1 - 8 : n1] + jnp.where(row8 >= 8 - sh, RX[f, 1, i : i + 1], 0.0)
        return jnp.concatenate([low, near[8 : n1 - 8], high], axis=0)

    def field(f):
        if f < 3:
            return S.at[f], n0
        return {V1I: (V1, m0)}[f]

    ZBUF = {NLI: (NL, NZ, m0), CII: (CI, CZ, m0), PI: (P, PZ, n0), NII: (NI, NZI, n0)}

    def message(f, a, d):
        if a == 0:
            if f in FINAL:
                src, dst = F.at[f - F0I, 0, pl.ds(0, n1)], F.at[f - F0I, n0, pl.ds(0, n1)]
            elif f in ZBUF:
                src, dst, n = ZBUF[f]
                src, dst = src.at[n - 1 if d else 0], dst.at[1 - d]
            else:
                ref, n = field(f)
                src = ref.at[n if d else 1, rows]
                dst = ref.at[0 if d else n + 1, rows]
        elif a == 1:
            count = m0 if f in COARSE else n0
            src, dst = SX.at[f, d, pl.ds(0, count)], RX.at[f, 1 - d, pl.ds(0, count)]
        else:
            src, dst = SY.at[f], RY.at[f, 1 - d]
        step = 1 if d else -1
        return pltpu.make_async_remote_copy(
            src_ref=src, dst_ref=dst, send_sem=send_sem.at[f, a, d], recv_sem=recv_sem.at[f, a, d],
            device_id={AXES[a]: lax.rem(me[a] + step + sizes[a], sizes[a])}, device_id_type=MESH,
        )

    def dirs(f):
        return (0,) if f in FINAL else (0, 1)

    def can_send(a, d):
        return me[a] < sizes[a] - 1 if d else me[a] > 0

    def send(f, a, only=(0, 1)):
        for d in [d for d in dirs(f) if d in only]:
            pl.when(can_send(a, d))(lambda f=f, a=a, d=d: message(f, a, d).start())

    def receive(f, a, only=(0, 1)):
        for d in [d for d in dirs(f) if d in only]:
            pl.when(can_send(a, 1 - d))(lambda f=f, a=a, d=d: message(f, a, d).wait_recv())

    def faces_x(f, get, count):
        for i in range(count):
            SX[f, 0, i : i + 1] = get(i, 0)
            if f not in FINAL:
                SX[f, 1, i : i + 1] = get(i, n1 - 1)

    def rows_x(f, ref):
        width = 2 if f in COARSE else 1
        for i in range(m0 if f in COARSE else n0):
            for w in range(width):
                ref[1 + i, PAD - 1 - w : PAD - w] = RX[f, 0, i : i + 1]
                ref[1 + i, PAD + n1 + w : PAD + n1 + w + 1] = RX[f, 1, i : i + 1]

    def line_message(offs, sign):
        z, x, y = [o * sign for o in offs]
        side = [0 if o > 0 else 1 for o in (z, x, y)]
        if not y:
            src, dst = LZX.at[1 - side[0], 1 - side[1]], RZX.at[side[0], side[1]]
        elif not x:
            plane = place(m0 - 1 if z > 0 else 0, 0, 4)[0]
            src, dst = SY.at[V1I, plane], RZY.at[side[0], side[2]]
        else:
            src, dst = LXY.at[1 - side[1]], RXY.at[side[1], side[2]]
        at = lines.index((z, x, y))
        return pltpu.make_async_remote_copy(
            src_ref=src, dst_ref=dst, send_sem=lsend.at[at], recv_sem=lrecv.at[at],
            device_id=device((z, x, y)), device_id_type=MESH,
        )

    def cross_message(a, b, d, sign):
        src, dst = (LRZ.at[0], HELLO.at[a + b - 1]) if d == 2 else {
            (0, 1): (LRZ.at[d], RRZ.at[d]),
            (1, 0): (LRX.at[d], RRX.at[d]),
            (0, 2): (SY.at[2, place(0 if d else n0 - 1, 0, 2)[0]], RZ2.at[d]),
            (2, 0): (LP0, RZ0.at[d]),
            (1, 2): (LY2.at[d], RX2.at[d]),
            (2, 1): (LY1, RX1.at[d]),
        }[a, b]
        at = (CROSS + GREET).index((a, b, d))
        return pltpu.make_async_remote_copy(
            src_ref=src, dst_ref=dst, send_sem=csend.at[at], recv_sem=crecv.at[at],
            device_id=device(cross_offs(a, b, d, sign)), device_id_type=MESH,
        )

    def cross_offs(a, b, d, sign):
        offs = [0, 0, 0]
        offs[a], offs[b] = (-sign if d else sign), (-sign if d == 2 else sign)
        return tuple(offs)

    CROSS_INTO = {(0, 1): RRZ, (1, 0): RRX, (0, 2): RZ2, (2, 0): RZ0, (1, 2): RX2, (2, 1): RX1}
    for a, b, d in CROSS:
        clear(cross_offs(a, b, d, -1), CROSS_INTO[a, b].at[d])

    def cross_rows():
        for d in (0, 1):
            i, r = (0 if d else n0 - 1), (0 if d else n1 - 1)
            LRZ[d] = S[1, 1 + i, PAD + n1 - 1 : PAD + n1]
            LRX[d] = S[0, n0, PAD + r : PAD + r + 1]
        for k, g in ((2, groups - 1), (2, 0), (1, groups - 1)):
            top = [((i, g), S[k, 1 + i, PAD + 8 * g : PAD + 8 * g + 8]) for i in range(n0)]
            for v, acc in gather(top, 2).items():
                line = acc[7:8] if g else acc[0:1]
                if k == 2:
                    LY2[0 if g else 1, v] = line
                else:
                    LY1[v] = line

    def cross_plane():
        top = [((n0 - 1, g), S[0, n0, PAD + 8 * g : PAD + 8 * g + 8]) for g in range(groups)]
        for acc in gather(top, 2).values():
            LP0[...] = acc

    def rows_rhs():
        rowi = lax.broadcasted_iota(jnp.int32, (n0, n2), 0)
        lanei = lax.broadcasted_iota(jnp.int32, (n0, n2), 1)
        inner = [S[1, 1 + i, PAD + n1 - 2 : PAD + n1 - 1] for i in range(n0)]
        for d in (0, 1):
            x = jnp.where(rowi >= 1, pltpu.roll(SX[0, d], 1, 0), 0.0) - SX[0, d]
            x = x + jnp.where(lanei >= 1, pltpu.roll(SX[2, d], 1, 1), 0.0) - SX[2, d]
            SX[PI, d] = x - SX[1, d] + jnp.concatenate(inner, axis=0) if d else x - SX[1, d]

    def cross_send(which):
        for at in [at for at in CROSS + GREET if (at[:2] in ((0, 2), (2, 0)) and at[2] < 2) == which]:
            pl.when(exists(cross_offs(*at, 1)))(lambda at=at: cross_message(*at, 1).start())

    def cross_receive():
        for at in CROSS + GREET:
            pl.when(exists(cross_offs(*at, -1)))(lambda at=at: cross_message(*at, -1).wait_recv())

    def halo_fg():
        for d in (0, 1):
            kk = place(0 if d else n0 - 1, 0, 2)[1]
            rhs = PZ[d] + S[0, n0, rows] if d else PZ[d]
            col = [pltpu.roll(RZ2[d], (2 * n2 - 2 * (kk + g) + 1) % n2, 1) for g in range(groups)]
            rhs = rhs + jnp.where(lane_full < 1, jnp.concatenate(col, axis=0), 0.0)
            first = rhs[0:8] + jnp.where(row8 < 1, RRZ[d], 0.0)
            FG[(n0 + 1) * d, rows] = jnp.concatenate([first, rhs[8:]], axis=0) * NZI[d]
        rowi = lax.broadcasted_iota(jnp.int32, (n0, n2), 0)
        lanei = lax.broadcasted_iota(jnp.int32, (n0, n2), 1)
        per = n2 // 2
        for d in (0, 1):
            rhs = RX[PI, d] + SX[1, 1] if d else RX[PI, d]
            rhs = rhs + jnp.where(rowi == 0, RRX[d], 0.0)
            index = rowi * groups + (0 if d else groups - 1)
            at = lax.rem(2 * lax.rem(index, per) + n2 - 1, n2)
            got = jnp.zeros((n0, n2), jnp.float32)
            for v in range(RX2.shape[1]):
                here = (lanei == at) & (index >= v * per) & (index < (v + 1) * per)
                got = got + jnp.where(here, RX2[d, v], 0.0)
            rhs = rhs + jnp.where(lanei < 1, jnp.sum(got, axis=1, keepdims=True), 0.0)
            RX[FGI, d] = rhs * RX[NII, d]
        ws = []
        for v, (ep, en) in enumerate(zip(edges(PI, 2), edges(NII, 2))):
            rhs = ep + jnp.where(is_low[2], SY[2, v], 0.0)
            if v == 0:
                k0 = place(n0 - 1, 0, 2)[1]
                moved = pltpu.roll(align(RZ0[0], RZ0[1], 2), (n2 - 2 * k0) % n2, 1)
                rhs = rhs + jnp.where(keys[2] < groups, moved, 0.0)
            line = align(jnp.broadcast_to(RX1[0, v], (8, n2)), jnp.broadcast_to(RX1[1, v], (8, n2)), 2)
            line = pltpu.roll(line, n2 - 2 * (groups - 1), 1)
            here = (lax.rem(keys[2], groups) == 0) & (row8 < 1)
            ws.append((rhs + jnp.where(here, line, 0.0)) * en)
        return ws

    def lines_send(which):
        for offs in [offs for offs in lines if which(offs)]:
            pl.when(exists(offs))(lambda offs=offs: line_message(offs, 1).start())

    def lines_receive():
        for offs in lines:
            pl.when(exists(offs))(lambda offs=offs: line_message(offs, -1).wait_recv())

    def align(low, high, p):
        return jnp.where(is_low[p], pltpu.roll(high, n2 - p // 2, 1), pltpu.roll(low, p // 2, 1))

    def halo_v2(ev, enl, eci):
        sh, kgroup = 2, [place(c, 0, 4) for c in (m0 - 1, 0)]
        col = [align(RZY[d, 0], RZY[d, 1], 4) for d in (0, 1)]
        for d, edge in ((0, 0), (1, m0 + 1)):
            v, kk = kgroup[d]
            near = NZ[d] + V1[1 if d == 0 else m0, rows]
            parts = [pltpu.roll(col[d], (n2 - 4 * (kk + g)) % n2, 1) for g in range(groups)]
            side = (lane_full < sh) | (lane_full >= n2 - sh)
            near = near + jnp.where(side, jnp.concatenate(parts, axis=0), 0.0)
            low = near[0:8] + jnp.where(row8 < sh, RZX[d, 0], 0.0)
            high = near[n1 - 8 : n1] + jnp.where(row8 >= 8 - sh, RZX[d, 1], 0.0)
            near = jnp.concatenate([low, near[8 : n1 - 8], high], axis=0)
            V2[edge, rows] = V1[edge, rows] - CZ[d] * near
        rowc = lax.broadcasted_iota(jnp.int32, (m0, n2), 0)
        lanec = lax.broadcasted_iota(jnp.int32, (m0, n2), 1)
        per = n2 // 4
        for d in (0, 1):
            near = RX[NLI, d, 0:m0] + SX[V1I, d, 0:m0]
            near = near + jnp.where(rowc == 0, RZX[0, d], 0.0) + jnp.where(rowc == m0 - 1, RZX[1, d], 0.0)
            for y in (0, 1):
                index = rowc * groups + (groups - 1 if d == 0 else 0)
                at = lax.rem(4 * lax.rem(index, per) + (n2 - 1 if y == 0 else 0), n2)
                got = jnp.zeros((m0, n2), jnp.float32)
                for v in range(RXY.shape[2]):
                    here = (lanec == at) & (index >= v * per) & (index < (v + 1) * per)
                    got = got + jnp.where(here, RXY[d, y, v], 0.0)
                got = jnp.sum(got, axis=1, keepdims=True)
                near = near + jnp.where((lanec < sh) if y == 0 else (lanec >= n2 - sh), got, 0.0)
            RX[V2I, d, 0:m0] = RX[V1I, d, 0:m0] - RX[CII, d, 0:m0] * near
        ws = []
        for v in range(len(ev)):
            near = enl[v] + SY[V1I, v]
            for d, c in ((0, 0), (1, m0 - 1)):
                into, k0 = place(c, 0, 4)
                if into == v:
                    shift = (4 * (k0 - kgroup[d][1])) % n2
                    moved = pltpu.roll(col[d], shift, 1) if shift else col[d]
                    near = near + jnp.where((keys[4] >= k0) & (keys[4] < k0 + groups), moved, 0.0)
            for d in (0, 1):
                line = align(
                    jnp.broadcast_to(RXY[d, 0, v], (8, n2)), jnp.broadcast_to(RXY[d, 1, v], (8, n2)), 4
                )
                jump = 4 * (groups - 1)
                line = pltpu.roll(line, n2 - jump if d == 0 else jump, 1)
                here = lax.rem(keys[4], groups) == (0 if d == 0 else groups - 1)
                here = here & ((row8 < sh) if d == 0 else (row8 >= 8 - sh))
                near = near + jnp.where(here, line, 0.0)
            ws.append(ev[v] - eci[v] * near)
        return ws

    def one(f, a, only=(0, 1)):
        ref, count = field(f)
        if a == 2:
            pack(f, lambda i: ref[1 + i, rows], count, 2)
        send(f, a, only)

    def spread_faces(f, ref, n, p):
        send(f, 0)
        faces_x(f, lambda c, r: ref[c, r : r + 1], n)
        send(f, 1)
        pack(f, lambda c: ref[c], n, p)
        send(f, 2)

    def shifted(i):
        return jnp.where(lane_full >= 1, pltpu.roll(S[2, 1 + i, rows], 1, 1), 0.0)

    def pack_last():
        blocks = [((i, g), S[2, 1 + i, PAD + 8 * g : PAD + 8 * g + 8]) for i in range(n0) for g in range(groups)]
        accs = gather(blocks, 4)
        half = n2 // 4
        at = 4 * lax.rem(keys[2], half) + n2
        found = []
        for back in (1, 2):
            source = lax.rem(at - jnp.where(is_low[2], back, 0), n2)
            for v in range(RY.shape[2]):
                x, y = [jnp.take_along_axis(accs[min(2 * v + h, len(accs) - 1)], source, axis=1) for h in (0, 1)]
                found.append(jnp.where(keys[2] < half, x, y))
        for v in range(RY.shape[2]):
            SY[2, v] = found[v]
        return found[RY.shape[2] :]

    def scale(k, first, count):
        at = pl.ds(first, count)
        for part in (0, 1):
            loads[k, first, part].wait()
        inv = 1.0 / D[k, :, at]
        D[k, :, at] = inv
        S[k, pl.ds(1, n0), pl.ds(PAD + first, count)] = R[k, :, at] * inv

    loads[3].wait()
    for i in range(n0):
        NI[i] = 1.0 / (6.0 + NI[i])
    faces_x(NII, lambda i, r: NI[i, r : r + 1], n0)
    pack(NII, lambda i: NI[i], n0, 2)
    for k in (1, 2, 0):
        for first in bands:
            scale(k, first, 8)
        faces_x(k, lambda i, r: S[k, 1 + i, PAD + r : PAD + r + 1], n0)
    cross_rows()
    rows_rhs()
    pl.semaphore_wait(barrier, total)
    fence()
    cross_send(False)
    send(1, 1, (1,))
    send(PI, 1)
    send(NII, 1)
    send(NII, 2)
    send(NII, 0)
    fence()
    for k in (1, 2, 0):
        scale(k, 8, n1 - 16)
        if k == 2:
            last2 = pack_last()
            send(2, 2, (1,))
    send(0, 0, (1,))
    cross_plane()
    cross_send(True)
    for i in range(n0):
        x1 = S[1, 1 + i, rows]
        rhs = jnp.where(row_full >= 1, S[1, 1 + i, pl.ds(PAD - 1, n1)], 0.0) - x1 - S[2, 1 + i, rows]
        rhs = rhs - S[0, 1 + i, rows]
        if i > 0:
            rhs = rhs + S[0, i, rows]
        P[i] = rhs
    pack(PI, lambda i: P[i], n0, 2)
    for v, x in enumerate(last2):
        SY[PI, v] = SY[PI, v] + jnp.where(is_low[2], x, 0.0)
    send(PI, 2)
    for i in (0, n0 - 1):
        P[i] = P[i] + shifted(i)
    send(PI, 0)
    fence()
    loads[4].wait()
    spread_cols = (
        lax.broadcasted_iota(jnp.int32, (m2, n2), 1) // 2 == lax.broadcasted_iota(jnp.int32, (m2, n2), 0)
    ).astype(jnp.float32)
    inverse = (1.0 / (6.0 + CS[...])).reshape(m0 * m1, m2)
    inverse = jnp.dot(
        inverse, spread_cols, precision=lax.Precision.HIGHEST, preferred_element_type=jnp.float32
    ).reshape(m0, m1, n2)
    for c in range(m0):
        for r in (0, 1):
            CI[c, pl.ds(r, m1, stride=2)] = inverse[c]
    spread_faces(CII, CI, m0, 4)

    for i in range(n0):
        if 0 < i < n0 - 1:
            P[i] = P[i] + shifted(i)
        FG[1 + i, rows] = P[i] * NI[i]

    def gradients(j, G):
        for i in range(n0):
            x = F[j, i, 0:n1]
            above = F[j, i + 1, 0:n1] - x if i < n0 - 1 else -x
            ahead = jnp.where(lane_full >= n2 - 1, 0.0, pltpu.roll(x, n2 - 1, 1)) - x
            for k, grad in enumerate((above, F[j, i, 1 : n1 + 1] - x, ahead)):
                G[k, i] = G[k, i] + grad if j == 0 else grad


    def smooth(k):
        for a in range(3):
            receive(k, a, (0,) if (k, a) in from_low else (0, 1))
        rows_x(k, S.at[k])
        w = edges(k, 2)
        for i in range(n0):
            x = S[k, 1 + i, rows]
            near = S[k, i, rows] + S[k, i + 2, rows] + inplane(S.at[k, 1 + i], x, halo(w, i, 2), 1)
            OB[k, i] = x + near * D[k, i]

    for i in range(n0):
        F[0, i, 0:n1] = local_near(FG, i, n0, 1)

    def pair_rows(t, slot):
        t = t + jnp.where(lane_full % 2 == 0, pltpu.roll(t, n2 - 1, 1), pltpu.roll(t, 1, 1))
        T[slot, rows] = t
        return t + jnp.where(row_full % 2 == 0, T[slot, pl.ds(PAD + 1, n1)], T[slot, pl.ds(PAD - 1, n1)])

    for c in range(m0):
        CR[c] = pair_rows(F[0, 2 * c, 0:n1] + F[0, 2 * c + 1, 0:n1], c)
    from_low = ((0, 0), (1, 1), (2, 2))
    for f, a in from_low:
        receive(f, a, (1,))
    low2 = [jnp.where(is_low[2], 0.0, pltpu.roll(RY[2, 0, v], 1, 1)) for v in range(RY.shape[2])]
    add = S[0, 0, rows] * NI[0]
    T[2, rows] = add
    t = add + jnp.where(row_full >= 1, T[2, pl.ds(PAD - 1, n1)], 0.0)
    t = t + jnp.where(row_full < n1 - 1, T[2, pl.ds(PAD + 1, n1)], 0.0)
    t = t + jnp.where(lane_full >= 1, pltpu.roll(add, 1, 1), 0.0)
    t = t + jnp.where(lane_full < n2 - 1, pltpu.roll(add, n2 - 1, 1), 0.0)
    A1[0] = t
    lanei = lax.broadcasted_iota(jnp.int32, (n0, n2), 1)
    add = RX[1, 0] * SX[NII, 0]
    DX[pl.ds(PAD, n0)] = add
    x = add + DX[pl.ds(PAD - 1, n0)] + DX[pl.ds(PAD + 1, n0)]
    x = x + jnp.where(lanei >= 1, pltpu.roll(add, 1, 1), 0.0)
    SX[FGI, 0] = x + jnp.where(lanei < n2 - 1, pltpu.roll(add, n2 - 1, 1), 0.0)
    adds = [e * SY[NII, v] for v, e in enumerate(low2)]
    group, hop, per = lax.rem(keys[2], groups), 2 * groups, n2 // 2
    source = 2 * (2 * groups * (keys[4] // groups) + keys[4] % groups) + n2 - is_low[4].astype(jnp.int32)
    source = lax.rem(source, n2)
    spread = []
    for v, add in enumerate(adds):
        ahead = jnp.where(group < groups - 1, pltpu.roll(pltpu.roll(add, n2 - 2, 1), 7, 0), 0.0)
        behind = jnp.where(group > 0, pltpu.roll(pltpu.roll(add, 2, 1), 1, 0), 0.0)
        w = add + jnp.where(row8 < 7, pltpu.roll(add, 7, 0), ahead)
        w = w + jnp.where(row8 > 0, pltpu.roll(add, 1, 0), behind)
        ahead = pltpu.roll(adds[v + 1], n2 - hop, 1) if v + 1 < len(adds) else 0.0
        behind = pltpu.roll(adds[v - 1], hop, 1) if v else 0.0
        w = w + jnp.where(keys[2] < per - groups, pltpu.roll(add, n2 - hop, 1), ahead)
        w = w + jnp.where(keys[2] >= groups, pltpu.roll(add, hop, 1), behind)
        spread.append(w)
    for f in (NII, PI):
        for a in range(3):
            receive(f, a)
    cross_receive()
    ws = halo_fg()
    CR[0] = CR[0] + pair_rows(FG[0, rows] + A1[0], 0)
    CR[m0 - 1] = CR[m0 - 1] + pair_rows(FG[n0 + 1, rows], 1)
    SX[FGI, 0] = SX[FGI, 0] + RX[FGI, 0]
    SX[FGI, 1] = RX[FGI, 1]
    even = lax.broadcasted_iota(jnp.int32, (m0, n2), 1) % 2 == 0
    for d in (0, 1):
        x = SX[FGI, d, pl.ds(0, m0, stride=2)] + SX[FGI, d, pl.ds(1, m0, stride=2)]
        RX[V2I, d, 0:m0] = x + jnp.where(even, pltpu.roll(x, n2 - 1, 1), pltpu.roll(x, 1, 1))
    blocks = []
    for v, (w, add) in enumerate(zip(ws, spread)):
        w = w + add
        w = w + pltpu.roll(w, n2 - hop, 1)
        w = w + jnp.where(row8 % 2 == 0, pltpu.roll(w, 7, 0), pltpu.roll(w, 1, 0))
        blocks.append(jnp.take_along_axis(w, source, axis=1))
    side = (lane_full < 2) | (lane_full >= n2 - 2)
    for c in range(m0):
        t = CR[c] + jnp.where(side, halo(blocks, c, 4), 0.0)
        low = t[0:8] + jnp.where(row8 < 2, RX[V2I, 0, c : c + 1], 0.0)
        high = t[n1 - 8 : n1] + jnp.where(row8 >= 6, RX[V2I, 1, c : c + 1], 0.0)
        t = jnp.concatenate([low, t[8 : n1 - 8], high], axis=0)
        CR[c] = t
        V1[1 + c, rows] = t * CI[c]
    rowc = lax.broadcasted_iota(jnp.int32, (m0, n2), 0)
    lanec = lax.broadcasted_iota(jnp.int32, (m0, n2), 1)
    faces_x(V1I, lambda c, r: V1[1 + c, PAD + r : PAD + r + 1], m0)
    send(V1I, 1)
    for z in (0, 1):
        for x in (0, 1):
            c = (m0 - 1) * z
            LZX[z, x] = SX[V1I, x, c : c + 1]
    for x in (0, 1):
        g = (groups - 1) * x
        ends = [((c, g), V1[1 + c, PAD + 8 * g : PAD + 8 * g + 8]) for c in range(m0)]
        for v, acc in gather(ends, 4).items():
            LXY[x, v] = acc[7 * x : 7 * x + 1]
    lines_send(lambda offs: offs[1] != 0)
    for d, r in ((0, 2), (1, n1 - 3)):
        x = SX[V1I, d, 0:m0]
        near = jnp.concatenate([V1[1 + c, PAD + r : PAD + r + 1] for c in range(m0)], axis=0)
        near = near + jnp.where(rowc >= 1, pltpu.roll(x, 1, 0), 0.0)
        near = near + jnp.where(rowc < m0 - 1, pltpu.roll(x, m0 - 1, 0), 0.0)
        near = near + jnp.where(lanec >= 2, pltpu.roll(x, 2, 1), 0.0)
        SX[NLI, d, 0:m0] = near + jnp.where(lanec < n2 - 2, pltpu.roll(x, n2 - 2, 1), 0.0)
    send(NLI, 1)
    send(V1I, 0)
    pack(V1I, lambda c: V1[1 + c, rows], m0, 4)
    lines_send(lambda offs: offs[1] == 0)
    send(V1I, 2)
    fence()
    for c in range(m0):
        NL[c] = local_near(V1, c, m0, 2)
    send(NLI, 0)
    pack(NLI, lambda c: NL[c], m0, 4)
    send(NLI, 2)
    fence()

    def faces_f(j):
        f = F0I + j
        send(f, 0)
        faces_x(f, lambda i, r: F[j, i, r : r + 1], n0)
        send(f, 1)
        pack(f, lambda i: F[j, i, 0:n1], n0, 2)
        send(f, 2)

    for f, a in ((0, 1), (2, 1), (1, 0), (2, 0), (0, 2), (1, 2)):
        one(f, a)
    for f, a in from_low:
        send(f, a, (0,))
    for i in range(n0):
        rhs = P[i] + jnp.where(lane_full < 1, halo(low2, i, 2), 0.0)
        if i == 0:
            rhs = rhs + S[0, 0, rows]
        first = rhs[0:8] + jnp.where(row8 < 1, RX[1, 0, i : i + 1], 0.0)
        FG[1 + i, rows] = jnp.concatenate([first, rhs[8:]], axis=0) * NI[i]
    for i in range(n0):
        near = outer_near(local_near(FG, i, n0, 1), FG, FGI, ws, i, n0, 2)
        F[0, i, 0:n1] = FG[1 + i, rows] + near * NI[i]
    faces_f(0)

    def fold(x):
        acc = x[0:8]
        for g in range(1, groups):
            acc = acc + x[8 * g : 8 * g + 8]
        return acc

    sums = [jnp.zeros((8, n2), jnp.float32) for _ in range(4)]
    for c in range(m0):
        sums[0] = sums[0] + fold(V1[1 + c, rows] * CR[c])

    for f in (CII, V1I, NLI):
        for a in range(3):
            receive(f, a)
    lines_receive()
    ws = edges(V1I, 4)
    for c in range(m0):
        near = outer_near(NL[c], V1, V1I, ws, c, m0, 4)
        A1[c] = CR[c] - near
        V2[1 + c, rows] = V1[1 + c, rows] - near * CI[c]
    faces_x(V2I, lambda c, r: V2[1 + c, PAD + r : PAD + r + 1], m0)
    pack(V2I, lambda c: V2[1 + c, rows], m0, 4)
    w2 = halo_v2(ws, edges(NLI, 4), edges(CII, 4))

    def spread_near(j, V, w):
        for c in range(m0):
            x = V[1 + c, rows]
            near = x + inplane(V.at[1 + c], x, halo(w, c, 4), 1)
            F[j, 2 * c, 0:n1] = (near + V[c, rows]) * NI[2 * c]
            F[j, 2 * c + 1, 0:n1] = (near + V[c + 2, rows]) * NI[2 * c + 1]
        faces_f(j)

    for c in range(m0):
        v1, v2, a1 = V1[1 + c, rows], V2[1 + c, rows], A1[c]
        near = jnp.where(row_full < n1 - 2, V2[1 + c, pl.ds(PAD + 2, n1)], 0.0)
        near = near + jnp.where(lane_full < n2 - 2, pltpu.roll(v2, n2 - 2, 1), 0.0)
        if c < m0 - 1:
            near = near + V2[2 + c, rows]
        sums[1] = sums[1] + fold(v1 * a1)
        sums[2] = sums[2] + fold(v2 * a1)
        sums[3] = sums[3] + fold(v2 * (a1 - 2.0 * near))
    outer = fold(V2[1, rows] * V2[0, rows] + V2[m0, rows] * V2[m0 + 1, rows])
    for v, w in enumerate(w2):
        outer = outer + SY[V2I, v] * w
    rim = SX[V2I, 0, 0:m0] * RX[V2I, 0, 0:m0] + SX[V2I, 1, 0:m0] * RX[V2I, 1, 0:m0]
    sums[3] = sums[3] - outer
    rim = 2.0 * jnp.sum(rim, axis=0, keepdims=True)
    sums[3] = sums[3] - jnp.where(row8 == 0, rim, 0.0)
    lane1 = lax.broadcasted_iota(jnp.int32, (1, n2), 1)
    part = jnp.zeros((1, n2), jnp.float32)
    for q, s in enumerate(sums):
        part = jnp.where(lane1 == q, jnp.sum(jnp.sum(s, axis=0, keepdims=True), axis=1, keepdims=True), part)

    def slot(axes, at):
        index = 0
        for a in axes:
            index = index * sizes[a] + at(a)
        return index

    def sum_message(p, offs, sign):
        axes, slots = phases[p], slots_of[p]
        other = partner(axes, offs, sign)
        index = slot(axes, (lambda a: me[a]) if sign > 0 else (lambda a: other[AXES[a]]))
        sem = p * slots_of[0].shape[0] + slot(axes, lambda a: offs[axes.index(a)])
        return pltpu.make_async_remote_copy(
            src_ref=slots.at[index], dst_ref=slots.at[index], send_sem=psend.at[sem], recv_sem=precv.at[sem],
            device_id=other, device_id_type=MESH,
        )

    def sum_start(p, value):
        slots_of[p][slot(phases[p], lambda a: me[a])] = value
        for offs in offsets(phases[p]):
            sum_message(p, offs, 1).start()

    def sum_end(p):
        for offs in offsets(phases[p]):
            sum_message(p, offs, -1).wait_recv()
        terms = [slots_of[p][d] for d in range(slots_of[p].shape[0])]
        while len(terms) > 1:
            terms = [functools.reduce(lambda x, y: x + y, terms[t : t + 2]) for t in range(0, len(terms), 2)]
        return terms[0]

    sum_start(0, part)
    fence()
    rows_x(V2I, V2)
    spread_near(2, V2, w2)
    rows_x(V1I, V1)
    spread_near(1, V1, ws)
    gradients(1, G1)
    gradients(2, G2)
    for k in (1, 2, 0):
        smooth(k)
    gradients(0, OB)

    def drain(fields):
        for a in range(3):
            for d in (0, 1):
                def over(a=a, d=d):
                    for f in fields:
                        if f not in LOCAL and d in dirs(f):
                            message(f, a, d).wait_send()
                pl.when(can_send(a, d))(over)

    drain([f for f in range(FIELDS) if f not in FINAL])
    for offs in lines:
        pl.when(exists(offs))(lambda offs=offs: line_message(offs, 1).wait_send())
    for at in CROSS + GREET:
        pl.when(exists(cross_offs(*at, 1)))(lambda at=at: cross_message(*at, 1).wait_send())

    part = sum_end(0)
    for p in range(1, len(phases)):
        sum_start(p, part)
        part = sum_end(p)
    gone, hone, hmix, htwo = [
        jnp.sum(jnp.where(lane1 == q, part, 0.0), axis=1, keepdims=True) for q in range(4)
    ]
    two = (hone - hmix * gone / hone) / (htwo - hmix * hmix / hone)
    oneco = (gone - hmix * two) / hone
    CO[0:1] = jnp.broadcast_to(oneco, (1, n2))
    CO[1:2] = jnp.broadcast_to(two, (1, n2))
    for f in FINAL:
        for a in range(3):
            receive(f, a)

    def mix(get):
        a = get(0)
        return a + jnp.broadcast_to(oneco, a.shape) * get(1) + jnp.broadcast_to(two, a.shape) * get(2)

    MZ[...] = mix(lambda j: F[j, n0, 0:n1])
    MX[...] = mix(lambda j: RX[F0I + j, 1])
    for v in range(RY.shape[2]):
        MY[v] = pltpu.roll(mix(lambda j: RY[F0I + j, 1, v]), n2 - 1, 1)

    for p in range(len(phases)):
        for offs in offsets(phases[p]):
            sum_message(p, offs, 1).wait_send()
    drain(FINAL)


def combine(parts, OB, G1, G2, CO, MZ, MX, MY, out, W, sem):
    _, n0, n1, n2 = OB.shape
    one = jnp.broadcast_to(CO[0:1], (n1, n2))
    two = jnp.broadcast_to(CO[1:2], (n1, n2))
    groups, per, step = n1 // 8, n2 // 2, n0 // parts
    row8 = lax.broadcasted_iota(jnp.int32, (8, n2), 0)
    lane_full = lax.broadcasted_iota(jnp.int32, (n1, n2), 1)

    def edge(k, i, x):
        if k == 0:
            return x + MZ[...] if i == n0 - 1 else x
        if k == 1:
            last = x[n1 - 8 : n1] + jnp.where(row8 == 7, MX[i : i + 1], 0.0)
            return jnp.concatenate([x[0 : n1 - 8], last], axis=0)
        ats = [divmod(i * groups + g, per) for g in range(groups)]
        parts = [pltpu.roll(MY[v], (n2 - 2 * kk) % n2, 1) for v, kk in ats]
        return x + jnp.where(lane_full >= n2 - 1, jnp.concatenate(parts, axis=0), 0.0)

    copies = []
    for k in range(3):
        for h in range(parts):
            for i in range(h * step, (h + 1) * step):
                W[k, i] = edge(k, i, OB[k, i] + one * G1[k, i] + two * G2[k, i])
            planes = pl.ds(h * step, step)
            copies.append(pltpu.make_async_copy(W.at[k, planes], out.at[k, planes], sem.at[k * parts + h]))
            copies[-1].start()
    for c in copies:
        c.wait()


def solution(mesh):
    sizes = tuple(mesh.shape[a] for a in AXES)

    def local(residual, edge_diag, node_shift, coarse_shift):
        n0, n1, n2 = node_shift.shape
        m0, m1, m2 = coarse_shift.shape
        vecs = max(-(-(n0 * (n1 // 8)) // (n2 // 2)), -(-(m0 * (n1 // 8)) // (n2 // 4)))
        f32 = jnp.float32
        counts = [math.prod(sizes[a] for a in axes) for axes in phases_of(sizes)]
        V = lambda *s: pltpu.VMEM(s, f32)
        scratch = [
            V(3, n0, n1, n2), V(3, n0, n1, n2), V(n0, n1, n2), V(m0, m1, m2),
            V(3, n0 + 2, n1 + 2 * PAD, n2), V(n0 + 2, n1 + 2 * PAD, n2),
            V(m0, n1, n2), V(m0, n1, n2), V(m0, n1, n2), V(m0, n1, n2), V(m0, n1 + 2 * PAD, n2),
            V(m0 + 2, n1 + 2 * PAD, n2), V(m0 + 2, n1 + 2 * PAD, n2),
            V(3, n0 + 1, n1 + PAD, n2),
            V(FIELDS, 2, n0, n2), V(FIELDS, 2, n0, n2), V(FIELDS, vecs, 8, n2), V(FIELDS, 2, vecs, 8, n2),
            V(2, n1, n2), V(2, n1, n2), V(2, 2, 1, n2), V(2, vecs, 1, n2),
            V(2, 2, 1, n2), V(2, 2, 8, n2), V(2, 2, vecs, 1, n2),
            V(n0, n1, n2), V(2, n1, n2), V(2, n1, n2), V(2, 1, n2), V(2, 1, n2), V(2, vecs, 1, n2), V(vecs, 1, n2),
            V(8, n2), V(2, 1, n2), V(2, 1, n2), V(2, 8, n2), V(2, 8, n2), V(2, vecs, 1, n2), V(2, vecs, 1, n2), V(n0 + 2 * PAD, n2), V(3, 1, n2),
            *[V(c, 1, n2) for c in counts],
        ]
        sems = [pltpu.SemaphoreType.DMA(s) for s in ((20,), *[(FIELDS, 3, 2)] * 2, *[(sum(counts),)] * 2, *[(12,)] * 2, *[(15,)] * 2)]

        def scoped(*refs):
            plain, slots_of = refs[: -len(counts)], refs[-len(counts) :]
            pl.run_scoped(functools.partial(kernel, sizes, *plain, slots_of), *sems)

        field = pltpu.VMEM(residual.shape, f32)
        limit = 67_043_328 - 12 * math.prod(residual.shape) - 2**18
        fields = pl.pallas_call(
            scoped,
            out_shape=[field] * 3 + [pltpu.VMEM(s, f32) for s in ((8, n2), (n1, n2), (n0, n2), (vecs, 8, n2))],
            in_specs=[pl.BlockSpec(memory_space=pltpu.HBM)] * 4,
            out_specs=[pl.BlockSpec(memory_space=pltpu.VMEM)] * 7,
            scratch_shapes=scratch,
            compiler_params=pltpu.CompilerParams(collective_id=0, has_side_effects=True, vmem_limit_bytes=limit),
        )(residual, edge_diag, node_shift, coarse_shift)
        parts = 2 if n0 % 2 == 0 else 1
        return pl.pallas_call(
            functools.partial(combine, parts),
            out_shape=jax.ShapeDtypeStruct(residual.shape, f32),
            in_specs=[pl.BlockSpec(memory_space=pltpu.VMEM)] * 7,
            out_specs=pl.BlockSpec(memory_space=pltpu.HBM),
            scratch_shapes=[field, pltpu.SemaphoreType.DMA((3 * parts,))],
            compiler_params=pltpu.CompilerParams(vmem_limit_bytes=8 * math.prod(residual.shape)),
        )(*fields)

    placed = (
        P(None, "gz", "gx", "gy"),
        P(None, "gz", "gx", "gy"),
        P("gz", "gx", "gy"),
        P("gz", "gx", "gy"),
    )
    return jax.shard_map(
        local, mesh=mesh, in_specs=placed, out_specs=P(None, "gz", "gx", "gy"), check_vma=False
    )
```

```python
import functools
import itertools
import math

import jax
import jax.numpy as jnp
from jax import lax
from jax.experimental import pallas as pl
from jax.experimental.pallas import tpu as pltpu
from jax.sharding import PartitionSpec as P

MESH = pl.DeviceIdType.MESH
AXES = ("gz", "gx", "gy")
PI, V1I, V2I, F0I, NLI, CII, NII, FGI = 3, 4, 5, 6, 9, 10, 11, 12
FIELDS = 13
FINAL = (F0I, F0I + 1, F0I + 2)
COARSE = (V1I, V2I, NLI, CII)
LOCAL = (V2I, FGI)
CROSS = [(a, b, d) for a in range(3) for b in range(3) if a != b for d in (0, 1)]
GREET = [(a, b, 2) for a in range(3) for b in range(a)]
PAD = 8
FEW = 32


def fence():
    pl.delay(1)


def phases_of(sizes):
    return ((0, 1, 2),) if math.prod(sizes) <= FEW else ((1, 2), (0,))


def greeted(sizes, rounds):
    near = set(itertools.product((-1, 0, 1), repeat=3))
    known = set(near)
    for moves in rounds:
        known |= {tuple(p + q for p, q in zip(k, m)) for k in known for m in moves}
    needed = set()
    for axes in phases_of(sizes):
        spans = [range(1 - sizes[a], sizes[a]) if a in axes else (0,) for a in range(3)]
        needed |= set(itertools.product(*spans))
    every = near | (needed - known)
    return sorted(o for o in every if any(o) and all(abs(p) < n for p, n in zip(o, sizes)))


def kernel(
    sizes,
    res, dia, shf, csh, OB, G1, G2, CO, HZ, HX, HY,
    R, D, NI, CS, S, FG, CI, CR, A1, NL, T, V1, V2, F,
    SX, RX, SY, RY, NZ, CZ, LZX, LXY, RZX, RZY, RXY,
    P, PZ, NZI, LRZ, LRX, LY2, LY1, LP0, RRZ, RRX, RZ2, RZ0, RX2, RX1, DX, HELLO,
    slots_of,
    in_sem, send_sem, recv_sem, psend, precv, lsend, lrecv, csend, crecv,
):
    phases = phases_of(sizes)
    n0, n1, n2 = NI.shape
    m0, m1, m2 = CS.shape
    groups = n1 // 8
    me = [lax.axis_index(a) for a in AXES]
    rows = pl.ds(PAD, n1)

    def offsets(axes):
        every = itertools.product(*[range(sizes[a]) for a in axes])
        return [offs for offs in every if any(offs)]

    def partner(axes, offs, sign):
        return {
            AXES[a]: lax.rem(me[a] + (o if sign > 0 else sizes[a] - o), sizes[a]) for a, o in zip(axes, offs)
        }

    barrier = pltpu.get_barrier_semaphore()
    faces = [offs for offs in itertools.product((-1, 0, 1), repeat=3) if sum(map(abs, offs)) == 1]
    lines = [offs for offs in itertools.product((-1, 0, 1), repeat=3) if sum(map(abs, offs)) == 2]

    def exists(offs):
        inside = [(me[a] + o >= 0) & (me[a] + o < sizes[a]) for a, o in enumerate(offs) if o]
        return functools.reduce(jnp.logical_and, inside)

    def device(offs):
        return {AXES[a]: me[a] + o for a, o in enumerate(offs) if o}

    total = jnp.int32(0)
    for offs in greeted(sizes, (faces + lines, faces + lines)):
        there = exists(offs)
        pl.when(there)(
            lambda offs=offs: pl.semaphore_signal(
                barrier, inc=1, device_id=device(offs), device_id_type=MESH
            )
        )
        total = total + there.astype(jnp.int32)

    bands = (0, n1 - 8)
    loads = {}

    def load(key, src, dst):
        loads[key] = pltpu.make_async_copy(src, dst, in_sem.at[len(loads)])
        loads[key].start()

    load(3, shf, NI)
    for first, count in [(r, 8) for r in bands] + [(8, n1 - 16)]:
        at = pl.ds(first, count)
        for k in (1, 2, 0):
            load((k, first, 0), res.at[k, :, at], R.at[k, :, at])
            load((k, first, 1), dia.at[k, :, at], D.at[k, :, at])
    load(4, csh, CS)

    for k in range(3):
        for i in range(n0):
            F[k, i, n1 : n1 + 1] = jnp.zeros((1, n2), jnp.float32)
    DX[...] = jnp.zeros(DX.shape, jnp.float32)

    def clear(offs, *refs):
        @pl.when(jnp.logical_not(exists(offs)))
        def _():
            for ref in refs:
                ref[...] = jnp.zeros(ref.shape, jnp.float32)

    for d in (0, 1):
        step, i, c = (1, n0 + 1, m0 + 1) if d else (-1, 0, 0)
        planes = [S.at[k, i, rows] for k in range(3)] + [V1.at[c, rows], NZ.at[d], CZ.at[d], PZ.at[d], NZI.at[d]]
        clear((step, 0, 0), *planes, *([F.at[k, n0, pl.ds(0, n1)] for k in range(3)] if d else []))
        clear((0, step, 0), *[RX.at[f, d] for f in range(FIELDS) if f not in LOCAL])
        clear((0, 0, step), *[RY.at[f, d] for f in range(FIELDS) if f not in LOCAL])
    for offs in lines:
        z, x, y = [int(o > 0) for o in offs]
        clear(offs, RXY.at[x, y] if not offs[0] else RZY.at[z, y] if not offs[1] else RZX.at[z, x])

    lane = lax.broadcasted_iota(jnp.int32, (8, n2), 1)
    lane_full = lax.broadcasted_iota(jnp.int32, (n1, n2), 1)
    row_full = lax.broadcasted_iota(jnp.int32, (n1, n2), 0)
    row8 = lax.broadcasted_iota(jnp.int32, (8, n2), 0)
    keys = {p: ((lane + p // 2) // p) % (n2 // p) for p in (2, 4)}
    is_low = {p: (lane % p) >= p // 2 for p in (2, 4)}

    def place(i, g, p):
        k = i * groups + g
        per = n2 // p
        return k // per, k % per

    def gather(blocks, p):
        accs = {}
        for (i, g), part in blocks:
            v, kk = place(i, g, p)
            if kk:
                part = pltpu.roll(part, p * kk, 1)
            accs[v] = jnp.where(keys[p] == kk, part, accs.get(v, 0.0))
        return accs

    def pack(f, plane, count, p):
        at = [(i, g) for i in range(count) for g in range(groups)]
        planes = [plane(i) for i in range(count)]
        accs = gather([((i, g), planes[i][8 * g : 8 * g + 8]) for i, g in at], p)
        for v, acc in accs.items():
            SY[f, v] = acc

    def halo(ws, i, p):
        parts = []
        for g in range(groups):
            v, kk = place(i, g, p)
            parts.append(pltpu.roll(ws[v], n2 - p * kk, 1) if kk else ws[v])
        return jnp.concatenate(parts, axis=0)

    def inplane(ref, x, h, sh):
        near = ref[pl.ds(PAD - sh, n1)] + ref[pl.ds(PAD + sh, n1)]
        near = near + jnp.where(lane_full < sh, h, pltpu.roll(x, sh, 1))
        return near + jnp.where(lane_full >= n2 - sh, h, pltpu.roll(x, n2 - sh, 1))

    def local_near(ref, i, n, sh):
        x = ref[1 + i, rows]
        near = jnp.where(row_full >= sh, ref[1 + i, pl.ds(PAD - sh, n1)], 0.0)
        near = near + jnp.where(row_full < n1 - sh, ref[1 + i, pl.ds(PAD + sh, n1)], 0.0)
        near = near + jnp.where(lane_full >= sh, pltpu.roll(x, sh, 1), 0.0)
        near = near + jnp.where(lane_full < n2 - sh, pltpu.roll(x, n2 - sh, 1), 0.0)
        if i > 0:
            near = near + ref[i, rows]
        if i < n - 1:
            near = near + ref[i + 2, rows]
        return near

    def edges(f, p):
        sh = p // 2
        return [
            jnp.where(is_low[p], pltpu.roll(RY[f, 1, v], n2 - sh, 1), pltpu.roll(RY[f, 0, v], sh, 1))
            for v in range(RY.shape[2])
        ]

    def outer_near(near, ref, f, ws, i, n, p):
        sh = p // 2
        if i == 0:
            near = near + ref[0, rows]
        if i == n - 1:
            near = near + ref[n + 1, rows]
        side = (lane_full < sh) | (lane_full >= n2 - sh)
        near = near + jnp.where(side, halo(ws, i, p), 0.0)
        low = near[0:8] + jnp.where(row8 < sh, RX[f, 0, i : i + 1], 0.0)
        high = near[n1 - 8 : n1] + jnp.where(row8 >= 8 - sh, RX[f, 1, i : i + 1], 0.0)
        return jnp.concatenate([low, near[8 : n1 - 8], high], axis=0)

    def field(f):
        if f < 3:
            return S.at[f], n0
        return {V1I: (V1, m0)}[f]

    ZBUF = {NLI: (NL, NZ, m0), CII: (CI, CZ, m0), PI: (P, PZ, n0), NII: (NI, NZI, n0)}

    def message(f, a, d):
        if a == 0:
            if f in FINAL:
                src, dst = F.at[f - F0I, 0, pl.ds(0, n1)], F.at[f - F0I, n0, pl.ds(0, n1)]
            elif f in ZBUF:
                src, dst, n = ZBUF[f]
                src, dst = src.at[n - 1 if d else 0], dst.at[1 - d]
            else:
                ref, n = field(f)
                src = ref.at[n if d else 1, rows]
                dst = ref.at[0 if d else n + 1, rows]
        elif a == 1:
            count = m0 if f in COARSE else n0
            src, dst = SX.at[f, d, pl.ds(0, count)], RX.at[f, 1 - d, pl.ds(0, count)]
        else:
            src, dst = SY.at[f], RY.at[f, 1 - d]
        step = 1 if d else -1
        return pltpu.make_async_remote_copy(
            src_ref=src, dst_ref=dst, send_sem=send_sem.at[f, a, d], recv_sem=recv_sem.at[f, a, d],
            device_id={AXES[a]: lax.rem(me[a] + step + sizes[a], sizes[a])}, device_id_type=MESH,
        )

    def dirs(f):
        return (0,) if f in FINAL else (0, 1)

    def can_send(a, d):
        return me[a] < sizes[a] - 1 if d else me[a] > 0

    def send(f, a, only=(0, 1)):
        for d in [d for d in dirs(f) if d in only]:
            pl.when(can_send(a, d))(lambda f=f, a=a, d=d: message(f, a, d).start())

    def receive(f, a, only=(0, 1)):
        for d in [d for d in dirs(f) if d in only]:
            pl.when(can_send(a, 1 - d))(lambda f=f, a=a, d=d: message(f, a, d).wait_recv())

    def faces_x(f, get, count):
        for i in range(count):
            SX[f, 0, i : i + 1] = get(i, 0)
            if f not in FINAL:
                SX[f, 1, i : i + 1] = get(i, n1 - 1)

    def rows_x(f, ref):
        width = 2 if f in COARSE else 1
        for i in range(m0 if f in COARSE else n0):
            for w in range(width):
                ref[1 + i, PAD - 1 - w : PAD - w] = RX[f, 0, i : i + 1]
                ref[1 + i, PAD + n1 + w : PAD + n1 + w + 1] = RX[f, 1, i : i + 1]

    def line_message(offs, sign):
        z, x, y = [o * sign for o in offs]
        side = [0 if o > 0 else 1 for o in (z, x, y)]
        if not y:
            src, dst = LZX.at[1 - side[0], 1 - side[1]], RZX.at[side[0], side[1]]
        elif not x:
            plane = place(m0 - 1 if z > 0 else 0, 0, 4)[0]
            src, dst = SY.at[V1I, plane], RZY.at[side[0], side[2]]
        else:
            src, dst = LXY.at[1 - side[1]], RXY.at[side[1], side[2]]
        at = lines.index((z, x, y))
        return pltpu.make_async_remote_copy(
            src_ref=src, dst_ref=dst, send_sem=lsend.at[at], recv_sem=lrecv.at[at],
            device_id=device((z, x, y)), device_id_type=MESH,
        )

    def cross_message(a, b, d, sign):
        src, dst = (LRZ.at[0], HELLO.at[a + b - 1]) if d == 2 else {
            (0, 1): (LRZ.at[d], RRZ.at[d]),
            (1, 0): (LRX.at[d], RRX.at[d]),
            (0, 2): (SY.at[2, place(0 if d else n0 - 1, 0, 2)[0]], RZ2.at[d]),
            (2, 0): (LP0, RZ0.at[d]),
            (1, 2): (LY2.at[d], RX2.at[d]),
            (2, 1): (LY1, RX1.at[d]),
        }[a, b]
        at = (CROSS + GREET).index((a, b, d))
        return pltpu.make_async_remote_copy(
            src_ref=src, dst_ref=dst, send_sem=csend.at[at], recv_sem=crecv.at[at],
            device_id=device(cross_offs(a, b, d, sign)), device_id_type=MESH,
        )

    def cross_offs(a, b, d, sign):
        offs = [0, 0, 0]
        offs[a], offs[b] = (-sign if d else sign), (-sign if d == 2 else sign)
        return tuple(offs)

    CROSS_INTO = {(0, 1): RRZ, (1, 0): RRX, (0, 2): RZ2, (2, 0): RZ0, (1, 2): RX2, (2, 1): RX1}
    for a, b, d in CROSS:
        clear(cross_offs(a, b, d, -1), CROSS_INTO[a, b].at[d])

    def cross_rows():
        for d in (0, 1):
            i, r = (0 if d else n0 - 1), (0 if d else n1 - 1)
            LRZ[d] = S[1, 1 + i, PAD + n1 - 1 : PAD + n1]
            LRX[d] = S[0, n0, PAD + r : PAD + r + 1]
        for k, g in ((2, groups - 1), (2, 0), (1, groups - 1)):
            top = [((i, g), S[k, 1 + i, PAD + 8 * g : PAD + 8 * g + 8]) for i in range(n0)]
            for v, acc in gather(top, 2).items():
                line = acc[7:8] if g else acc[0:1]
                if k == 2:
                    LY2[0 if g else 1, v] = line
                else:
                    LY1[v] = line

    def cross_plane():
        top = [((n0 - 1, g), S[0, n0, PAD + 8 * g : PAD + 8 * g + 8]) for g in range(groups)]
        for acc in gather(top, 2).values():
            LP0[...] = acc

    def rows_rhs():
        rowi = lax.broadcasted_iota(jnp.int32, (n0, n2), 0)
        lanei = lax.broadcasted_iota(jnp.int32, (n0, n2), 1)
        inner = [S[1, 1 + i, PAD + n1 - 2 : PAD + n1 - 1] for i in range(n0)]
        for d in (0, 1):
            x = jnp.where(rowi >= 1, pltpu.roll(SX[0, d], 1, 0), 0.0) - SX[0, d]
            x = x + jnp.where(lanei >= 1, pltpu.roll(SX[2, d], 1, 1), 0.0) - SX[2, d]
            SX[PI, d] = x - SX[1, d] + jnp.concatenate(inner, axis=0) if d else x - SX[1, d]

    def cross_send(which):
        for at in [at for at in CROSS + GREET if (at[:2] in ((0, 2), (2, 0)) and at[2] < 2) == which]:
            pl.when(exists(cross_offs(*at, 1)))(lambda at=at: cross_message(*at, 1).start())

    def cross_receive():
        for at in CROSS + GREET:
            pl.when(exists(cross_offs(*at, -1)))(lambda at=at: cross_message(*at, -1).wait_recv())

    def halo_fg():
        for d in (0, 1):
            kk = place(0 if d else n0 - 1, 0, 2)[1]
            rhs = PZ[d] + S[0, n0, rows] if d else PZ[d]
            col = [pltpu.roll(RZ2[d], (2 * n2 - 2 * (kk + g) + 1) % n2, 1) for g in range(groups)]
            rhs = rhs + jnp.where(lane_full < 1, jnp.concatenate(col, axis=0), 0.0)
            first = rhs[0:8] + jnp.where(row8 < 1, RRZ[d], 0.0)
            FG[(n0 + 1) * d, rows] = jnp.concatenate([first, rhs[8:]], axis=0) * NZI[d]
        rowi = lax.broadcasted_iota(jnp.int32, (n0, n2), 0)
        lanei = lax.broadcasted_iota(jnp.int32, (n0, n2), 1)
        per = n2 // 2
        for d in (0, 1):
            rhs = RX[PI, d] + SX[1, 1] if d else RX[PI, d]
            rhs = rhs + jnp.where(rowi == 0, RRX[d], 0.0)
            index = rowi * groups + (0 if d else groups - 1)
            at = lax.rem(2 * lax.rem(index, per) + n2 - 1, n2)
            got = jnp.zeros((n0, n2), jnp.float32)
            for v in range(RX2.shape[1]):
                here = (lanei == at) & (index >= v * per) & (index < (v + 1) * per)
                got = got + jnp.where(here, RX2[d, v], 0.0)
            rhs = rhs + jnp.where(lanei < 1, jnp.sum(got, axis=1, keepdims=True), 0.0)
            RX[FGI, d] = rhs * RX[NII, d]
        ws = []
        for v, (ep, en) in enumerate(zip(edges(PI, 2), edges(NII, 2))):
            rhs = ep + jnp.where(is_low[2], SY[2, v], 0.0)
            if v == 0:
                k0 = place(n0 - 1, 0, 2)[1]
                moved = pltpu.roll(align(RZ0[0], RZ0[1], 2), (n2 - 2 * k0) % n2, 1)
                rhs = rhs + jnp.where(keys[2] < groups, moved, 0.0)
            line = align(jnp.broadcast_to(RX1[0, v], (8, n2)), jnp.broadcast_to(RX1[1, v], (8, n2)), 2)
            line = pltpu.roll(line, n2 - 2 * (groups - 1), 1)
            here = (lax.rem(keys[2], groups) == 0) & (row8 < 1)
            ws.append((rhs + jnp.where(here, line, 0.0)) * en)
        return ws

    def lines_send(which):
        for offs in [offs for offs in lines if which(offs)]:
            pl.when(exists(offs))(lambda offs=offs: line_message(offs, 1).start())

    def lines_receive():
        for offs in lines:
            pl.when(exists(offs))(lambda offs=offs: line_message(offs, -1).wait_recv())

    def align(low, high, p):
        return jnp.where(is_low[p], pltpu.roll(high, n2 - p // 2, 1), pltpu.roll(low, p // 2, 1))

    def halo_v2(ev, enl, eci):
        sh, kgroup = 2, [place(c, 0, 4) for c in (m0 - 1, 0)]
        col = [align(RZY[d, 0], RZY[d, 1], 4) for d in (0, 1)]
        for d, edge in ((0, 0), (1, m0 + 1)):
            v, kk = kgroup[d]
            near = NZ[d] + V1[1 if d == 0 else m0, rows]
            parts = [pltpu.roll(col[d], (n2 - 4 * (kk + g)) % n2, 1) for g in range(groups)]
            side = (lane_full < sh) | (lane_full >= n2 - sh)
            near = near + jnp.where(side, jnp.concatenate(parts, axis=0), 0.0)
            low = near[0:8] + jnp.where(row8 < sh, RZX[d, 0], 0.0)
            high = near[n1 - 8 : n1] + jnp.where(row8 >= 8 - sh, RZX[d, 1], 0.0)
            near = jnp.concatenate([low, near[8 : n1 - 8], high], axis=0)
            V2[edge, rows] = V1[edge, rows] - CZ[d] * near
        rowc = lax.broadcasted_iota(jnp.int32, (m0, n2), 0)
        lanec = lax.broadcasted_iota(jnp.int32, (m0, n2), 1)
        per = n2 // 4
        for d in (0, 1):
            near = RX[NLI, d, 0:m0] + SX[V1I, d, 0:m0]
            near = near + jnp.where(rowc == 0, RZX[0, d], 0.0) + jnp.where(rowc == m0 - 1, RZX[1, d], 0.0)
            for y in (0, 1):
                index = rowc * groups + (groups - 1 if d == 0 else 0)
                at = lax.rem(4 * lax.rem(index, per) + (n2 - 1 if y == 0 else 0), n2)
                got = jnp.zeros((m0, n2), jnp.float32)
                for v in range(RXY.shape[2]):
                    here = (lanec == at) & (index >= v * per) & (index < (v + 1) * per)
                    got = got + jnp.where(here, RXY[d, y, v], 0.0)
                got = jnp.sum(got, axis=1, keepdims=True)
                near = near + jnp.where((lanec < sh) if y == 0 else (lanec >= n2 - sh), got, 0.0)
            RX[V2I, d, 0:m0] = RX[V1I, d, 0:m0] - RX[CII, d, 0:m0] * near
        ws = []
        for v in range(len(ev)):
            near = enl[v] + SY[V1I, v]
            for d, c in ((0, 0), (1, m0 - 1)):
                into, k0 = place(c, 0, 4)
                if into == v:
                    shift = (4 * (k0 - kgroup[d][1])) % n2
                    moved = pltpu.roll(col[d], shift, 1) if shift else col[d]
                    near = near + jnp.where((keys[4] >= k0) & (keys[4] < k0 + groups), moved, 0.0)
            for d in (0, 1):
                line = align(
                    jnp.broadcast_to(RXY[d, 0, v], (8, n2)), jnp.broadcast_to(RXY[d, 1, v], (8, n2)), 4
                )
                jump = 4 * (groups - 1)
                line = pltpu.roll(line, n2 - jump if d == 0 else jump, 1)
                here = lax.rem(keys[4], groups) == (0 if d == 0 else groups - 1)
                here = here & ((row8 < sh) if d == 0 else (row8 >= 8 - sh))
                near = near + jnp.where(here, line, 0.0)
            ws.append(ev[v] - eci[v] * near)
        return ws

    def one(f, a, only=(0, 1)):
        ref, count = field(f)
        if a == 2:
            pack(f, lambda i: ref[1 + i, rows], count, 2)
        send(f, a, only)

    def spread_faces(f, ref, n, p):
        send(f, 0)
        faces_x(f, lambda c, r: ref[c, r : r + 1], n)
        send(f, 1)
        pack(f, lambda c: ref[c], n, p)
        send(f, 2)

    def shifted(i):
        return jnp.where(lane_full >= 1, pltpu.roll(S[2, 1 + i, rows], 1, 1), 0.0)

    def pack_last():
        blocks = [((i, g), S[2, 1 + i, PAD + 8 * g : PAD + 8 * g + 8]) for i in range(n0) for g in range(groups)]
        accs = gather(blocks, 4)
        half = n2 // 4
        at = 4 * lax.rem(keys[2], half) + n2
        found = []
        for back in (1, 2):
            source = lax.rem(at - jnp.where(is_low[2], back, 0), n2)
            for v in range(RY.shape[2]):
                x, y = [jnp.take_along_axis(accs[min(2 * v + h, len(accs) - 1)], source, axis=1) for h in (0, 1)]
                found.append(jnp.where(keys[2] < half, x, y))
        for v in range(RY.shape[2]):
            SY[2, v] = found[v]
        return found[RY.shape[2] :]

    def scale(k, first, count):
        at = pl.ds(first, count)
        for part in (0, 1):
            loads[k, first, part].wait()
        inv = 1.0 / D[k, :, at]
        D[k, :, at] = inv
        S[k, pl.ds(1, n0), pl.ds(PAD + first, count)] = R[k, :, at] * inv

    loads[3].wait()
    for i in range(n0):
        NI[i] = 1.0 / (6.0 + NI[i])
    faces_x(NII, lambda i, r: NI[i, r : r + 1], n0)
    pack(NII, lambda i: NI[i], n0, 2)
    for k in (1, 2, 0):
        for first in bands:
            scale(k, first, 8)
        faces_x(k, lambda i, r: S[k, 1 + i, PAD + r : PAD + r + 1], n0)
    cross_rows()
    rows_rhs()
    pl.semaphore_wait(barrier, total)
    fence()
    cross_send(False)
    send(1, 1, (1,))
    send(PI, 1)
    send(NII, 1)
    send(NII, 2)
    send(NII, 0)
    fence()
    for k in (1, 2, 0):
        scale(k, 8, n1 - 16)
        if k == 2:
            last2 = pack_last()
            send(2, 2, (1,))
    send(0, 0, (1,))
    cross_plane()
    cross_send(True)
    for i in range(n0):
        x1 = S[1, 1 + i, rows]
        rhs = jnp.where(row_full >= 1, S[1, 1 + i, pl.ds(PAD - 1, n1)], 0.0) - x1 - S[2, 1 + i, rows]
        rhs = rhs - S[0, 1 + i, rows]
        if i > 0:
            rhs = rhs + S[0, i, rows]
        P[i] = rhs
    pack(PI, lambda i: P[i], n0, 2)
    for v, x in enumerate(last2):
        SY[PI, v] = SY[PI, v] + jnp.where(is_low[2], x, 0.0)
    send(PI, 2)
    for i in (0, n0 - 1):
        P[i] = P[i] + shifted(i)
    send(PI, 0)
    fence()
    loads[4].wait()
    spread_cols = (
        lax.broadcasted_iota(jnp.int32, (m2, n2), 1) // 2 == lax.broadcasted_iota(jnp.int32, (m2, n2), 0)
    ).astype(jnp.float32)
    inverse = (1.0 / (6.0 + CS[...])).reshape(m0 * m1, m2)
    inverse = jnp.dot(
        inverse, spread_cols, precision=lax.Precision.HIGHEST, preferred_element_type=jnp.float32
    ).reshape(m0, m1, n2)
    for c in range(m0):
        for r in (0, 1):
            CI[c, pl.ds(r, m1, stride=2)] = inverse[c]
    spread_faces(CII, CI, m0, 4)

    for i in range(n0):
        if 0 < i < n0 - 1:
            P[i] = P[i] + shifted(i)
        FG[1 + i, rows] = P[i] * NI[i]

    def gradients(j, G):
        for i in range(n0):
            x = F[j, i, 0:n1]
            above = F[j, i + 1, 0:n1] - x if i < n0 - 1 else -x
            ahead = jnp.where(lane_full >= n2 - 1, 0.0, pltpu.roll(x, n2 - 1, 1)) - x
            for k, grad in enumerate((above, F[j, i, 1 : n1 + 1] - x, ahead)):
                G[k, i] = G[k, i] + grad if j == 0 else grad


    def smooth(k):
        for a in range(3):
            receive(k, a, (0,) if (k, a) in from_low else (0, 1))
        rows_x(k, S.at[k])
        w = edges(k, 2)
        for i in range(n0):
            x = S[k, 1 + i, rows]
            near = S[k, i, rows] + S[k, i + 2, rows] + inplane(S.at[k, 1 + i], x, halo(w, i, 2), 1)
            OB[k, i] = x + near * D[k, i]

    for i in range(n0):
        F[0, i, 0:n1] = local_near(FG, i, n0, 1)

    def pair_rows(t, slot):
        t = t + jnp.where(lane_full % 2 == 0, pltpu.roll(t, n2 - 1, 1), pltpu.roll(t, 1, 1))
        T[slot, rows] = t
        return t + jnp.where(row_full % 2 == 0, T[slot, pl.ds(PAD + 1, n1)], T[slot, pl.ds(PAD - 1, n1)])

    for c in range(m0):
        CR[c] = pair_rows(F[0, 2 * c, 0:n1] + F[0, 2 * c + 1, 0:n1], c)
    from_low = ((0, 0), (1, 1), (2, 2))
    for f, a in from_low:
        receive(f, a, (1,))
    low2 = [jnp.where(is_low[2], 0.0, pltpu.roll(RY[2, 0, v], 1, 1)) for v in range(RY.shape[2])]
    add = S[0, 0, rows] * NI[0]
    T[2, rows] = add
    t = add + jnp.where(row_full >= 1, T[2, pl.ds(PAD - 1, n1)], 0.0)
    t = t + jnp.where(row_full < n1 - 1, T[2, pl.ds(PAD + 1, n1)], 0.0)
    t = t + jnp.where(lane_full >= 1, pltpu.roll(add, 1, 1), 0.0)
    t = t + jnp.where(lane_full < n2 - 1, pltpu.roll(add, n2 - 1, 1), 0.0)
    A1[0] = t
    lanei = lax.broadcasted_iota(jnp.int32, (n0, n2), 1)
    add = RX[1, 0] * SX[NII, 0]
    DX[pl.ds(PAD, n0)] = add
    x = add + DX[pl.ds(PAD - 1, n0)] + DX[pl.ds(PAD + 1, n0)]
    x = x + jnp.where(lanei >= 1, pltpu.roll(add, 1, 1), 0.0)
    SX[FGI, 0] = x + jnp.where(lanei < n2 - 1, pltpu.roll(add, n2 - 1, 1), 0.0)
    adds = [e * SY[NII, v] for v, e in enumerate(low2)]
    group, hop, per = lax.rem(keys[2], groups), 2 * groups, n2 // 2
    source = 2 * (2 * groups * (keys[4] // groups) + keys[4] % groups) + n2 - is_low[4].astype(jnp.int32)
    source = lax.rem(source, n2)
    spread = []
    for v, add in enumerate(adds):
        ahead = jnp.where(group < groups - 1, pltpu.roll(pltpu.roll(add, n2 - 2, 1), 7, 0), 0.0)
        behind = jnp.where(group > 0, pltpu.roll(pltpu.roll(add, 2, 1), 1, 0), 0.0)
        w = add + jnp.where(row8 < 7, pltpu.roll(add, 7, 0), ahead)
        w = w + jnp.where(row8 > 0, pltpu.roll(add, 1, 0), behind)
        ahead = pltpu.roll(adds[v + 1], n2 - hop, 1) if v + 1 < len(adds) else 0.0
        behind = pltpu.roll(adds[v - 1], hop, 1) if v else 0.0
        w = w + jnp.where(keys[2] < per - groups, pltpu.roll(add, n2 - hop, 1), ahead)
        w = w + jnp.where(keys[2] >= groups, pltpu.roll(add, hop, 1), behind)
        spread.append(w)
    for f in (NII, PI):
        for a in range(3):
            receive(f, a)
    cross_receive()
    ws = halo_fg()
    CR[0] = CR[0] + pair_rows(FG[0, rows] + A1[0], 0)
    CR[m0 - 1] = CR[m0 - 1] + pair_rows(FG[n0 + 1, rows], 1)
    SX[FGI, 0] = SX[FGI, 0] + RX[FGI, 0]
    SX[FGI, 1] = RX[FGI, 1]
    even = lax.broadcasted_iota(jnp.int32, (m0, n2), 1) % 2 == 0
    for d in (0, 1):
        x = SX[FGI, d, pl.ds(0, m0, stride=2)] + SX[FGI, d, pl.ds(1, m0, stride=2)]
        RX[V2I, d, 0:m0] = x + jnp.where(even, pltpu.roll(x, n2 - 1, 1), pltpu.roll(x, 1, 1))
    blocks = []
    for v, (w, add) in enumerate(zip(ws, spread)):
        w = w + add
        w = w + pltpu.roll(w, n2 - hop, 1)
        w = w + jnp.where(row8 % 2 == 0, pltpu.roll(w, 7, 0), pltpu.roll(w, 1, 0))
        blocks.append(jnp.take_along_axis(w, source, axis=1))
    side = (lane_full < 2) | (lane_full >= n2 - 2)
    for c in range(m0):
        t = CR[c] + jnp.where(side, halo(blocks, c, 4), 0.0)
        low = t[0:8] + jnp.where(row8 < 2, RX[V2I, 0, c : c + 1], 0.0)
        high = t[n1 - 8 : n1] + jnp.where(row8 >= 6, RX[V2I, 1, c : c + 1], 0.0)
        t = jnp.concatenate([low, t[8 : n1 - 8], high], axis=0)
        CR[c] = t
        V1[1 + c, rows] = t * CI[c]
    rowc = lax.broadcasted_iota(jnp.int32, (m0, n2), 0)
    lanec = lax.broadcasted_iota(jnp.int32, (m0, n2), 1)
    faces_x(V1I, lambda c, r: V1[1 + c, PAD + r : PAD + r + 1], m0)
    send(V1I, 1)
    for z in (0, 1):
        for x in (0, 1):
            c = (m0 - 1) * z
            LZX[z, x] = SX[V1I, x, c : c + 1]
    for x in (0, 1):
        g = (groups - 1) * x
        ends = [((c, g), V1[1 + c, PAD + 8 * g : PAD + 8 * g + 8]) for c in range(m0)]
        for v, acc in gather(ends, 4).items():
            LXY[x, v] = acc[7 * x : 7 * x + 1]
    lines_send(lambda offs: offs[1] != 0)
    for d, r in ((0, 2), (1, n1 - 3)):
        x = SX[V1I, d, 0:m0]
        near = jnp.concatenate([V1[1 + c, PAD + r : PAD + r + 1] for c in range(m0)], axis=0)
        near = near + jnp.where(rowc >= 1, pltpu.roll(x, 1, 0), 0.0)
        near = near + jnp.where(rowc < m0 - 1, pltpu.roll(x, m0 - 1, 0), 0.0)
        near = near + jnp.where(lanec >= 2, pltpu.roll(x, 2, 1), 0.0)
        SX[NLI, d, 0:m0] = near + jnp.where(lanec < n2 - 2, pltpu.roll(x, n2 - 2, 1), 0.0)
    send(NLI, 1)
    send(V1I, 0)
    pack(V1I, lambda c: V1[1 + c, rows], m0, 4)
    lines_send(lambda offs: offs[1] == 0)
    send(V1I, 2)
    fence()
    for c in range(m0):
        NL[c] = local_near(V1, c, m0, 2)
    send(NLI, 0)
    pack(NLI, lambda c: NL[c], m0, 4)
    send(NLI, 2)
    fence()

    def faces_f(j):
        f = F0I + j
        send(f, 0)
        faces_x(f, lambda i, r: F[j, i, r : r + 1], n0)
        send(f, 1)
        pack(f, lambda i: F[j, i, 0:n1], n0, 2)
        send(f, 2)

    for f, a in ((0, 1), (2, 1), (1, 0), (2, 0), (0, 2), (1, 2)):
        one(f, a)
    for f, a in from_low:
        send(f, a, (0,))
    for i in range(n0):
        rhs = P[i] + jnp.where(lane_full < 1, halo(low2, i, 2), 0.0)
        if i == 0:
            rhs = rhs + S[0, 0, rows]
        first = rhs[0:8] + jnp.where(row8 < 1, RX[1, 0, i : i + 1], 0.0)
        FG[1 + i, rows] = jnp.concatenate([first, rhs[8:]], axis=0) * NI[i]
    for i in range(n0):
        near = outer_near(local_near(FG, i, n0, 1), FG, FGI, ws, i, n0, 2)
        F[0, i, 0:n1] = FG[1 + i, rows] + near * NI[i]
    faces_f(0)

    def fold(x):
        acc = x[0:8]
        for g in range(1, groups):
            acc = acc + x[8 * g : 8 * g + 8]
        return acc

    sums = [jnp.zeros((8, n2), jnp.float32) for _ in range(4)]
    for c in range(m0):
        sums[0] = sums[0] + fold(V1[1 + c, rows] * CR[c])

    for f in (CII, V1I, NLI):
        for a in range(3):
            receive(f, a)
    lines_receive()
    ws = edges(V1I, 4)
    for c in range(m0):
        near = outer_near(NL[c], V1, V1I, ws, c, m0, 4)
        A1[c] = CR[c] - near
        V2[1 + c, rows] = V1[1 + c, rows] - near * CI[c]
    faces_x(V2I, lambda c, r: V2[1 + c, PAD + r : PAD + r + 1], m0)
    pack(V2I, lambda c: V2[1 + c, rows], m0, 4)
    w2 = halo_v2(ws, edges(NLI, 4), edges(CII, 4))

    def spread_near(j, V, w):
        for c in range(m0):
            x = V[1 + c, rows]
            near = x + inplane(V.at[1 + c], x, halo(w, c, 4), 1)
            F[j, 2 * c, 0:n1] = (near + V[c, rows]) * NI[2 * c]
            F[j, 2 * c + 1, 0:n1] = (near + V[c + 2, rows]) * NI[2 * c + 1]
        faces_f(j)

    for c in range(m0):
        v1, v2, a1 = V1[1 + c, rows], V2[1 + c, rows], A1[c]
        near = jnp.where(row_full < n1 - 2, V2[1 + c, pl.ds(PAD + 2, n1)], 0.0)
        near = near + jnp.where(lane_full < n2 - 2, pltpu.roll(v2, n2 - 2, 1), 0.0)
        if c < m0 - 1:
            near = near + V2[2 + c, rows]
        sums[1] = sums[1] + fold(v1 * a1)
        sums[2] = sums[2] + fold(v2 * a1)
        sums[3] = sums[3] + fold(v2 * (a1 - 2.0 * near))
    outer = fold(V2[1, rows] * V2[0, rows] + V2[m0, rows] * V2[m0 + 1, rows])
    for v, w in enumerate(w2):
        outer = outer + SY[V2I, v] * w
    rim = SX[V2I, 0, 0:m0] * RX[V2I, 0, 0:m0] + SX[V2I, 1, 0:m0] * RX[V2I, 1, 0:m0]
    sums[3] = sums[3] - outer
    rim = 2.0 * jnp.sum(rim, axis=0, keepdims=True)
    sums[3] = sums[3] - jnp.where(row8 == 0, rim, 0.0)
    lane1 = lax.broadcasted_iota(jnp.int32, (1, n2), 1)
    part = jnp.zeros((1, n2), jnp.float32)
    for q, s in enumerate(sums):
        part = jnp.where(lane1 == q, jnp.sum(jnp.sum(s, axis=0, keepdims=True), axis=1, keepdims=True), part)

    def slot(axes, at):
        index = 0
        for a in axes:
            index = index * sizes[a] + at(a)
        return index

    def sum_message(p, offs, sign):
        axes, slots = phases[p], slots_of[p]
        other = partner(axes, offs, sign)
        index = slot(axes, (lambda a: me[a]) if sign > 0 else (lambda a: other[AXES[a]]))
        sem = p * slots_of[0].shape[0] + slot(axes, lambda a: offs[axes.index(a)])
        return pltpu.make_async_remote_copy(
            src_ref=slots.at[index], dst_ref=slots.at[index], send_sem=psend.at[sem], recv_sem=precv.at[sem],
            device_id=other, device_id_type=MESH,
        )

    def sum_start(p, value):
        slots_of[p][slot(phases[p], lambda a: me[a])] = value
        for offs in offsets(phases[p]):
            sum_message(p, offs, 1).start()

    def sum_end(p):
        for offs in offsets(phases[p]):
            sum_message(p, offs, -1).wait_recv()
        terms = [slots_of[p][d] for d in range(slots_of[p].shape[0])]
        while len(terms) > 1:
            terms = [functools.reduce(lambda x, y: x + y, terms[t : t + 2]) for t in range(0, len(terms), 2)]
        return terms[0]

    sum_start(0, part)
    fence()
    rows_x(V2I, V2)
    spread_near(2, V2, w2)
    rows_x(V1I, V1)
    spread_near(1, V1, ws)
    gradients(1, G1)
    gradients(2, G2)
    for k in (1, 2, 0):
        smooth(k)
    gradients(0, OB)

    def drain(fields):
        for a in range(3):
            for d in (0, 1):
                def over(a=a, d=d):
                    for f in fields:
                        if f not in LOCAL and d in dirs(f):
                            message(f, a, d).wait_send()
                pl.when(can_send(a, d))(over)

    drain(range(FIELDS))
    for offs in lines:
        pl.when(exists(offs))(lambda offs=offs: line_message(offs, 1).wait_send())
    for at in CROSS + GREET:
        pl.when(exists(cross_offs(*at, 1)))(lambda at=at: cross_message(*at, 1).wait_send())

    for offs in offsets(phases[0]):
        sum_message(0, offs, 1).wait_send()
    for j, f in enumerate(FINAL):
        for a in range(3):
            receive(f, a)
        HZ[j] = F[j, n0, 0:n1]
        HX[j] = RX[f, 1]
        HY[j] = RY[f, 1]

    part = sum_end(0)
    for p in range(1, len(phases)):
        sum_start(p, part)
        part = sum_end(p)
        for offs in offsets(phases[p]):
            sum_message(p, offs, 1).wait_send()
    gone, hone, hmix, htwo = [
        jnp.sum(jnp.where(lane1 == q, part, 0.0), axis=1, keepdims=True) for q in range(4)
    ]
    two = (hone - hmix * gone / hone) / (htwo - hmix * hmix / hone)
    oneco = (gone - hmix * two) / hone
    CO[0:1] = jnp.broadcast_to(oneco, (1, n2))
    CO[1:2] = jnp.broadcast_to(two, (1, n2))


def combine(parts, OB, G1, G2, CO, HZ, HX, HY, out, W, sem):
    _, n0, n1, n2 = OB.shape
    one = jnp.broadcast_to(CO[0:1], (n1, n2))
    two = jnp.broadcast_to(CO[1:2], (n1, n2))
    groups, per, step = n1 // 8, n2 // 2, n0 // parts
    row8 = lax.broadcasted_iota(jnp.int32, (8, n2), 0)
    lane_full = lax.broadcasted_iota(jnp.int32, (n1, n2), 1)

    def mix(get):
        a = get(0)
        c1, c2 = [jnp.broadcast_to(CO[q : q + 1], a.shape) for q in (0, 1)]
        return a + c1 * get(1) + c2 * get(2)

    ends = [pltpu.roll(mix(lambda j: HY[j, v]), n2 - 1, 1) for v in range(HY.shape[1])]

    def edge(k, i, x):
        if k == 0:
            return x + mix(lambda j: HZ[j]) if i == n0 - 1 else x
        if k == 1:
            last = x[n1 - 8 : n1] + jnp.where(row8 == 7, mix(lambda j: HX[j, i : i + 1]), 0.0)
            return jnp.concatenate([x[0 : n1 - 8], last], axis=0)
        ats = [divmod(i * groups + g, per) for g in range(groups)]
        parts = [pltpu.roll(ends[v], (n2 - 2 * kk) % n2, 1) for v, kk in ats]
        return x + jnp.where(lane_full >= n2 - 1, jnp.concatenate(parts, axis=0), 0.0)

    copies = []
    for k in range(3):
        for h in range(parts):
            for i in range(h * step, (h + 1) * step):
                W[k, i] = edge(k, i, OB[k, i] + one * G1[k, i] + two * G2[k, i])
            planes = pl.ds(h * step, step)
            copies.append(pltpu.make_async_copy(W.at[k, planes], out.at[k, planes], sem.at[k * parts + h]))
            copies[-1].start()
    for c in copies:
        c.wait()


def solution(mesh):
    sizes = tuple(mesh.shape[a] for a in AXES)

    def local(residual, edge_diag, node_shift, coarse_shift):
        n0, n1, n2 = node_shift.shape
        m0, m1, m2 = coarse_shift.shape
        vecs = max(-(-(n0 * (n1 // 8)) // (n2 // 2)), -(-(m0 * (n1 // 8)) // (n2 // 4)))
        f32 = jnp.float32
        counts = [math.prod(sizes[a] for a in axes) for axes in phases_of(sizes)]
        V = lambda *s: pltpu.VMEM(s, f32)
        scratch = [
            V(3, n0, n1, n2), V(3, n0, n1, n2), V(n0, n1, n2), V(m0, m1, m2),
            V(3, n0 + 2, n1 + 2 * PAD, n2), V(n0 + 2, n1 + 2 * PAD, n2),
            V(m0, n1, n2), V(m0, n1, n2), V(m0, n1, n2), V(m0, n1, n2), V(m0, n1 + 2 * PAD, n2),
            V(m0 + 2, n1 + 2 * PAD, n2), V(m0 + 2, n1 + 2 * PAD, n2),
            V(3, n0 + 1, n1 + PAD, n2),
            V(FIELDS, 2, n0, n2), V(FIELDS, 2, n0, n2), V(FIELDS, vecs, 8, n2), V(FIELDS, 2, vecs, 8, n2),
            V(2, n1, n2), V(2, n1, n2), V(2, 2, 1, n2), V(2, vecs, 1, n2),
            V(2, 2, 1, n2), V(2, 2, 8, n2), V(2, 2, vecs, 1, n2),
            V(n0, n1, n2), V(2, n1, n2), V(2, n1, n2), V(2, 1, n2), V(2, 1, n2), V(2, vecs, 1, n2), V(vecs, 1, n2),
            V(8, n2), V(2, 1, n2), V(2, 1, n2), V(2, 8, n2), V(2, 8, n2), V(2, vecs, 1, n2), V(2, vecs, 1, n2), V(n0 + 2 * PAD, n2), V(3, 1, n2),
            *[V(c, 1, n2) for c in counts],
        ]
        sems = [pltpu.SemaphoreType.DMA(s) for s in ((20,), *[(FIELDS, 3, 2)] * 2, *[(sum(counts),)] * 2, *[(12,)] * 2, *[(15,)] * 2)]

        def scoped(*refs):
            plain, slots_of = refs[: -len(counts)], refs[-len(counts) :]
            pl.run_scoped(functools.partial(kernel, sizes, *plain, slots_of), *sems)

        field = pltpu.VMEM(residual.shape, f32)
        limit = 67_043_328 - 12 * math.prod(residual.shape) - 2**18
        fields = pl.pallas_call(
            scoped,
            out_shape=[field] * 3 + [pltpu.VMEM(s, f32) for s in ((8, n2), (3, n1, n2), (3, n0, n2), (3, vecs, 8, n2))],
            in_specs=[pl.BlockSpec(memory_space=pltpu.HBM)] * 4,
            out_specs=[pl.BlockSpec(memory_space=pltpu.VMEM)] * 7,
            scratch_shapes=scratch,
            compiler_params=pltpu.CompilerParams(collective_id=0, has_side_effects=True, vmem_limit_bytes=limit),
        )(residual, edge_diag, node_shift, coarse_shift)
        parts = 2 if n0 % 2 == 0 else 1
        return pl.pallas_call(
            functools.partial(combine, parts),
            out_shape=jax.ShapeDtypeStruct(residual.shape, f32),
            in_specs=[pl.BlockSpec(memory_space=pltpu.VMEM)] * 7,
            out_specs=pl.BlockSpec(memory_space=pltpu.HBM),
            scratch_shapes=[field, pltpu.SemaphoreType.DMA((3 * parts,))],
            compiler_params=pltpu.CompilerParams(vmem_limit_bytes=8 * math.prod(residual.shape)),
        )(*fields)

    placed = (
        P(None, "gz", "gx", "gy"),
        P(None, "gz", "gx", "gy"),
        P("gz", "gx", "gy"),
        P("gz", "gx", "gy"),
    )
    return jax.shard_map(
        local, mesh=mesh, in_specs=placed, out_specs=P(None, "gz", "gx", "gy"), check_vma=False
    )
```

```python
import functools
import itertools
import math

import jax
import jax.numpy as jnp
from jax import lax
from jax.experimental import pallas as pl
from jax.experimental.pallas import tpu as pltpu
from jax.sharding import PartitionSpec as P

MESH = pl.DeviceIdType.MESH
AXES = ("gz", "gx", "gy")
PI, V1I, V2I, F0I, NLI, CII, NII, FGI = 3, 4, 5, 6, 9, 10, 11, 12
FIELDS = 13
FINAL = (F0I, F0I + 1, F0I + 2)
COARSE = (V1I, V2I, NLI, CII)
LOCAL = (V2I, FGI)
CROSS = [(a, b, d) for a in range(3) for b in range(3) if a != b for d in (0, 1)]
GREET = [(a, b, 2) for a in range(3) for b in range(a)]
PAD = 8
FEW = 32


def fence():
    pl.delay(1)


def phases_of(sizes):
    return ((0, 1, 2),) if math.prod(sizes) <= FEW else ((1, 2), (0,))


def greeted(sizes, rounds):
    near = set(itertools.product((-1, 0, 1), repeat=3))
    known = set(near)
    for moves in rounds:
        known |= {tuple(p + q for p, q in zip(k, m)) for k in known for m in moves}
    needed = set()
    for axes in phases_of(sizes):
        spans = [range(1 - sizes[a], sizes[a]) if a in axes else (0,) for a in range(3)]
        needed |= set(itertools.product(*spans))
    every = near | (needed - known)
    return sorted(o for o in every if any(o) and all(abs(p) < n for p, n in zip(o, sizes)))


def kernel(
    sizes,
    res, dia, shf, csh, OB, G1, G2, CO, HZ, HX, HY,
    R, D, NI, CS, S, FG, CI, CR, A1, NL, T, V1, V2, F,
    SX, RX, SY, RY, NZ, CZ, LZX, LXY, RZX, RZY, RXY,
    P, PZ, NZI, LRZ, LRX, LY2, LY1, LP0, RRZ, RRX, RZ2, RZ0, RX2, RX1, DX, HELLO,
    slots_of,
    in_sem, send_sem, recv_sem, psend, precv, lsend, lrecv, csend, crecv,
):
    phases = phases_of(sizes)
    n0, n1, n2 = NI.shape
    m0, m1, m2 = CS.shape
    groups = n1 // 8
    me = [lax.axis_index(a) for a in AXES]
    rows = pl.ds(PAD, n1)

    def offsets(axes):
        every = itertools.product(*[range(sizes[a]) for a in axes])
        return [offs for offs in every if any(offs)]

    def partner(axes, offs, sign):
        return {
            AXES[a]: lax.rem(me[a] + (o if sign > 0 else sizes[a] - o), sizes[a]) for a, o in zip(axes, offs)
        }

    barrier = pltpu.get_barrier_semaphore()
    faces = [offs for offs in itertools.product((-1, 0, 1), repeat=3) if sum(map(abs, offs)) == 1]
    lines = [offs for offs in itertools.product((-1, 0, 1), repeat=3) if sum(map(abs, offs)) == 2]

    def exists(offs):
        inside = [(me[a] + o >= 0) & (me[a] + o < sizes[a]) for a, o in enumerate(offs) if o]
        return functools.reduce(jnp.logical_and, inside)

    def device(offs):
        return {AXES[a]: me[a] + o for a, o in enumerate(offs) if o}

    total = jnp.int32(0)
    for offs in greeted(sizes, (faces + lines, faces + lines)):
        there = exists(offs)
        pl.when(there)(
            lambda offs=offs: pl.semaphore_signal(
                barrier, inc=1, device_id=device(offs), device_id_type=MESH
            )
        )
        total = total + there.astype(jnp.int32)

    bands = (0, n1 - 8)
    loads = {}

    def load(key, src, dst):
        loads[key] = pltpu.make_async_copy(src, dst, in_sem.at[len(loads)])
        loads[key].start()

    load(3, shf, NI)
    for first, count in [(r, 8) for r in bands] + [(8, n1 - 16)]:
        at = pl.ds(first, count)
        for k in (1, 2, 0):
            load((k, first, 0), res.at[k, :, at], R.at[k, :, at])
            load((k, first, 1), dia.at[k, :, at], D.at[k, :, at])
    load(4, csh, CS)

    for k in range(3):
        for i in range(n0):
            F[k, i, n1 : n1 + 1] = jnp.zeros((1, n2), jnp.float32)
    DX[...] = jnp.zeros(DX.shape, jnp.float32)

    def clear(offs, *refs):
        @pl.when(jnp.logical_not(exists(offs)))
        def _():
            for ref in refs:
                ref[...] = jnp.zeros(ref.shape, jnp.float32)

    for d in (0, 1):
        step, i, c = (1, n0 + 1, m0 + 1) if d else (-1, 0, 0)
        planes = [S.at[k, i, rows] for k in range(3)] + [V1.at[c, rows], NZ.at[d], CZ.at[d], PZ.at[d], NZI.at[d]]
        clear((step, 0, 0), *planes, *([F.at[k, n0, pl.ds(0, n1)] for k in range(3)] if d else []))
        clear((0, step, 0), *[RX.at[f, d] for f in range(FIELDS) if f not in LOCAL])
        clear((0, 0, step), *[RY.at[f, d] for f in range(FIELDS) if f not in LOCAL])
    for offs in lines:
        z, x, y = [int(o > 0) for o in offs]
        clear(offs, RXY.at[x, y] if not offs[0] else RZY.at[z, y] if not offs[1] else RZX.at[z, x])

    lane = lax.broadcasted_iota(jnp.int32, (8, n2), 1)
    lane_full = lax.broadcasted_iota(jnp.int32, (n1, n2), 1)
    row_full = lax.broadcasted_iota(jnp.int32, (n1, n2), 0)
    row8 = lax.broadcasted_iota(jnp.int32, (8, n2), 0)
    keys = {p: ((lane + p // 2) // p) % (n2 // p) for p in (2, 4)}
    is_low = {p: (lane % p) >= p // 2 for p in (2, 4)}

    def place(i, g, p):
        k = i * groups + g
        per = n2 // p
        return k // per, k % per

    def gather(blocks, p):
        accs = {}
        for (i, g), part in blocks:
            v, kk = place(i, g, p)
            if kk:
                part = pltpu.roll(part, p * kk, 1)
            accs[v] = jnp.where(keys[p] == kk, part, accs.get(v, 0.0))
        return accs

    def pack(f, plane, count, p):
        at = [(i, g) for i in range(count) for g in range(groups)]
        planes = [plane(i) for i in range(count)]
        accs = gather([((i, g), planes[i][8 * g : 8 * g + 8]) for i, g in at], p)
        for v, acc in accs.items():
            SY[f, v] = acc

    def halo(ws, i, p):
        parts = []
        for g in range(groups):
            v, kk = place(i, g, p)
            parts.append(pltpu.roll(ws[v], n2 - p * kk, 1) if kk else ws[v])
        return jnp.concatenate(parts, axis=0)

    def inplane(ref, x, h, sh):
        near = ref[pl.ds(PAD - sh, n1)] + ref[pl.ds(PAD + sh, n1)]
        near = near + jnp.where(lane_full < sh, h, pltpu.roll(x, sh, 1))
        return near + jnp.where(lane_full >= n2 - sh, h, pltpu.roll(x, n2 - sh, 1))

    def local_near(ref, i, n, sh):
        x = ref[1 + i, rows]
        near = jnp.where(row_full >= sh, ref[1 + i, pl.ds(PAD - sh, n1)], 0.0)
        near = near + jnp.where(row_full < n1 - sh, ref[1 + i, pl.ds(PAD + sh, n1)], 0.0)
        near = near + jnp.where(lane_full >= sh, pltpu.roll(x, sh, 1), 0.0)
        near = near + jnp.where(lane_full < n2 - sh, pltpu.roll(x, n2 - sh, 1), 0.0)
        if i > 0:
            near = near + ref[i, rows]
        if i < n - 1:
            near = near + ref[i + 2, rows]
        return near

    def edges(f, p):
        sh = p // 2
        return [
            jnp.where(is_low[p], pltpu.roll(RY[f, 1, v], n2 - sh, 1), pltpu.roll(RY[f, 0, v], sh, 1))
            for v in range(RY.shape[2])
        ]

    def outer_near(near, ref, f, ws, i, n, p):
        sh = p // 2
        if i == 0:
            near = near + ref[0, rows]
        if i == n - 1:
            near = near + ref[n + 1, rows]
        side = (lane_full < sh) | (lane_full >= n2 - sh)
        near = near + jnp.where(side, halo(ws, i, p), 0.0)
        low = near[0:8] + jnp.where(row8 < sh, RX[f, 0, i : i + 1], 0.0)
        high = near[n1 - 8 : n1] + jnp.where(row8 >= 8 - sh, RX[f, 1, i : i + 1], 0.0)
        return jnp.concatenate([low, near[8 : n1 - 8], high], axis=0)

    def field(f):
        if f < 3:
            return S.at[f], n0
        return {V1I: (V1, m0)}[f]

    ZBUF = {NLI: (NL, NZ, m0), CII: (CI, CZ, m0), PI: (P, PZ, n0), NII: (NI, NZI, n0)}

    def message(f, a, d):
        if a == 0:
            if f in FINAL:
                src, dst = F.at[f - F0I, 0, pl.ds(0, n1)], F.at[f - F0I, n0, pl.ds(0, n1)]
            elif f in ZBUF:
                src, dst, n = ZBUF[f]
                src, dst = src.at[n - 1 if d else 0], dst.at[1 - d]
            else:
                ref, n = field(f)
                src = ref.at[n if d else 1, rows]
                dst = ref.at[0 if d else n + 1, rows]
        elif a == 1:
            count = m0 if f in COARSE else n0
            src, dst = SX.at[f, d, pl.ds(0, count)], RX.at[f, 1 - d, pl.ds(0, count)]
        else:
            src, dst = SY.at[f], RY.at[f, 1 - d]
        step = 1 if d else -1
        return pltpu.make_async_remote_copy(
            src_ref=src, dst_ref=dst, send_sem=send_sem.at[f, a, d], recv_sem=recv_sem.at[f, a, d],
            device_id={AXES[a]: lax.rem(me[a] + step + sizes[a], sizes[a])}, device_id_type=MESH,
        )

    def dirs(f):
        return (0,) if f in FINAL else (0, 1)

    def can_send(a, d):
        return me[a] < sizes[a] - 1 if d else me[a] > 0

    def send(f, a, only=(0, 1)):
        for d in [d for d in dirs(f) if d in only]:
            pl.when(can_send(a, d))(lambda f=f, a=a, d=d: message(f, a, d).start())

    def receive(f, a, only=(0, 1)):
        for d in [d for d in dirs(f) if d in only]:
            pl.when(can_send(a, 1 - d))(lambda f=f, a=a, d=d: message(f, a, d).wait_recv())

    def faces_x(f, get, count):
        for i in range(count):
            SX[f, 0, i : i + 1] = get(i, 0)
            if f not in FINAL:
                SX[f, 1, i : i + 1] = get(i, n1 - 1)

    def rows_x(f, ref):
        width = 2 if f in COARSE else 1
        for i in range(m0 if f in COARSE else n0):
            for w in range(width):
                ref[1 + i, PAD - 1 - w : PAD - w] = RX[f, 0, i : i + 1]
                ref[1 + i, PAD + n1 + w : PAD + n1 + w + 1] = RX[f, 1, i : i + 1]

    def line_message(offs, sign):
        z, x, y = [o * sign for o in offs]
        side = [0 if o > 0 else 1 for o in (z, x, y)]
        if not y:
            src, dst = LZX.at[1 - side[0], 1 - side[1]], RZX.at[side[0], side[1]]
        elif not x:
            plane = place(m0 - 1 if z > 0 else 0, 0, 4)[0]
            src, dst = SY.at[V1I, plane], RZY.at[side[0], side[2]]
        else:
            src, dst = LXY.at[1 - side[1]], RXY.at[side[1], side[2]]
        at = lines.index((z, x, y))
        return pltpu.make_async_remote_copy(
            src_ref=src, dst_ref=dst, send_sem=lsend.at[at], recv_sem=lrecv.at[at],
            device_id=device((z, x, y)), device_id_type=MESH,
        )

    def cross_message(a, b, d, sign):
        src, dst = (LRZ.at[0], HELLO.at[a + b - 1]) if d == 2 else {
            (0, 1): (LRZ.at[d], RRZ.at[d]),
            (1, 0): (LRX.at[d], RRX.at[d]),
            (0, 2): (SY.at[2, place(0 if d else n0 - 1, 0, 2)[0]], RZ2.at[d]),
            (2, 0): (LP0, RZ0.at[d]),
            (1, 2): (LY2.at[d], RX2.at[d]),
            (2, 1): (LY1, RX1.at[d]),
        }[a, b]
        at = (CROSS + GREET).index((a, b, d))
        return pltpu.make_async_remote_copy(
            src_ref=src, dst_ref=dst, send_sem=csend.at[at], recv_sem=crecv.at[at],
            device_id=device(cross_offs(a, b, d, sign)), device_id_type=MESH,
        )

    def cross_offs(a, b, d, sign):
        offs = [0, 0, 0]
        offs[a], offs[b] = (-sign if d else sign), (-sign if d == 2 else sign)
        return tuple(offs)

    CROSS_INTO = {(0, 1): RRZ, (1, 0): RRX, (0, 2): RZ2, (2, 0): RZ0, (1, 2): RX2, (2, 1): RX1}
    for a, b, d in CROSS:
        clear(cross_offs(a, b, d, -1), CROSS_INTO[a, b].at[d])

    def cross_rows():
        for d in (0, 1):
            i, r = (0 if d else n0 - 1), (0 if d else n1 - 1)
            LRZ[d] = S[1, 1 + i, PAD + n1 - 1 : PAD + n1]
            LRX[d] = S[0, n0, PAD + r : PAD + r + 1]
        for k, g in ((2, groups - 1), (2, 0), (1, groups - 1)):
            top = [((i, g), S[k, 1 + i, PAD + 8 * g : PAD + 8 * g + 8]) for i in range(n0)]
            for v, acc in gather(top, 2).items():
                line = acc[7:8] if g else acc[0:1]
                if k == 2:
                    LY2[0 if g else 1, v] = line
                else:
                    LY1[v] = line

    def cross_plane():
        top = [((n0 - 1, g), S[0, n0, PAD + 8 * g : PAD + 8 * g + 8]) for g in range(groups)]
        for acc in gather(top, 2).values():
            LP0[...] = acc

    def rows_rhs():
        rowi = lax.broadcasted_iota(jnp.int32, (n0, n2), 0)
        lanei = lax.broadcasted_iota(jnp.int32, (n0, n2), 1)
        inner = [S[1, 1 + i, PAD + n1 - 2 : PAD + n1 - 1] for i in range(n0)]
        for d in (0, 1):
            x = jnp.where(rowi >= 1, pltpu.roll(SX[0, d], 1, 0), 0.0) - SX[0, d]
            x = x + jnp.where(lanei >= 1, pltpu.roll(SX[2, d], 1, 1), 0.0) - SX[2, d]
            SX[PI, d] = x - SX[1, d] + jnp.concatenate(inner, axis=0) if d else x - SX[1, d]

    def cross_send(which):
        for at in [at for at in CROSS + GREET if (at[:2] in ((0, 2), (2, 0)) and at[2] < 2) == which]:
            pl.when(exists(cross_offs(*at, 1)))(lambda at=at: cross_message(*at, 1).start())

    def cross_receive():
        for at in CROSS + GREET:
            pl.when(exists(cross_offs(*at, -1)))(lambda at=at: cross_message(*at, -1).wait_recv())

    def halo_fg():
        for d in (0, 1):
            kk = place(0 if d else n0 - 1, 0, 2)[1]
            rhs = PZ[d] + S[0, n0, rows] if d else PZ[d]
            col = [pltpu.roll(RZ2[d], (2 * n2 - 2 * (kk + g) + 1) % n2, 1) for g in range(groups)]
            rhs = rhs + jnp.where(lane_full < 1, jnp.concatenate(col, axis=0), 0.0)
            first = rhs[0:8] + jnp.where(row8 < 1, RRZ[d], 0.0)
            FG[(n0 + 1) * d, rows] = jnp.concatenate([first, rhs[8:]], axis=0) * NZI[d]
        rowi = lax.broadcasted_iota(jnp.int32, (n0, n2), 0)
        lanei = lax.broadcasted_iota(jnp.int32, (n0, n2), 1)
        per = n2 // 2
        for d in (0, 1):
            rhs = RX[PI, d] + SX[1, 1] if d else RX[PI, d]
            rhs = rhs + jnp.where(rowi == 0, RRX[d], 0.0)
            index = rowi * groups + (0 if d else groups - 1)
            at = lax.rem(2 * lax.rem(index, per) + n2 - 1, n2)
            got = jnp.zeros((n0, n2), jnp.float32)
            for v in range(RX2.shape[1]):
                here = (lanei == at) & (index >= v * per) & (index < (v + 1) * per)
                got = got + jnp.where(here, RX2[d, v], 0.0)
            rhs = rhs + jnp.where(lanei < 1, jnp.sum(got, axis=1, keepdims=True), 0.0)
            RX[FGI, d] = rhs * RX[NII, d]
        ws = []
        for v, (ep, en) in enumerate(zip(edges(PI, 2), edges(NII, 2))):
            rhs = ep + jnp.where(is_low[2], SY[2, v], 0.0)
            if v == 0:
                k0 = place(n0 - 1, 0, 2)[1]
                moved = pltpu.roll(align(RZ0[0], RZ0[1], 2), (n2 - 2 * k0) % n2, 1)
                rhs = rhs + jnp.where(keys[2] < groups, moved, 0.0)
            line = align(jnp.broadcast_to(RX1[0, v], (8, n2)), jnp.broadcast_to(RX1[1, v], (8, n2)), 2)
            line = pltpu.roll(line, n2 - 2 * (groups - 1), 1)
            here = (lax.rem(keys[2], groups) == 0) & (row8 < 1)
            ws.append((rhs + jnp.where(here, line, 0.0)) * en)
        return ws

    def lines_send(which):
        for offs in [offs for offs in lines if which(offs)]:
            pl.when(exists(offs))(lambda offs=offs: line_message(offs, 1).start())

    def lines_receive():
        for offs in lines:
            pl.when(exists(offs))(lambda offs=offs: line_message(offs, -1).wait_recv())

    def align(low, high, p):
        return jnp.where(is_low[p], pltpu.roll(high, n2 - p // 2, 1), pltpu.roll(low, p // 2, 1))

    def halo_v2(ev, enl, eci):
        sh, kgroup = 2, [place(c, 0, 4) for c in (m0 - 1, 0)]
        col = [align(RZY[d, 0], RZY[d, 1], 4) for d in (0, 1)]
        for d, edge in ((0, 0), (1, m0 + 1)):
            v, kk = kgroup[d]
            near = NZ[d] + V1[1 if d == 0 else m0, rows]
            parts = [pltpu.roll(col[d], (n2 - 4 * (kk + g)) % n2, 1) for g in range(groups)]
            side = (lane_full < sh) | (lane_full >= n2 - sh)
            near = near + jnp.where(side, jnp.concatenate(parts, axis=0), 0.0)
            low = near[0:8] + jnp.where(row8 < sh, RZX[d, 0], 0.0)
            high = near[n1 - 8 : n1] + jnp.where(row8 >= 8 - sh, RZX[d, 1], 0.0)
            near = jnp.concatenate([low, near[8 : n1 - 8], high], axis=0)
            V2[edge, rows] = V1[edge, rows] - CZ[d] * near
        rowc = lax.broadcasted_iota(jnp.int32, (m0, n2), 0)
        lanec = lax.broadcasted_iota(jnp.int32, (m0, n2), 1)
        per = n2 // 4
        for d in (0, 1):
            near = RX[NLI, d, 0:m0] + SX[V1I, d, 0:m0]
            near = near + jnp.where(rowc == 0, RZX[0, d], 0.0) + jnp.where(rowc == m0 - 1, RZX[1, d], 0.0)
            for y in (0, 1):
                index = rowc * groups + (groups - 1 if d == 0 else 0)
                at = lax.rem(4 * lax.rem(index, per) + (n2 - 1 if y == 0 else 0), n2)
                got = jnp.zeros((m0, n2), jnp.float32)
                for v in range(RXY.shape[2]):
                    here = (lanec == at) & (index >= v * per) & (index < (v + 1) * per)
                    got = got + jnp.where(here, RXY[d, y, v], 0.0)
                got = jnp.sum(got, axis=1, keepdims=True)
                near = near + jnp.where((lanec < sh) if y == 0 else (lanec >= n2 - sh), got, 0.0)
            RX[V2I, d, 0:m0] = RX[V1I, d, 0:m0] - RX[CII, d, 0:m0] * near
        ws = []
        for v in range(len(ev)):
            near = enl[v] + SY[V1I, v]
            for d, c in ((0, 0), (1, m0 - 1)):
                into, k0 = place(c, 0, 4)
                if into == v:
                    shift = (4 * (k0 - kgroup[d][1])) % n2
                    moved = pltpu.roll(col[d], shift, 1) if shift else col[d]
                    near = near + jnp.where((keys[4] >= k0) & (keys[4] < k0 + groups), moved, 0.0)
            for d in (0, 1):
                line = align(
                    jnp.broadcast_to(RXY[d, 0, v], (8, n2)), jnp.broadcast_to(RXY[d, 1, v], (8, n2)), 4
                )
                jump = 4 * (groups - 1)
                line = pltpu.roll(line, n2 - jump if d == 0 else jump, 1)
                here = lax.rem(keys[4], groups) == (0 if d == 0 else groups - 1)
                here = here & ((row8 < sh) if d == 0 else (row8 >= 8 - sh))
                near = near + jnp.where(here, line, 0.0)
            ws.append(ev[v] - eci[v] * near)
        return ws

    def one(f, a, only=(0, 1)):
        ref, count = field(f)
        if a == 2:
            pack(f, lambda i: ref[1 + i, rows], count, 2)
        send(f, a, only)

    def spread_faces(f, ref, n, p):
        send(f, 0)
        faces_x(f, lambda c, r: ref[c, r : r + 1], n)
        send(f, 1)
        pack(f, lambda c: ref[c], n, p)
        send(f, 2)

    def shifted(i):
        return jnp.where(lane_full >= 1, pltpu.roll(S[2, 1 + i, rows], 1, 1), 0.0)

    def pack_last():
        blocks = [((i, g), S[2, 1 + i, PAD + 8 * g : PAD + 8 * g + 8]) for i in range(n0) for g in range(groups)]
        accs = gather(blocks, 4)
        half = n2 // 4
        at = 4 * lax.rem(keys[2], half) + n2
        found = []
        for back in (1, 2):
            source = lax.rem(at - jnp.where(is_low[2], back, 0), n2)
            for v in range(RY.shape[2]):
                x, y = [jnp.take_along_axis(accs[min(2 * v + h, len(accs) - 1)], source, axis=1) for h in (0, 1)]
                found.append(jnp.where(keys[2] < half, x, y))
        for v in range(RY.shape[2]):
            SY[2, v] = found[v]
        return found[RY.shape[2] :]

    def scale(k, first, count):
        at = pl.ds(first, count)
        for part in (0, 1):
            loads[k, first, part].wait()
        inv = 1.0 / D[k, :, at]
        D[k, :, at] = inv
        S[k, pl.ds(1, n0), pl.ds(PAD + first, count)] = R[k, :, at] * inv

    loads[3].wait()
    for i in range(n0):
        NI[i] = 1.0 / (6.0 + NI[i])
    faces_x(NII, lambda i, r: NI[i, r : r + 1], n0)
    pack(NII, lambda i: NI[i], n0, 2)
    for k in (1, 2, 0):
        for first in bands:
            scale(k, first, 8)
        faces_x(k, lambda i, r: S[k, 1 + i, PAD + r : PAD + r + 1], n0)
    cross_rows()
    rows_rhs()
    pl.semaphore_wait(barrier, total)
    fence()
    cross_send(False)
    send(1, 1, (1,))
    send(PI, 1)
    send(NII, 1)
    send(NII, 2)
    send(NII, 0)
    fence()
    for k in (1, 2, 0):
        scale(k, 8, n1 - 16)
        if k == 2:
            last2 = pack_last()
            send(2, 2, (1,))
    send(0, 0, (1,))
    cross_plane()
    cross_send(True)
    for i in range(n0):
        x1 = S[1, 1 + i, rows]
        rhs = jnp.where(row_full >= 1, S[1, 1 + i, pl.ds(PAD - 1, n1)], 0.0) - x1 - S[2, 1 + i, rows]
        rhs = rhs - S[0, 1 + i, rows]
        if i > 0:
            rhs = rhs + S[0, i, rows]
        P[i] = rhs
    pack(PI, lambda i: P[i], n0, 2)
    for v, x in enumerate(last2):
        SY[PI, v] = SY[PI, v] + jnp.where(is_low[2], x, 0.0)
    send(PI, 2)
    for i in (0, n0 - 1):
        P[i] = P[i] + shifted(i)
    send(PI, 0)
    fence()
    loads[4].wait()
    spread_cols = (
        lax.broadcasted_iota(jnp.int32, (m2, n2), 1) // 2 == lax.broadcasted_iota(jnp.int32, (m2, n2), 0)
    ).astype(jnp.float32)
    inverse = (1.0 / (6.0 + CS[...])).reshape(m0 * m1, m2)
    inverse = jnp.dot(
        inverse, spread_cols, precision=lax.Precision.HIGHEST, preferred_element_type=jnp.float32
    ).reshape(m0, m1, n2)
    for c in range(m0):
        for r in (0, 1):
            CI[c, pl.ds(r, m1, stride=2)] = inverse[c]
    spread_faces(CII, CI, m0, 4)

    for i in range(n0):
        if 0 < i < n0 - 1:
            P[i] = P[i] + shifted(i)
        FG[1 + i, rows] = P[i] * NI[i]

    def gradients(j, G):
        for i in range(n0):
            x = F[j, i, 0:n1]
            above = F[j, i + 1, 0:n1] - x if i < n0 - 1 else -x
            ahead = jnp.where(lane_full >= n2 - 1, 0.0, pltpu.roll(x, n2 - 1, 1)) - x
            for k, grad in enumerate((above, F[j, i, 1 : n1 + 1] - x, ahead)):
                G[k, i] = G[k, i] + grad if j == 0 else grad


    def smooth(k):
        for a in range(3):
            receive(k, a, (0,) if (k, a) in from_low else (0, 1))
        rows_x(k, S.at[k])
        w = edges(k, 2)
        for i in range(n0):
            x = S[k, 1 + i, rows]
            near = S[k, i, rows] + S[k, i + 2, rows] + inplane(S.at[k, 1 + i], x, halo(w, i, 2), 1)
            OB[k, i] = x + near * D[k, i]

    for i in range(n0):
        F[0, i, 0:n1] = local_near(FG, i, n0, 1)

    def pair_rows(t, slot):
        t = t + jnp.where(lane_full % 2 == 0, pltpu.roll(t, n2 - 1, 1), pltpu.roll(t, 1, 1))
        T[slot, rows] = t
        return t + jnp.where(row_full % 2 == 0, T[slot, pl.ds(PAD + 1, n1)], T[slot, pl.ds(PAD - 1, n1)])

    for c in range(m0):
        CR[c] = pair_rows(F[0, 2 * c, 0:n1] + F[0, 2 * c + 1, 0:n1], c)
    from_low = ((0, 0), (1, 1), (2, 2))
    for f, a in from_low:
        receive(f, a, (1,))
    low2 = [jnp.where(is_low[2], 0.0, pltpu.roll(RY[2, 0, v], 1, 1)) for v in range(RY.shape[2])]
    add = S[0, 0, rows] * NI[0]
    T[2, rows] = add
    t = add + jnp.where(row_full >= 1, T[2, pl.ds(PAD - 1, n1)], 0.0)
    t = t + jnp.where(row_full < n1 - 1, T[2, pl.ds(PAD + 1, n1)], 0.0)
    t = t + jnp.where(lane_full >= 1, pltpu.roll(add, 1, 1), 0.0)
    t = t + jnp.where(lane_full < n2 - 1, pltpu.roll(add, n2 - 1, 1), 0.0)
    A1[0] = t
    lanei = lax.broadcasted_iota(jnp.int32, (n0, n2), 1)
    add = RX[1, 0] * SX[NII, 0]
    DX[pl.ds(PAD, n0)] = add
    x = add + DX[pl.ds(PAD - 1, n0)] + DX[pl.ds(PAD + 1, n0)]
    x = x + jnp.where(lanei >= 1, pltpu.roll(add, 1, 1), 0.0)
    SX[FGI, 0] = x + jnp.where(lanei < n2 - 1, pltpu.roll(add, n2 - 1, 1), 0.0)
    adds = [e * SY[NII, v] for v, e in enumerate(low2)]
    group, hop, per = lax.rem(keys[2], groups), 2 * groups, n2 // 2
    source = 2 * (2 * groups * (keys[4] // groups) + keys[4] % groups) + n2 - is_low[4].astype(jnp.int32)
    source = lax.rem(source, n2)
    spread = []
    for v, add in enumerate(adds):
        ahead = jnp.where(group < groups - 1, pltpu.roll(pltpu.roll(add, n2 - 2, 1), 7, 0), 0.0)
        behind = jnp.where(group > 0, pltpu.roll(pltpu.roll(add, 2, 1), 1, 0), 0.0)
        w = add + jnp.where(row8 < 7, pltpu.roll(add, 7, 0), ahead)
        w = w + jnp.where(row8 > 0, pltpu.roll(add, 1, 0), behind)
        ahead = pltpu.roll(adds[v + 1], n2 - hop, 1) if v + 1 < len(adds) else 0.0
        behind = pltpu.roll(adds[v - 1], hop, 1) if v else 0.0
        w = w + jnp.where(keys[2] < per - groups, pltpu.roll(add, n2 - hop, 1), ahead)
        w = w + jnp.where(keys[2] >= groups, pltpu.roll(add, hop, 1), behind)
        spread.append(w)
    for f in (NII, PI):
        for a in range(3):
            receive(f, a)
    cross_receive()
    ws = halo_fg()
    CR[0] = CR[0] + pair_rows(FG[0, rows] + A1[0], 0)
    CR[m0 - 1] = CR[m0 - 1] + pair_rows(FG[n0 + 1, rows], 1)
    SX[FGI, 0] = SX[FGI, 0] + RX[FGI, 0]
    SX[FGI, 1] = RX[FGI, 1]
    even = lax.broadcasted_iota(jnp.int32, (m0, n2), 1) % 2 == 0
    for d in (0, 1):
        x = SX[FGI, d, pl.ds(0, m0, stride=2)] + SX[FGI, d, pl.ds(1, m0, stride=2)]
        RX[V2I, d, 0:m0] = x + jnp.where(even, pltpu.roll(x, n2 - 1, 1), pltpu.roll(x, 1, 1))
    blocks = []
    for v, (w, add) in enumerate(zip(ws, spread)):
        w = w + add
        w = w + pltpu.roll(w, n2 - hop, 1)
        w = w + jnp.where(row8 % 2 == 0, pltpu.roll(w, 7, 0), pltpu.roll(w, 1, 0))
        blocks.append(jnp.take_along_axis(w, source, axis=1))
    side = (lane_full < 2) | (lane_full >= n2 - 2)
    for c in range(m0):
        t = CR[c] + jnp.where(side, halo(blocks, c, 4), 0.0)
        low = t[0:8] + jnp.where(row8 < 2, RX[V2I, 0, c : c + 1], 0.0)
        high = t[n1 - 8 : n1] + jnp.where(row8 >= 6, RX[V2I, 1, c : c + 1], 0.0)
        t = jnp.concatenate([low, t[8 : n1 - 8], high], axis=0)
        CR[c] = t
        V1[1 + c, rows] = t * CI[c]
    rowc = lax.broadcasted_iota(jnp.int32, (m0, n2), 0)
    lanec = lax.broadcasted_iota(jnp.int32, (m0, n2), 1)
    faces_x(V1I, lambda c, r: V1[1 + c, PAD + r : PAD + r + 1], m0)
    send(V1I, 1)
    fence()
    for z in (0, 1):
        for x in (0, 1):
            c = (m0 - 1) * z
            LZX[z, x] = SX[V1I, x, c : c + 1]
    for x in (0, 1):
        g = (groups - 1) * x
        ends = [((c, g), V1[1 + c, PAD + 8 * g : PAD + 8 * g + 8]) for c in range(m0)]
        for v, acc in gather(ends, 4).items():
            LXY[x, v] = acc[7 * x : 7 * x + 1]
    lines_send(lambda offs: offs[1] != 0)
    for d, r in ((0, 2), (1, n1 - 3)):
        x = SX[V1I, d, 0:m0]
        near = jnp.concatenate([V1[1 + c, PAD + r : PAD + r + 1] for c in range(m0)], axis=0)
        near = near + jnp.where(rowc >= 1, pltpu.roll(x, 1, 0), 0.0)
        near = near + jnp.where(rowc < m0 - 1, pltpu.roll(x, m0 - 1, 0), 0.0)
        near = near + jnp.where(lanec >= 2, pltpu.roll(x, 2, 1), 0.0)
        SX[NLI, d, 0:m0] = near + jnp.where(lanec < n2 - 2, pltpu.roll(x, n2 - 2, 1), 0.0)
    send(NLI, 1)
    send(V1I, 0)
    pack(V1I, lambda c: V1[1 + c, rows], m0, 4)
    lines_send(lambda offs: offs[1] == 0)
    send(V1I, 2)
    fence()
    for c in range(m0):
        NL[c] = local_near(V1, c, m0, 2)
    send(NLI, 0)
    pack(NLI, lambda c: NL[c], m0, 4)
    send(NLI, 2)
    fence()

    def faces_f(j):
        f = F0I + j
        send(f, 0)
        faces_x(f, lambda i, r: F[j, i, r : r + 1], n0)
        send(f, 1)
        pack(f, lambda i: F[j, i, 0:n1], n0, 2)
        send(f, 2)

    for f, a in ((0, 1), (2, 1), (1, 0), (2, 0), (0, 2), (1, 2)):
        one(f, a)
    for f, a in from_low:
        send(f, a, (0,))
    for i in range(n0):
        rhs = P[i] + jnp.where(lane_full < 1, halo(low2, i, 2), 0.0)
        if i == 0:
            rhs = rhs + S[0, 0, rows]
        first = rhs[0:8] + jnp.where(row8 < 1, RX[1, 0, i : i + 1], 0.0)
        FG[1 + i, rows] = jnp.concatenate([first, rhs[8:]], axis=0) * NI[i]
    for i in range(n0):
        near = outer_near(local_near(FG, i, n0, 1), FG, FGI, ws, i, n0, 2)
        F[0, i, 0:n1] = FG[1 + i, rows] + near * NI[i]
    faces_f(0)

    def fold(x):
        acc = x[0:8]
        for g in range(1, groups):
            acc = acc + x[8 * g : 8 * g + 8]
        return acc

    sums = [jnp.zeros((8, n2), jnp.float32) for _ in range(4)]
    for c in range(m0):
        sums[0] = sums[0] + fold(V1[1 + c, rows] * CR[c])

    for f in (CII, V1I, NLI):
        for a in range(3):
            receive(f, a)
    lines_receive()
    ws = edges(V1I, 4)
    for c in range(m0):
        near = outer_near(NL[c], V1, V1I, ws, c, m0, 4)
        A1[c] = CR[c] - near
        V2[1 + c, rows] = V1[1 + c, rows] - near * CI[c]
    faces_x(V2I, lambda c, r: V2[1 + c, PAD + r : PAD + r + 1], m0)
    pack(V2I, lambda c: V2[1 + c, rows], m0, 4)
    w2 = halo_v2(ws, edges(NLI, 4), edges(CII, 4))

    def spread_near(j, V, w):
        for c in range(m0):
            x = V[1 + c, rows]
            near = x + inplane(V.at[1 + c], x, halo(w, c, 4), 1)
            F[j, 2 * c, 0:n1] = (near + V[c, rows]) * NI[2 * c]
            F[j, 2 * c + 1, 0:n1] = (near + V[c + 2, rows]) * NI[2 * c + 1]
        faces_f(j)

    for c in range(m0):
        v1, v2, a1 = V1[1 + c, rows], V2[1 + c, rows], A1[c]
        near = jnp.where(row_full < n1 - 2, V2[1 + c, pl.ds(PAD + 2, n1)], 0.0)
        near = near + jnp.where(lane_full < n2 - 2, pltpu.roll(v2, n2 - 2, 1), 0.0)
        if c < m0 - 1:
            near = near + V2[2 + c, rows]
        sums[1] = sums[1] + fold(v1 * a1)
        sums[2] = sums[2] + fold(v2 * a1)
        sums[3] = sums[3] + fold(v2 * (a1 - 2.0 * near))
    outer = fold(V2[1, rows] * V2[0, rows] + V2[m0, rows] * V2[m0 + 1, rows])
    for v, w in enumerate(w2):
        outer = outer + SY[V2I, v] * w
    rim = SX[V2I, 0, 0:m0] * RX[V2I, 0, 0:m0] + SX[V2I, 1, 0:m0] * RX[V2I, 1, 0:m0]
    sums[3] = sums[3] - outer
    rim = 2.0 * jnp.sum(rim, axis=0, keepdims=True)
    sums[3] = sums[3] - jnp.where(row8 == 0, rim, 0.0)
    lane1 = lax.broadcasted_iota(jnp.int32, (1, n2), 1)
    part = jnp.zeros((1, n2), jnp.float32)
    for q, s in enumerate(sums):
        part = jnp.where(lane1 == q, jnp.sum(jnp.sum(s, axis=0, keepdims=True), axis=1, keepdims=True), part)

    def slot(axes, at):
        index = 0
        for a in axes:
            index = index * sizes[a] + at(a)
        return index

    def sum_message(p, offs, sign):
        axes, slots = phases[p], slots_of[p]
        other = partner(axes, offs, sign)
        index = slot(axes, (lambda a: me[a]) if sign > 0 else (lambda a: other[AXES[a]]))
        sem = p * slots_of[0].shape[0] + slot(axes, lambda a: offs[axes.index(a)])
        return pltpu.make_async_remote_copy(
            src_ref=slots.at[index], dst_ref=slots.at[index], send_sem=psend.at[sem], recv_sem=precv.at[sem],
            device_id=other, device_id_type=MESH,
        )

    def sum_start(p, value):
        slots_of[p][slot(phases[p], lambda a: me[a])] = value
        for offs in offsets(phases[p]):
            sum_message(p, offs, 1).start()

    def sum_end(p):
        for offs in offsets(phases[p]):
            sum_message(p, offs, -1).wait_recv()
        terms = [slots_of[p][d] for d in range(slots_of[p].shape[0])]
        while len(terms) > 1:
            terms = [functools.reduce(lambda x, y: x + y, terms[t : t + 2]) for t in range(0, len(terms), 2)]
        return terms[0]

    sum_start(0, part)
    fence()
    rows_x(V2I, V2)
    spread_near(2, V2, w2)
    rows_x(V1I, V1)
    spread_near(1, V1, ws)
    gradients(1, G1)
    gradients(2, G2)
    for k in (1, 2, 0):
        smooth(k)
    gradients(0, OB)

    def drain(fields):
        for a in range(3):
            for d in (0, 1):
                def over(a=a, d=d):
                    for f in fields:
                        if f not in LOCAL and d in dirs(f):
                            message(f, a, d).wait_send()
                pl.when(can_send(a, d))(over)

    drain(range(FIELDS))
    for offs in lines:
        pl.when(exists(offs))(lambda offs=offs: line_message(offs, 1).wait_send())
    for at in CROSS + GREET:
        pl.when(exists(cross_offs(*at, 1)))(lambda at=at: cross_message(*at, 1).wait_send())

    for offs in offsets(phases[0]):
        sum_message(0, offs, 1).wait_send()
    for j, f in enumerate(FINAL):
        for a in range(3):
            receive(f, a)
        HZ[j] = F[j, n0, 0:n1]
        HX[j] = RX[f, 1]
        HY[j] = RY[f, 1]

    part = sum_end(0)
    for p in range(1, len(phases)):
        sum_start(p, part)
        part = sum_end(p)
        for offs in offsets(phases[p]):
            sum_message(p, offs, 1).wait_send()
    gone, hone, hmix, htwo = [
        jnp.sum(jnp.where(lane1 == q, part, 0.0), axis=1, keepdims=True) for q in range(4)
    ]
    two = (hone - hmix * gone / hone) / (htwo - hmix * hmix / hone)
    oneco = (gone - hmix * two) / hone
    CO[0:1] = jnp.broadcast_to(oneco, (1, n2))
    CO[1:2] = jnp.broadcast_to(two, (1, n2))


def combine(parts, OB, G1, G2, CO, HZ, HX, HY, out, W, sem):
    _, n0, n1, n2 = OB.shape
    one = jnp.broadcast_to(CO[0:1], (n1, n2))
    two = jnp.broadcast_to(CO[1:2], (n1, n2))
    groups, per, step = n1 // 8, n2 // 2, n0 // parts
    row8 = lax.broadcasted_iota(jnp.int32, (8, n2), 0)
    lane_full = lax.broadcasted_iota(jnp.int32, (n1, n2), 1)

    def mix(get):
        a = get(0)
        c1, c2 = [jnp.broadcast_to(CO[q : q + 1], a.shape) for q in (0, 1)]
        return a + c1 * get(1) + c2 * get(2)

    ends = [pltpu.roll(mix(lambda j: HY[j, v]), n2 - 1, 1) for v in range(HY.shape[1])]

    def edge(k, i, x):
        if k == 0:
            return x + mix(lambda j: HZ[j]) if i == n0 - 1 else x
        if k == 1:
            last = x[n1 - 8 : n1] + jnp.where(row8 == 7, mix(lambda j: HX[j, i : i + 1]), 0.0)
            return jnp.concatenate([x[0 : n1 - 8], last], axis=0)
        ats = [divmod(i * groups + g, per) for g in range(groups)]
        parts = [pltpu.roll(ends[v], (n2 - 2 * kk) % n2, 1) for v, kk in ats]
        return x + jnp.where(lane_full >= n2 - 1, jnp.concatenate(parts, axis=0), 0.0)

    copies = []
    for k in range(3):
        for h in range(parts):
            for i in range(h * step, (h + 1) * step):
                W[k, i] = edge(k, i, OB[k, i] + one * G1[k, i] + two * G2[k, i])
            planes = pl.ds(h * step, step)
            copies.append(pltpu.make_async_copy(W.at[k, planes], out.at[k, planes], sem.at[k * parts + h]))
            copies[-1].start()
    for c in copies:
        c.wait()


def solution(mesh):
    sizes = tuple(mesh.shape[a] for a in AXES)

    def local(residual, edge_diag, node_shift, coarse_shift):
        n0, n1, n2 = node_shift.shape
        m0, m1, m2 = coarse_shift.shape
        vecs = max(-(-(n0 * (n1 // 8)) // (n2 // 2)), -(-(m0 * (n1 // 8)) // (n2 // 4)))
        f32 = jnp.float32
        counts = [math.prod(sizes[a] for a in axes) for axes in phases_of(sizes)]
        V = lambda *s: pltpu.VMEM(s, f32)
        scratch = [
            V(3, n0, n1, n2), V(3, n0, n1, n2), V(n0, n1, n2), V(m0, m1, m2),
            V(3, n0 + 2, n1 + 2 * PAD, n2), V(n0 + 2, n1 + 2 * PAD, n2),
            V(m0, n1, n2), V(m0, n1, n2), V(m0, n1, n2), V(m0, n1, n2), V(m0, n1 + 2 * PAD, n2),
            V(m0 + 2, n1 + 2 * PAD, n2), V(m0 + 2, n1 + 2 * PAD, n2),
            V(3, n0 + 1, n1 + PAD, n2),
            V(FIELDS, 2, n0, n2), V(FIELDS, 2, n0, n2), V(FIELDS, vecs, 8, n2), V(FIELDS, 2, vecs, 8, n2),
            V(2, n1, n2), V(2, n1, n2), V(2, 2, 1, n2), V(2, vecs, 1, n2),
            V(2, 2, 1, n2), V(2, 2, 8, n2), V(2, 2, vecs, 1, n2),
            V(n0, n1, n2), V(2, n1, n2), V(2, n1, n2), V(2, 1, n2), V(2, 1, n2), V(2, vecs, 1, n2), V(vecs, 1, n2),
            V(8, n2), V(2, 1, n2), V(2, 1, n2), V(2, 8, n2), V(2, 8, n2), V(2, vecs, 1, n2), V(2, vecs, 1, n2), V(n0 + 2 * PAD, n2), V(3, 1, n2),
            *[V(c, 1, n2) for c in counts],
        ]
        sems = [pltpu.SemaphoreType.DMA(s) for s in ((20,), *[(FIELDS, 3, 2)] * 2, *[(sum(counts),)] * 2, *[(12,)] * 2, *[(15,)] * 2)]

        def scoped(*refs):
            plain, slots_of = refs[: -len(counts)], refs[-len(counts) :]
            pl.run_scoped(functools.partial(kernel, sizes, *plain, slots_of), *sems)

        field = pltpu.VMEM(residual.shape, f32)
        limit = 67_043_328 - 12 * math.prod(residual.shape) - 2**18
        fields = pl.pallas_call(
            scoped,
            out_shape=[field] * 3 + [pltpu.VMEM(s, f32) for s in ((8, n2), (3, n1, n2), (3, n0, n2), (3, vecs, 8, n2))],
            in_specs=[pl.BlockSpec(memory_space=pltpu.HBM)] * 4,
            out_specs=[pl.BlockSpec(memory_space=pltpu.VMEM)] * 7,
            scratch_shapes=scratch,
            compiler_params=pltpu.CompilerParams(collective_id=0, has_side_effects=True, vmem_limit_bytes=limit),
        )(residual, edge_diag, node_shift, coarse_shift)
        parts = 2 if n0 % 2 == 0 else 1
        return pl.pallas_call(
            functools.partial(combine, parts),
            out_shape=jax.ShapeDtypeStruct(residual.shape, f32),
            in_specs=[pl.BlockSpec(memory_space=pltpu.VMEM)] * 7,
            out_specs=pl.BlockSpec(memory_space=pltpu.HBM),
            scratch_shapes=[field, pltpu.SemaphoreType.DMA((3 * parts,))],
            compiler_params=pltpu.CompilerParams(vmem_limit_bytes=8 * math.prod(residual.shape)),
        )(*fields)

    placed = (
        P(None, "gz", "gx", "gy"),
        P(None, "gz", "gx", "gy"),
        P("gz", "gx", "gy"),
        P("gz", "gx", "gy"),
    )
    return jax.shard_map(
        local, mesh=mesh, in_specs=placed, out_specs=P(None, "gz", "gx", "gy"), check_vma=False
    )
```
